256 devices in a mesh: freq: 32 (over z_hi, y, x), slab: 8 (over z_lo, core).
Axes of the slice: x: 4, y: 4, z: 8 (z_hi: 2, z_lo: 4; z = z_hi * 4 + z_lo), core: 2. Of those that a mesh axis runs over, the one named last changes fastest.
Arguments:
- log_conductivity: float32 [40, 32, 128], P('slab'), may hold values from -1 to 1
- omega: float32 [32], P('freq'), may hold values from 0.1 to 2
- sources: float32 [32, 2, 2, 3, 40, 32, 128], P('freq', None, None, None, 'slab'), may hold values from -8 to 8
- receivers: int32 [1024], P('slab'), may hold values from 0 to 20479
- observed: float32 [32, 2, 2, 3, 1024], P('freq', None, None, None, 'slab'), may hold values from -2.4 to 2.4
- data_weight: float32 [32, 2, 3, 1024], P('freq', None, None, 'slab'), may hold values from 3 to 30
- prior_gradient: float32 [40, 32, 128], P('slab', 'freq'), may hold values from -6 to 6
- prior_direction: float32 [40, 32, 128], P('slab', 'freq'), may hold values from -6 to 6
- step_length: float32 [1], replicated, may hold values from 0.2 to 0.6
Outputs:
- unit_direction: float32 [40, 32, 128], P('slab', 'freq')
- trial_model: float32 [40, 32, 128], P('slab')
The draws below stay inside these ranges and needn't reach their ends.
Inputs may be any that keep to these rules, and one draw needn't show every extreme that they name: Each block of 128 receivers belongs to one slab of 5 layers, slabs in order; an entry is z * 32 * 128 + y * 128 + x within its slab; cells may repeat.
All inputs are finite; a program needn't handle non-finite values.
Results may differ from the reference program's by a relative error of at most 0.0011.
Values sent between devices are 32-bit elements; how exact they have to be, the bound alone decides.
A program may use at most 128 MiB of HBM per device.

```python
import math
import jax
import jax.numpy as jnp
from jax import lax

NX = 128
NY = 32
CZ = 5
REC_DEV = 128
ITERS = 4
FREQS = 32
NZ = 40
RECS = 1024


def draw_sources(key, part):
    shape = (FREQS, 2, 2, 3, NZ, NY, NX)
    depth_scale = (0.5 + jnp.arange(NZ, dtype=jnp.float32) / NZ)[:, None, None]
    drawn_values = jax.random.normal(key, shape, jnp.float32) * depth_scale
    return jnp.clip(drawn_values, -8.0, 8.0)


def place_ends(entries, own_key, low, high):
    longest = entries.shape.index(max(entries.shape))
    spots = []
    for shift in (0, 1):
        where = [jax.random.randint(jax.random.fold_in(own_key, axis), (), 0, length) for axis, length in enumerate(entries.shape)]
        where[longest] = (where[longest] + shift) % entries.shape[longest]
        spots.append(tuple(where))
    return entries.at[spots[0]].set(low).at[spots[1]].set(high)


def level_of(key, shape, cuts, smallest, largest):
    level, own = 1.0, jax.random.fold_in(key, 6)
    for position, shards_of in cuts:
        draws = jnp.exp(jax.random.uniform(jax.random.fold_in(own, position), (shards_of,), jnp.float32, smallest / len(cuts), largest / len(cuts)))
        level = level * jnp.repeat(draws, shape[position] // shards_of).reshape([-1 if axis == position else 1 for axis in range(len(shape))])
    return level


def noise(key, shape, scale, most, shards=(), kind=jnp.bfloat16):
    factor_of = level_of(key, shape, shards, -0.22, 0.18) if shards else 1.0
    result = jax.random.normal(key, shape, jnp.float32) * scale * factor_of
    return jnp.minimum(jnp.maximum(result, -most), most).astype(kind)


def setup_inputs(seed: int = 0) -> dict:
    key_of = jax.random.split(jax.random.key(seed), 10)
    log_conductivity = jnp.clip(jax.random.uniform(key_of[0], (NZ, NY, NX), jnp.float32, -1.0, 1.0) * level_of(key_of[0], (NZ, NY, NX), ((0, 8),), -0.4, 0.0), -1.0, 1.0)
    omega = jnp.clip(jnp.exp(math.log(2.0) - 2.9957323 * jax.random.uniform(key_of[1], (FREQS,), jnp.float32) ** level_of(key_of[1], (FREQS,), ((0, 32),), -0.2, 0.2)), 0.1, 2.0)
    sources = draw_sources(jax.random.fold_in(key_of[9], 71), 0)
    receivers = place_ends(jax.random.randint(key_of[3], (RECS,), 0, CZ * NY * NX), jax.random.fold_in(key_of[3], 1), 0, (CZ * NY * NX) - 1).astype(jnp.int32)
    observed = noise(key_of[4], (FREQS, 2, 2, 3, RECS), 0.3, 2.4, ((0, 32), (4, 8)), jnp.float32)
    data_weight = jnp.clip(jnp.exp(math.log(30.0) - 2.3025851 * jax.random.uniform(key_of[5], (FREQS, 2, 3, RECS), jnp.float32) ** level_of(key_of[5], (FREQS, 2, 3, RECS), ((0, 32), (3, 8)), -0.2, 0.2)), 3.0, 30.0)
    prior_gradient = noise(key_of[6], (NZ, NY, NX), 1.0, 6.0, ((0, 8), (1, 32)), jnp.float32)
    prior_direction = noise(key_of[7], (NZ, NY, NX), 1.0, 6.0, ((0, 8), (1, 32)), jnp.float32)
    step_length = jnp.clip(jax.random.uniform(key_of[8], (1,), jnp.float32, 0.2, 0.6), 0.2, 0.6)
    return {"log_conductivity": log_conductivity, "omega": omega, "sources": sources, "receivers": receivers, "observed": observed, "data_weight": data_weight, "prior_gradient": prior_gradient, "prior_direction": prior_direction, "step_length": step_length}


epsilon = 1e-06

def complex_div(dividend, divisor):
    modulus = divisor[0] * divisor[0] + divisor[1] * divisor[1]
    return jnp.stack([(dividend[0] * divisor[0] + dividend[1] * divisor[1]) / modulus, (dividend[1] * divisor[0] - dividend[0] * divisor[1]) / modulus])

def scaled(factor, vector):
    factor_re = factor[0][:, None, None, None, None]
    factor_im = factor[1][:, None, None, None, None]
    return jnp.stack([factor_re * vector[:, 0] - factor_im * vector[:, 1], factor_re * vector[:, 1] + factor_im * vector[:, 0]], axis=1)

def inner_sums(former, latter):
    real_part = lax.optimization_barrier(jnp.sum(former[:, 0] * latter[:, 0] - former[:, 1] * latter[:, 1], axis=(1, 2, 3, 4)))
    imag_part = lax.optimization_barrier(jnp.sum(former[:, 0] * latter[:, 1] + former[:, 1] * latter[:, 0], axis=(1, 2, 3, 4)))
    return jnp.stack([real_part, imag_part])

def operate(electric, coupling):
    padded = jnp.pad(electric, ((0, 0), (0, 0), (0, 0), (1, 1), (1, 1), (1, 1)))
    beside = padded[..., 2:, 1:-1, 1:-1] + padded[..., :-2, 1:-1, 1:-1]
    beside = beside + padded[..., 1:-1, 2:, 1:-1] + padded[..., 1:-1, :-2, 1:-1]
    beside = beside + padded[..., 1:-1, 1:-1, 2:] + padded[..., 1:-1, 1:-1, :-2]
    laplace = 6.0 * electric - beside
    return jnp.stack([laplace[:, 0] - coupling * electric[:, 1], laplace[:, 1] + coupling * electric[:, 0]], axis=1)

def krylov_solve(source, coupling):
    solution = jnp.zeros_like(source)
    residual = source
    direction = source
    rho_now = inner_sums(residual, residual)
    for iteration in range(ITERS):
        image = operate(direction, coupling)
        alpha_step = complex_div(rho_now, inner_sums(direction, image))
        solution = solution + scaled(alpha_step, direction)
        residual = residual - scaled(alpha_step, image)
        if iteration + 1 < ITERS:
            rho_next = inner_sums(residual, residual)
            beta_ratio = complex_div(rho_next, rho_now)
            direction = residual + scaled(beta_ratio, direction)
            rho_now = rho_next
    return solution

def reference(log_conductivity, omega, sources, receivers, observed, data_weight, prior_gradient, prior_direction, step_length):
    conductivity = jnp.exp(log_conductivity)
    slab_cells = CZ * NY * NX
    owner_slab = jnp.arange(RECS, dtype=jnp.int32) // REC_DEV
    flat_index = (owner_slab * slab_cells + receivers).astype(jnp.int32)

    def one_frequency(member):
        frequency, source, observed_now, weight = member
        coupling = frequency * conductivity
        electric = krylov_solve(source, coupling)
        flat_field = electric.reshape(2, 2, 3, NZ * NY * NX)
        misfit = flat_field[..., flat_index] - observed_now
        weight_sq = weight * weight
        adjoint_data = jnp.stack([weight_sq * misfit[:, 0], -weight_sq * misfit[:, 1]], axis=1)
        adjoint_source = jnp.zeros_like(flat_field).at[..., flat_index].add(adjoint_data).reshape(electric.shape)
        adjoint = krylov_solve(adjoint_source, coupling)
        return coupling * lax.optimization_barrier(jnp.sum(adjoint[:, 0] * electric[:, 1] + adjoint[:, 1] * electric[:, 0], axis=(0, 1)))
    freq_terms = lax.map(one_frequency, (omega, sources, observed, data_weight))
    gradient = lax.optimization_barrier(jnp.sum(freq_terms, axis=0))
    mean_square = jnp.mean(gradient * gradient)
    scaled_grad = gradient / jnp.sqrt(mean_square + epsilon)
    beta_ratio = (jnp.sum(scaled_grad * scaled_grad) - jnp.sum(scaled_grad * prior_gradient)) / (jnp.sum(prior_gradient * prior_gradient) + epsilon)
    direction = -scaled_grad + beta_ratio * prior_direction
    unit_direction = direction / jnp.sqrt(jnp.mean(direction * direction) + epsilon)
    trial_model = log_conductivity + step_length[0] * unit_direction
    return (unit_direction, trial_model)
```

```python
import functools

import jax
import jax.numpy as jnp
from jax import lax
from jax.experimental import pallas as pl
from jax.experimental.pallas import tpu as pltpu
from jax.sharding import PartitionSpec as P


MESH = pl.DeviceIdType.MESH
epsilon = 1e-06
F32 = jnp.float32
BF16 = jnp.bfloat16
LOW = 3
HIGH = 4


def cmul(a, b):
    return a[0] * b[0] - a[1] * b[1], a[0] * b[1] + a[1] * b[0]


def cadd(a, b):
    return a[0] + b[0], a[1] + b[1]


def csub(a, b):
    return a[0] - b[0], a[1] - b[1]


def cdiv(a, b):
    modulus = b[0] * b[0] + b[1] * b[1]
    return (a[0] * b[0] + a[1] * b[1]) / modulus, (a[1] * b[0] - a[0] * b[1]) / modulus


def square_poly(p):
    out = [None] * (2 * len(p) - 1)
    for i in range(len(p)):
        for j in range(i, len(p)):
            term = cmul(p[i], p[j])
            if j > i:
                term = (term[0] + term[0], term[1] + term[1])
            out[i + j] = term if out[i + j] is None else cadd(out[i + j], term)
    return out


def against(poly, moments):
    total = None
    for c, m in zip(poly, moments):
        term = cmul(c, m)
        total = term if total is None else cadd(total, term)
    return total


def coefficients(moments):
    steps = [csub(a, b) for a, b in zip(moments, moments[1:])]
    one = (jnp.ones_like(moments[0][0]), jnp.zeros_like(moments[0][0]))
    residual, direction, rho = [one], [one], moments[0]
    solution = []
    for iteration in range(4):
        alpha = cdiv(rho, against(square_poly(direction), steps))
        moved = [cmul(alpha, c) for c in direction]
        solution = [cadd(a, b) for a, b in zip(solution, moved)] + moved[len(solution) :]
        if iteration < 3:
            grown = [csub(r, m) for r, m in zip(residual, moved)]
            grown.append((jnp.zeros_like(rho[0]), jnp.zeros_like(rho[0])))
            residual = [grown[0]] + [cadd(grown[k + 1], moved[k]) for k in range(len(moved))]
            rho_next = against(square_poly(residual), moments)
            beta = cdiv(rho_next, rho)
            direction = [
                cadd(residual[k], cmul(beta, direction[k])) for k in range(len(direction))
            ] + [residual[-1]]
            rho = rho_next
    return [(c[0] * 6.0 ** -(k + 1), c[1] * 6.0 ** -(k + 1)) for k, c in enumerate(solution)]


def split3(x):
    high = x.astype(BF16)
    rest = x - high.astype(F32)
    mid = rest.astype(BF16)
    low = (rest - mid.astype(F32)).astype(BF16)
    return high, mid, low


def kernel(
    layers,
    slabs,
    positions,
    omega_ref,
    step_ref,
    logc_ref,
    src_ref,
    rec_ref,
    obs_ref,
    wt_ref,
    pg_ref,
    pd_ref,
    dir_ref,
    trial_ref,
    v0,
    v1,
    v2,
    v3,
    field,
    kap,
    lcg,
    recs,
    data,
    allred,
    prior_pair,
    prior_all,
    grad,
    grad_src,
    grad_in,
    grad_pair,
    grad_all,
    unit,
    natural,
    load_sem,
    near_send,
    near_recv,
    data_send,
    data_recv,
    ar_send,
    ar_recv,
    pair_send,
    pair_recv,
    fan_send,
    fan_recv,
):
    freq = lax.axis_index("freq")
    slab = lax.axis_index("slab")
    half = freq // positions
    place = freq % positions
    base = half * positions
    partner = (1 - half) * positions + place
    own_lo, own_hi = LOW, LOW + layers
    total_layers = LOW + layers + HIGH

    def remote(src, dst, send, recv, to):
        return pltpu.make_async_remote_copy(
            src_ref=src, dst_ref=dst, send_sem=send, recv_sem=recv, device_id=to, device_id_type=MESH
        )

    barrier = pltpu.get_barrier_semaphore()
    for d in range(1, slabs):
        to = (freq, (slab + d) % slabs)
        pl.semaphore_signal(barrier, inc=1, device_id=to, device_id_type=MESH)
    for d in range(1, positions):
        to = (base + (place + d) % positions, slab)
        pl.semaphore_signal(barrier, inc=1, device_id=to, device_id_type=MESH)
    pl.semaphore_signal(barrier, inc=1, device_id=(partner, slab), device_id_type=MESH)

    load = pltpu.make_async_copy(
        src_ref, v0.at[:, pl.ds(own_lo, layers), pl.ds(8, 32), :], load_sem
    )
    load.start()

    edge = jnp.zeros((12, total_layers, 8, 128), F32)
    for v in (v0, v1, v2, v3):
        v[:, :, 0:8, :] = edge
        v[:, :, 40:48, :] = edge
    has_below = slab > 0
    has_above = slab < slabs - 1

    @pl.when(slab == 0)
    def _():
        v0[:, 0:LOW, 8:40, :] = jnp.zeros((12, LOW, 32, 128), F32)
        lcg[0:2] = jnp.zeros((2, 32, 128), F32)
        recs[0] = jnp.zeros((1, 128), jnp.int32)
        data[0] = jnp.zeros((12, 128), F32)

    @pl.when(slab == slabs - 1)
    def _():
        v0[:, own_hi:total_layers, 8:40, :] = jnp.zeros((12, HIGH, 32, 128), F32)
        lcg[2:5] = jnp.zeros((3, 32, 128), F32)
        recs[2] = jnp.zeros((1, 128), jnp.int32)
        data[2] = jnp.zeros((12, 128), F32)

    omega = omega_ref[0]
    kap[own_lo:own_hi] = omega * jnp.exp(logc_ref[...])
    for l in range(layers):
        prior_pair[half, 0, l : l + 1, :] = pg_ref[l]
        prior_pair[half, 1, l : l + 1, :] = pd_ref[l]
    recs[1] = rec_ref[...]

    load.wait()
    pl.semaphore_wait(barrier, slabs + positions - 1)

    rows = pl.ds(8, 32)
    below_to = (freq, lax.max(slab - 1, 0))
    above_to = (freq, lax.min(slab + 1, slabs - 1))
    upward = []
    downward = []
    upward.append((rec_ref, recs.at[0]))
    downward.append((rec_ref, recs.at[2]))
    upward.append((logc_ref.at[pl.ds(layers - 2, 2)], lcg.at[pl.ds(0, 2)]))
    downward.append((logc_ref.at[pl.ds(0, 3)], lcg.at[pl.ds(2, 3)]))
    for k in range(HIGH):
        if k < LOW:
            upward.append(
                (v0.at[:, own_hi - 1 - k, rows, :], v0.at[:, own_lo - 1 - k, rows, :])
            )
        downward.append((v0.at[:, own_lo + k, rows, :], v0.at[:, own_hi + k, rows, :]))
    ups = [
        remote(s, d, near_send.at[0, n], near_recv.at[0, n], above_to)
        for n, (s, d) in enumerate(upward)
    ]
    downs = [
        remote(s, d, near_send.at[1, n], near_recv.at[1, n], below_to)
        for n, (s, d) in enumerate(downward)
    ]

    @pl.when(has_above)
    def _():
        for c in ups:
            c.start()

    @pl.when(has_below)
    def _():
        for c in downs:
            c.start()

    prior_copy = remote(
        prior_pair.at[half], prior_pair.at[half], pair_send.at[0], pair_recv.at[0], (partner, slab)
    )
    prior_copy.start()

    def arrived(n):
        if n < len(ups):

            @pl.when(has_below)
            def _():
                ups[n].wait_recv()

        @pl.when(has_above)
        def _():
            downs[n].wait_recv()

    lane = lax.broadcasted_iota(jnp.int32, (32, 128), 1)
    first_lane, last_lane = lane == 0, lane == 127
    alive_low = jnp.where(slab == 0, 0.0, 1.0).astype(F32)
    alive_high = jnp.where(slab == slabs - 1, 0.0, 1.0).astype(F32)

    def step(src, dst, l, mask=None):
        coupling = kap[l]

        def around(p):
            here = src[p, l, 8:40, :]
            total = src[p, l - 1, 8:40, :] + src[p, l + 1, 8:40, :]
            total = total + (src[p, l, 7:39, :] + src[p, l, 9:41, :])
            left = jnp.where(first_lane, 0.0, pltpu.roll(here, 1, 1))
            right = jnp.where(last_lane, 0.0, pltpu.roll(here, 127, 1))
            return here, total + (left + right)

        for pol in range(2):
            for comp in range(3):
                p = pol * 6 + comp
                re, around_re = around(p)
                im, around_im = around(p + 3)
                new_re = around_re + coupling * im
                new_im = around_im - coupling * re
                if mask is not None:
                    new_re, new_im = mask * new_re, mask * new_im
                dst[p, l, 8:40, :] = new_re
                dst[p + 3, l, 8:40, :] = new_im

    def sweep(src, dst, lo, hi, mask=None):
        def body(l, carry):
            step(src, dst, l, mask)
            return carry

        lax.fori_loop(lo, hi, body, 0)

    def both(src, dst, low, high, ghost):
        def body(n, carry):
            mask = jnp.where(n == 0, alive_low, alive_high) if ghost else None
            step(src, dst, low + n * (high - low), mask)
            return carry

        lax.fori_loop(0, 2, body, 0)

    def moment_row(v_list):
        a, b, c, e = v_list
        sums = []
        lane8 = lax.broadcasted_iota(jnp.int32, (8, 128), 1)
        last8 = lane8 == 127
        for pol in range(2):

            def body(l, acc):
                acc = list(acc)

                def add(k, value):
                    acc[k] = acc[k] + value

                for comp in range(3):
                    p = pol * 6 + comp
                    for r in range(4):
                        y = 8 + 8 * r
                        vs = [(v[p, l, y : y + 8, :], v[p + 3, l, y : y + 8, :]) for v in v_list]
                        for k in range(4):
                            re, im = vs[k]
                            add(4 * k, (re - im) * (re + im))
                            add(4 * k + 1, re * im)
                        coupling = kap[l, 8 * r : 8 * r + 8, :]
                        halves = []
                        for q in (p, p + 3):
                            here = e[q, l, y : y + 8, :]
                            right = jnp.where(last8, 0.0, pltpu.roll(here, 127, 1))
                            more = e[q, l + 1, y : y + 8, :] + e[q, l, y + 1 : y + 9, :] + right
                            halves.append(more + more)
                        re, im = vs[3]
                        after = (halves[0] + coupling * im, halves[1] - coupling * re)
                        pairs = [(vs[0], vs[1]), (vs[1], vs[2]), (vs[2], vs[3]), (vs[3], after)]
                        for k, (u, w) in enumerate(pairs):
                            add(4 * k + 2, u[0] * w[0] - u[1] * w[1])
                            add(4 * k + 3, u[0] * w[1] + u[1] * w[0])
                return tuple(acc)

            zero = jnp.zeros((8, 128), F32)
            sums += list(lax.fori_loop(own_lo, own_hi, body, (zero,) * 16))
        lanes = lax.broadcasted_iota(jnp.int32, (1, 128), 1)
        row = jnp.zeros((1, 128), F32)
        for n, s in enumerate(sums):
            line = jnp.sum(s, axis=0, keepdims=True)
            row = row + jnp.where(lanes == n, jnp.sum(line, axis=1, keepdims=True), 0.0)
        return row

    def slab_total(n, row):
        allred[n, slab] = row
        copies = []
        for d in range(1, slabs):
            to = (freq, (slab + d) % slabs)
            copies.append(
                remote(
                    allred.at[n, slab],
                    allred.at[n, slab],
                    ar_send.at[n, d],
                    ar_recv.at[n, slab],
                    to,
                )
            )
        for c in copies:
            c.start()
        for d in range(1, slabs):
            other = (slab + d) % slabs
            remote(
                allred.at[n, other],
                allred.at[n, other],
                ar_send.at[n, d],
                ar_recv.at[n, other],
                (freq, other),
            ).wait_recv()
        total = allred[n, 0]
        for j in range(1, slabs):
            total = total + allred[n, j]
        return total, copies

    def solve_coefficients(row):
        lanes = lax.broadcasted_iota(jnp.int32, (1, 128), 1)

        def pick(n):
            return jnp.sum(jnp.where(lanes == n, row, 0.0), axis=1, keepdims=True)

        found = []
        for pol in range(2):
            moments = []
            for k in range(8):
                re = pick(16 * pol + 2 * k) * 6.0**-k
                im = pick(16 * pol + 2 * k + 1) * 6.0**-k
                if k % 2 == 0:
                    im = im + im
                moments.append((re, im))
            most = None
            for m in moments:
                size = jnp.maximum(jnp.abs(m[0]), jnp.abs(m[1]))
                most = size if most is None else jnp.maximum(most, size)
            moments = [(m[0] / most, m[1] / most) for m in moments]
            found.append(coefficients(moments))
        return found

    def combined(coefs, pol, comp, l, y):
        p = pol * 6 + comp
        re = im = None
        for (cr, ci), v in zip(coefs[pol], (v0, v1, v2, v3)):
            a, b = v[p, l, y : y + 8, :], v[p + 3, l, y : y + 8, :]
            tr, ti = cr * a - ci * b, cr * b + ci * a
            re, im = (tr, ti) if re is None else (re + tr, im + ti)
        return re, im

    sweep(v0, v1, own_lo + 1, own_hi - 1)
    step(v1, v2, own_lo + 2)
    arrived(0)
    arrived(1)
    kap[1:3] = omega * jnp.exp(lcg[0:2])
    kap[own_hi : own_hi + 3] = omega * jnp.exp(lcg[2:5])
    arrived(2)
    both(v0, v1, own_lo, own_hi - 1, False)
    both(v1, v2, own_lo + 1, own_hi - 2, False)
    step(v2, v3, own_lo + 2)
    arrived(3)
    both(v0, v1, own_lo - 1, own_hi, True)
    both(v1, v2, own_lo, own_hi - 1, False)
    both(v2, v3, own_lo + 1, own_hi - 2, False)
    arrived(4)
    both(v0, v1, own_lo - 2, own_hi + 1, True)
    both(v1, v2, own_lo - 1, own_hi, True)
    both(v2, v3, own_lo, own_hi - 1, False)
    arrived(5)
    step(v0, v1, own_hi + 2, alive_high)
    step(v1, v2, own_hi + 1, alive_high)
    step(v2, v3, own_hi, alive_high)
    row, sent_a = slab_total(0, moment_row((v0, v1, v2, v3)))
    coefs = solve_coefficients(row)

    def write_field(l, carry):
        for pol in range(2):
            for comp in range(3):
                for r in range(4):
                    re, im = combined(coefs, pol, comp, l, 8 + 8 * r)
                    field[pol * 6 + comp, l - own_lo, 8 * r : 8 * r + 8, :] = re
                    field[pol * 6 + 3 + comp, l - own_lo, 8 * r : 8 * r + 8, :] = im
        return carry

    lax.fori_loop(own_lo, own_hi, write_field, 0)

    def onehots(n):
        where = recs[n]
        return where // 128, where % 128

    wide = 32 * layers
    line_of, lane_of = onehots(1)
    column = (lax.broadcasted_iota(jnp.int32, (128, 128), 0) == lane_of).astype(F32)
    column = column.astype(BF16)
    taller = jnp.concatenate([column] * 3, axis=0)
    at_row = lax.broadcasted_iota(jnp.int32, (wide, 128), 0) == line_of
    for pol in range(2):
        for ri in range(2):
            for comp in range(3):
                p = pol * 6 + ri * 3 + comp
                plane = field[p].reshape(wide, 128)
                parts = jnp.concatenate(split3(plane), axis=1)
                seen = jnp.dot(parts, taller, preferred_element_type=F32)
                value = jnp.sum(jnp.where(at_row, seen, 0.0), axis=0, keepdims=True)
                misfit = value - obs_ref[pol, ri, comp : comp + 1, :]
                weight = wt_ref[pol, comp : comp + 1, :]
                weighted = weight * weight * misfit
                data[1, p : p + 1, :] = weighted if ri == 0 else -weighted

    data_up = remote(data.at[1], data.at[0], data_send.at[0], data_recv.at[0], above_to)
    data_down = remote(data.at[1], data.at[2], data_send.at[1], data_recv.at[1], below_to)

    @pl.when(has_above)
    def _():
        data_up.start()
        for c in ups:
            c.wait_send()

    @pl.when(has_below)
    def _():
        data_down.start()
        for c in downs:
            c.wait_send()

    prior_copy.wait()
    prior_all[place] = prior_pair[...]
    fan = []
    for d in range(1, positions):
        to = (base + (place + d) % positions, slab)
        fan.append(
            remote(prior_pair, prior_all.at[place], fan_send.at[0, d], fan_recv.at[0, place], to)
        )
    for c in fan:
        c.start()

    def scatter(n, first_row, count, layer_at):
        line_of, lane_of = onehots(n)
        column = (lax.broadcasted_iota(jnp.int32, (128, 128), 0) == lane_of).astype(F32)
        column = column.astype(BF16)
        wider = jnp.concatenate([column] * 3, axis=1)
        rows_here = lax.broadcasted_iota(jnp.int32, (32 * count, 128), 0) + first_row
        hit = rows_here == line_of
        for p in range(12):
            parts = split3(data[n, p : p + 1, :])
            spread = [
                jnp.where(hit, part.astype(F32), 0.0).astype(BF16) for part in parts
            ]
            placed = lax.dot_general(
                jnp.concatenate(spread, axis=1),
                wider,
                (((1,), (1,)), ((), ())),
                preferred_element_type=F32,
            )
            v0[p, layer_at : layer_at + count, 8:40, :] = placed.reshape(count, 32, 128)

    scatter(1, 0, layers, own_lo)

    @pl.when(has_below)
    def _():
        data_up.wait_recv()

    @pl.when(has_above)
    def _():
        data_down.wait_recv()

    scatter(0, 32 * (layers - LOW), LOW, 0)
    scatter(2, 0, HIGH, own_hi)

    for src, dst, grow in ((v0, v1, 2), (v1, v2, 1), (v2, v3, 0)):
        if grow:
            sweep(src, dst, own_lo - grow, own_lo, alive_low)
        sweep(src, dst, own_lo, own_hi)
        sweep(src, dst, own_hi, own_hi + grow + 1, alive_high)
    row, sent_b = slab_total(1, moment_row((v0, v1, v2, v3)))
    coefs = solve_coefficients(row)

    def write_grad(l, carry):
        for r in range(4):
            total = None
            for pol in range(2):
                for comp in range(3):
                    re, im = combined(coefs, pol, comp, l, 8 + 8 * r)
                    f_re = field[pol * 6 + comp, l - own_lo, 8 * r : 8 * r + 8, :]
                    f_im = field[pol * 6 + 3 + comp, l - own_lo, 8 * r : 8 * r + 8, :]
                    term = re * f_im + im * f_re
                    total = term if total is None else total + term
            grad[l - own_lo, 8 * r : 8 * r + 8, :] = kap[l, 8 * r : 8 * r + 8, :] * total
        return carry

    lax.fori_loop(own_lo, own_hi, write_grad, 0)

    for y in range(2 * positions):
        for l in range(layers):
            grad_src[y % positions, y // positions, l : l + 1, :] = grad[l, y : y + 1, :]
    grad_in[place] = grad_src[place]
    spread = []
    for d in range(1, positions):
        j = (place + d) % positions
        spread.append(
            remote(
                grad_src.at[j],
                grad_in.at[place],
                fan_send.at[1, d],
                fan_recv.at[1, place],
                (base + j, slab),
            )
        )
    for c in spread:
        c.start()

    def gathered(n, ref):
        for d in range(1, positions):
            j = (place + d) % positions
            remote(
                ref.at[j], ref.at[j], fan_send.at[n, d], fan_recv.at[n, j], (base + j, slab)
            ).wait_recv()

    gathered(1, grad_in)
    partial = grad_in[0]
    for j in range(1, positions):
        partial = partial + grad_in[j]
    grad_pair[half] = partial
    pair_copy = remote(
        grad_pair.at[half], grad_pair.at[half], pair_send.at[1], pair_recv.at[1], (partner, slab)
    )
    pair_copy.start()
    gathered(0, prior_all)
    pair_copy.wait_recv()
    grad_all[place] = grad_pair[0] + grad_pair[1]
    share = []
    for d in range(1, positions):
        to = (base + (place + d) % positions, slab)
        share.append(
            remote(
                grad_all.at[place], grad_all.at[place], fan_send.at[2, d], fan_recv.at[2, place], to
            )
        )
    for c in share:
        c.start()
    gathered(2, grad_all)

    sums = [None] * 5
    for j in range(positions):
        for h in range(2):
            g, q, d = grad_all[j, h], prior_all[j, h, 0], prior_all[j, h, 1]
            for n, term in enumerate((g * g, g * q, g * d, q * q, d * d)):
                sums[n] = term if sums[n] is None else sums[n] + term
    lanes = lax.broadcasted_iota(jnp.int32, (1, 128), 1)
    row = jnp.zeros((1, 128), F32)
    for n, s in enumerate(sums):
        line = jnp.sum(s, axis=0, keepdims=True)
        row = row + jnp.where(lanes == n, jnp.sum(line, axis=1, keepdims=True), 0.0)
    row, sent_c = slab_total(2, row)
    gg, gq, gd, qq, dd = [
        jnp.sum(jnp.where(lanes == n, row, 0.0), axis=1, keepdims=True) for n in range(5)
    ]
    cells = float(slabs * layers * 32 * 128)
    mean_square = gg / cells + epsilon
    inverse = 1.0 / jnp.sqrt(mean_square)
    beta = (gg / mean_square - gq * inverse) / (qq + epsilon)
    squared = gg / mean_square - 2.0 * beta * (gd * inverse) + beta * beta * dd
    norm = 1.0 / jnp.sqrt(jnp.maximum(squared, 0.0) / cells + epsilon)
    from_grad = -inverse * norm
    from_prior = beta * norm
    for j in range(positions):
        for h in range(2):
            value = from_grad * grad_all[j, h] + from_prior * prior_all[j, h, 1]
            unit[j, h] = value
    for y in range(2 * positions):
        for l in range(layers):
            natural[l, y : y + 1, :] = unit[y % positions, y // positions, l : l + 1, :]
    for l in range(layers):
        dir_ref[l] = unit[place, half, l : l + 1, :]
    trial_ref[...] = logc_ref[...] + step_ref[0] * natural[...]

    @pl.when(has_above)
    def _():
        data_up.wait_send()

    @pl.when(has_below)
    def _():
        data_down.wait_send()

    pair_copy.wait_send()
    for c in sent_a + sent_b + sent_c + fan + spread + share:
        c.wait_send()


def per_device(
    slabs,
    positions,
    log_conductivity,
    omega,
    sources,
    receivers,
    observed,
    data_weight,
    prior_gradient,
    prior_direction,
    step_length,
):
    layers = log_conductivity.shape[0]
    total = LOW + layers + HIGH
    vmem = pl.BlockSpec(memory_space=pltpu.VMEM)
    smem = pl.BlockSpec(memory_space=pltpu.SMEM)
    wide = pltpu.VMEM((12, total, 48, 128), F32)
    chunk = (positions, 2, layers, 128)
    return pl.pallas_call(
        functools.partial(kernel, layers, slabs, positions),
        out_shape=(
            jax.ShapeDtypeStruct(prior_gradient.shape, F32),
            jax.ShapeDtypeStruct(log_conductivity.shape, F32),
        ),
        in_specs=[smem, smem, vmem, pl.BlockSpec(memory_space=pl.ANY)] + [vmem] * 5,
        out_specs=(vmem, vmem),
        scratch_shapes=[
            wide,
            wide,
            wide,
            wide,
            pltpu.VMEM((12, layers, 32, 128), F32),
            pltpu.VMEM((total, 32, 128), F32),
            pltpu.VMEM((5, 32, 128), F32),
            pltpu.VMEM((3, 1, 128), jnp.int32),
            pltpu.VMEM((3, 12, 128), F32),
            pltpu.VMEM((3, slabs, 1, 128), F32),
            pltpu.VMEM((2, 2, layers, 128), F32),
            pltpu.VMEM((positions, 2, 2, layers, 128), F32),
            pltpu.VMEM((layers, 32, 128), F32),
            pltpu.VMEM(chunk, F32),
            pltpu.VMEM(chunk, F32),
            pltpu.VMEM((2, 2, layers, 128), F32),
            pltpu.VMEM(chunk, F32),
            pltpu.VMEM(chunk, F32),
            pltpu.VMEM((layers, 32, 128), F32),
            pltpu.SemaphoreType.DMA,
            pltpu.SemaphoreType.DMA((2, 6)),
            pltpu.SemaphoreType.DMA((2, 6)),
            pltpu.SemaphoreType.DMA((2,)),
            pltpu.SemaphoreType.DMA((2,)),
            pltpu.SemaphoreType.DMA((3, slabs)),
            pltpu.SemaphoreType.DMA((3, slabs)),
            pltpu.SemaphoreType.DMA((2,)),
            pltpu.SemaphoreType.DMA((2,)),
            pltpu.SemaphoreType.DMA((3, positions)),
            pltpu.SemaphoreType.DMA((3, positions)),
        ],
        compiler_params=pltpu.CompilerParams(
            collective_id=0, has_side_effects=True, vmem_limit_bytes=48 * 1024 * 1024
        ),
        name="inversion_step",
    )(
        omega,
        step_length,
        log_conductivity,
        sources.reshape(12, layers, 32, 128),
        receivers.reshape(1, 128),
        observed[0],
        data_weight[0],
        prior_gradient,
        prior_direction,
    )


def solution(mesh):
    slabs = mesh.shape["slab"]
    positions = mesh.shape["freq"] // 2
    in_specs = (
        P("slab", None, None),
        P("freq"),
        P("freq", None, None, None, "slab", None, None),
        P("slab"),
        P("freq", None, None, None, "slab"),
        P("freq", None, None, "slab"),
        P("slab", "freq", None),
        P("slab", "freq", None),
        P(),
    )
    out_specs = (P("slab", "freq", None), P("slab", None, None))
    return jax.shard_map(
        functools.partial(per_device, slabs, positions),
        mesh=mesh,
        in_specs=in_specs,
        out_specs=out_specs,
        check_vma=False,
    )
```

```python
import functools

import jax
import jax.numpy as jnp
from jax import lax
from jax.experimental import pallas as pl
from jax.experimental.pallas import tpu as pltpu
from jax.sharding import PartitionSpec as P


MESH = pl.DeviceIdType.MESH
epsilon = 1e-06
F32 = jnp.float32
BF16 = jnp.bfloat16
LOW = 3
HIGH = 4


def cmul(a, b):
    return a[0] * b[0] - a[1] * b[1], a[0] * b[1] + a[1] * b[0]


def cadd(a, b):
    return a[0] + b[0], a[1] + b[1]


def csub(a, b):
    return a[0] - b[0], a[1] - b[1]


def cdiv(a, b):
    modulus = b[0] * b[0] + b[1] * b[1]
    return (a[0] * b[0] + a[1] * b[1]) / modulus, (a[1] * b[0] - a[0] * b[1]) / modulus


def square_poly(p):
    out = [None] * (2 * len(p) - 1)
    for i in range(len(p)):
        for j in range(i, len(p)):
            term = cmul(p[i], p[j])
            if j > i:
                term = (term[0] + term[0], term[1] + term[1])
            out[i + j] = term if out[i + j] is None else cadd(out[i + j], term)
    return out


def against(poly, moments):
    total = None
    for c, m in zip(poly, moments):
        term = cmul(c, m)
        total = term if total is None else cadd(total, term)
    return total


def coefficients(moments, theta):
    one = (jnp.ones_like(moments[0][0]), jnp.zeros_like(moments[0][0]))
    shift = (one[0] - theta[0] * (1.0 / 6.0), -theta[1] * (1.0 / 6.0))
    steps = [csub(cmul(shift, a), b) for a, b in zip(moments, moments[1:])]
    residual, direction, rho = [one], [one], moments[0]
    solution = []
    for iteration in range(4):
        alpha = cdiv(rho, against(square_poly(direction), steps))
        moved = [cmul(alpha, c) for c in direction]
        solution = [cadd(a, b) for a, b in zip(solution, moved)] + moved[len(solution) :]
        if iteration < 3:
            kept = [csub(r, cmul(shift, m)) for r, m in zip(residual, moved)]
            residual = [kept[0]]
            residual += [cadd(kept[k + 1], moved[k]) for k in range(len(moved) - 1)]
            residual += [moved[-1]]
            rho_next = against(square_poly(residual), moments)
            beta = cdiv(rho_next, rho)
            direction = [
                cadd(residual[k], cmul(beta, direction[k])) for k in range(len(direction))
            ] + [residual[-1]]
            rho = rho_next
    return [(c[0] * 6.0 ** -(k + 1), c[1] * 6.0 ** -(k + 1)) for k, c in enumerate(solution)]


def split3(x):
    high = x.astype(BF16)
    rest = x - high.astype(F32)
    mid = rest.astype(BF16)
    low = (rest - mid.astype(F32)).astype(BF16)
    return high, mid, low


def kernel(
    layers,
    slabs,
    positions,
    omega_in,
    step_in,
    logc_in,
    src_in,
    rec_in,
    obs_in,
    wt_in,
    pg_in,
    pd_in,
    dir_ref,
    trial_ref,
    omega_ref,
    step_ref,
    logc,
    obs,
    wt,
    pg,
    pd,
    v0,
    v1,
    v2,
    v3,
    field,
    kap,
    lcg,
    recs,
    data,
    allred,
    ends,
    prior_pair,
    prior_all,
    prior,
    grad,
    grad_src,
    grad_in,
    grad_pair,
    grad_all,
    whole,
    load_sem,
    near_send,
    near_recv,
    data_send,
    data_recv,
    ar_send,
    ar_recv,
    end_send,
    end_recv,
    pair_send,
    pair_recv,
    fan_send,
    fan_recv,
):
    freq = lax.axis_index("freq")
    slab = lax.axis_index("slab")
    half = freq // positions
    place = freq % positions
    base = half * positions
    cores = 2
    chips = slabs // cores
    line = 2 * chips
    high = half * chips + slab // cores
    core = slab % cores
    own_lo, own_hi = LOW, LOW + layers
    total_layers = LOW + layers + HIGH
    wide = 32 * layers
    chunk = wide // positions

    def remote(src, dst, send, recv, to):
        return pltpu.make_async_remote_copy(
            src_ref=src, dst_ref=dst, send_sem=send, recv_sem=recv, device_id=to, device_id_type=MESH
        )

    def on_line(away, other_core):
        z = (high + away) % line
        return (z // chips) * positions + place, (z % chips) * cores + other_core

    partner = on_line(chips, core)

    loads = [
        pltpu.make_async_copy(s, d, load_sem.at[n])
        for n, (s, d) in enumerate(
            (
                (src_in, v0.at[:, pl.ds(own_lo, layers), pl.ds(8, 32), :]),
                (logc_in, logc),
                (omega_in, omega_ref),
                (rec_in, recs.at[1]),
                (pg_in, pg),
                (pd_in, pd),
                (obs_in, obs),
                (wt_in, wt),
                (step_in, step_ref),
            )
        )
    ]
    for c in loads:
        c.start()
    barrier = pltpu.get_barrier_semaphore()
    greeted = [on_line(0, 1 - core)]
    greeted += [on_line(away, c) for away in range(1, line) for c in range(cores)]
    greeted += [(base + (place + d) % positions, slab) for d in range(1, positions)]
    for to in greeted:
        pl.semaphore_signal(barrier, inc=1, device_id=to, device_id_type=MESH)

    edge = jnp.zeros((12, total_layers, 1, 128), F32)
    for v in (v0, v1, v2, v3):
        v[:, :, 7:8, :] = edge
        v[:, :, 40:41, :] = edge
    has_below = slab > 0
    has_above = slab < slabs - 1

    @pl.when(slab == 0)
    def _():
        v0[:, 0:LOW, 8:40, :] = jnp.zeros((12, LOW, 32, 128), F32)
        lcg[0:2] = jnp.zeros((2, 32, 128), F32)
        recs[0] = jnp.zeros((1, 128), jnp.int32)
        data[0] = jnp.zeros((12, 128), F32)

    @pl.when(slab == slabs - 1)
    def _():
        v0[:, own_hi:total_layers, 8:40, :] = jnp.zeros((12, HIGH, 32, 128), F32)
        lcg[2:5] = jnp.zeros((3, 32, 128), F32)
        recs[2] = jnp.zeros((1, 128), jnp.int32)
        data[2] = jnp.zeros((12, 128), F32)

    lanes = lax.broadcasted_iota(jnp.int32, (1, 128), 1)
    lane8 = lax.broadcasted_iota(jnp.int32, (8, 128), 1)
    last8 = lane8 == 127

    def in_lanes(sums):
        row = jnp.zeros((1, 128), F32)
        for n, s in enumerate(sums):
            one = jnp.sum(s, axis=0, keepdims=True)
            row = row + jnp.where(lanes == n, jnp.sum(one, axis=1, keepdims=True), 0.0)
        return row

    def pick(row, n):
        return jnp.sum(jnp.where(lanes == n, row, 0.0), axis=1, keepdims=True)

    for n in (1, 2):
        loads[n].wait()
    omega = omega_ref[0]
    kap[own_lo:own_hi] = omega * jnp.exp(logc[...])
    loads[0].wait()

    def weigh(l, acc):
        acc = list(acc)
        across = jnp.where(l == own_hi - 1, 0.0, layers / (layers - 1.0)).astype(F32)
        beyond = jnp.where(l == own_hi - 1, l, l + 1)
        for r in range(4):
            y = 8 + 8 * r
            coupling = kap[l, 8 * r : 8 * r + 8, :]
            acc[6] = acc[6] + coupling
            for pol in range(2):
                square = product = None
                for p in range(6 * pol, 6 * pol + 6):
                    here = v0[p, l, y : y + 8, :]
                    more = jnp.where(last8, 0.0, pltpu.roll(here, 127, 1))
                    more = more + v0[p, l, y + 1 : y + 9, :]
                    more = more + across * v0[p, beyond, y : y + 8, :]
                    sq, pr = here * here, here * more
                    square = sq if square is None else square + sq
                    product = pr if product is None else product + pr
                acc[3 * pol] = acc[3 * pol] + square
                acc[3 * pol + 1] = acc[3 * pol + 1] + product
                acc[3 * pol + 2] = acc[3 * pol + 2] + coupling * square
        return tuple(acc)

    weights = lax.fori_loop(own_lo, own_hi, weigh, (jnp.zeros((8, 128), F32),) * 7)

    def slab_start(n, row):
        allred[n, slab] = row
        copies = [
            remote(
                allred.at[n, slab],
                allred.at[n, slab],
                ar_send.at[n, d],
                ar_recv.at[n, slab],
                (freq, (slab + d) % slabs),
            )
            for d in range(1, slabs)
        ]
        for c in copies:
            c.start()
        return copies

    def slab_finish(n):
        for d in range(1, slabs):
            other = (slab + d) % slabs
            remote(
                allred.at[n, other],
                allred.at[n, other],
                ar_send.at[n, d],
                ar_recv.at[n, other],
                (freq, other),
            ).wait_recv()
        total = allred[n, 0]
        for j in range(1, slabs):
            total = total + allred[n, j]
        return total

    weights = in_lanes(weights)
    for n in range(3, len(loads)):
        loads[n].wait()
    pl.semaphore_wait(barrier, len(greeted))
    sent = slab_start(0, weights)

    rows = pl.ds(8, 32)
    below_to = (freq, lax.max(slab - 1, 0))
    above_to = (freq, lax.min(slab + 1, slabs - 1))
    upward = [
        (recs.at[1], recs.at[0]),
        (logc.at[pl.ds(layers - 2, 2)], lcg.at[pl.ds(0, 2)]),
    ]
    downward = [
        (recs.at[1], recs.at[2]),
        (logc.at[pl.ds(0, 3)], lcg.at[pl.ds(2, 3)]),
    ]
    for k in range(HIGH):
        if k < LOW:
            upward.append(
                (v0.at[:, own_hi - 1 - k, rows, :], v0.at[:, own_lo - 1 - k, rows, :])
            )
        downward.append((v0.at[:, own_lo + k, rows, :], v0.at[:, own_hi + k, rows, :]))
    ups = [
        remote(s, d, near_send.at[0, n], near_recv.at[0, n], above_to)
        for n, (s, d) in enumerate(upward)
    ]
    downs = [
        remote(s, d, near_send.at[1, n], near_recv.at[1, n], below_to)
        for n, (s, d) in enumerate(downward)
    ]

    @pl.when(has_above)
    def _():
        for c in ups:
            c.start()

    @pl.when(has_below)
    def _():
        for c in downs:
            c.start()

    for l in range(layers):
        prior_pair[half, 0, l : l + 1, :] = pg[l]
        prior_pair[half, 1, l : l + 1, :] = pd[l]
    prior_copy = remote(
        prior_pair.at[half], prior_pair.at[half], pair_send.at[0], pair_recv.at[0], partner
    )
    prior_copy.start()

    def arrived(n):
        if n < len(ups):

            @pl.when(has_below)
            def _():
                ups[n].wait_recv()

        @pl.when(has_above)
        def _():
            downs[n].wait_recv()

    lane = lax.broadcasted_iota(jnp.int32, (32, 128), 1)
    first_lane, last_lane = lane == 0, lane == 127
    alive_low = jnp.where(slab == 0, 0.0, 1.0).astype(F32)
    alive_high = jnp.where(slab == slabs - 1, 0.0, 1.0).astype(F32)

    def step(theta, src, dst, l, mask=None):
        def around(p):
            here = src[p, l, 8:40, :]
            total = src[p, l - 1, 8:40, :] + src[p, l + 1, 8:40, :]
            total = total + (src[p, l, 7:39, :] + src[p, l, 9:41, :])
            left = jnp.where(first_lane, 0.0, pltpu.roll(here, 1, 1))
            right = jnp.where(last_lane, 0.0, pltpu.roll(here, 127, 1))
            return here, total + (left + right)

        for pol in range(2):
            shift_re, shift_im = theta[pol]
            coupling = kap[l] + shift_im
            for comp in range(3):
                p = pol * 6 + comp
                re, around_re = around(p)
                im, around_im = around(p + 3)
                if shift_re is not None:
                    around_re = around_re - shift_re * re
                    around_im = around_im - shift_re * im
                new_re = around_re + coupling * im
                new_im = around_im - coupling * re
                if mask is not None:
                    new_re, new_im = mask * new_re, mask * new_im
                dst[p, l, 8:40, :] = new_re
                dst[p + 3, l, 8:40, :] = new_im

    def sweep(theta, src, dst, lo, hi, mask=None):
        def body(l, carry):
            step(theta, src, dst, l, mask)
            return carry

        lax.fori_loop(lo, hi, body, 0)

    def both(theta, src, dst, low, high, ghost):
        def body(n, carry):
            mask = jnp.where(n == 0, alive_low, alive_high) if ghost else None
            step(theta, src, dst, low + n * (high - low), mask)
            return carry

        lax.fori_loop(0, 2, body, 0)

    def moment_sums(theta):
        v_list = (v0, v1, v2, v3)
        sums = []
        for pol in range(2):
            shift_re, shift_im = theta[pol]

            def body(l, acc):
                acc = list(acc)

                def add(k, value):
                    acc[k] = acc[k] + value

                for r in range(4):
                    y = 8 + 8 * r
                    coupling = kap[l, 8 * r : 8 * r + 8, :] + shift_im
                    for comp in range(3):
                        p = pol * 6 + comp
                        vs = [(v[p, l, y : y + 8, :], v[p + 3, l, y : y + 8, :]) for v in v_list]
                        for k in range(4):
                            re, im = vs[k]
                            add(4 * k, (re - im) * (re + im))
                            add(4 * k + 1, re * im)
                        halves = []
                        for q in (p, p + 3):
                            here = v3[q, l, y : y + 8, :]
                            right = jnp.where(last8, 0.0, pltpu.roll(here, 127, 1))
                            more = v3[q, l, y + 1 : y + 9, :] + right
                            halves.append(more + more)
                        re, im = vs[3]
                        if shift_re is not None:
                            halves = [halves[0] - shift_re * re, halves[1] - shift_re * im]
                        after = (halves[0] + coupling * im, halves[1] - coupling * re)
                        pairs = [(vs[0], vs[1]), (vs[1], vs[2]), (vs[2], vs[3]), (vs[3], after)]
                        for k, (u, w) in enumerate(pairs):
                            add(4 * k + 2, u[0] * w[0] - u[1] * w[1])
                            add(4 * k + 3, u[0] * w[1] + u[1] * w[0])
                return tuple(acc)

            zero = jnp.zeros((8, 128), F32)
            sums += list(lax.fori_loop(own_lo, own_hi, body, (zero,) * 16))
        return sums

    def layer_pair(l, acc):
        acc = list(acc)
        for pol in range(2):
            for comp in range(3):
                for r in range(4):
                    p, y = pol * 6 + comp, 8 + 8 * r
                    u = (v3[p, l, y : y + 8, :], v3[p + 3, l, y : y + 8, :])
                    w = (v3[p, l + 1, y : y + 8, :], v3[p + 3, l + 1, y : y + 8, :])
                    acc[2 * pol] = acc[2 * pol] + (u[0] * w[0] - u[1] * w[1])
                    acc[2 * pol + 1] = acc[2 * pol + 1] + (u[0] * w[1] + u[1] * w[0])
        return tuple(acc)

    def moment_row(sums, pairs):
        sums = list(sums)
        for pol in range(2):
            for part in range(2):
                at, more = 16 * pol + 14 + part, pairs[2 * pol + part]
                sums[at] = sums[at] + (more + more)
        return in_lanes(sums)

    no_pairs = (jnp.zeros((8, 128), F32),) * 4

    def solve_coefficients(row, theta):
        found = []
        for pol in range(2):
            moments = []
            for k in range(8):
                re = pick(row, 16 * pol + 2 * k) * 6.0**-k
                im = pick(row, 16 * pol + 2 * k + 1) * 6.0**-k
                if k % 2 == 0:
                    im = im + im
                moments.append((re, im))
            most = None
            for m in moments:
                size = jnp.maximum(jnp.abs(m[0]), jnp.abs(m[1]))
                most = size if most is None else jnp.maximum(most, size)
            scale = 1.0 / most
            moments = [(m[0] * scale, m[1] * scale) for m in moments]
            found.append(coefficients(moments, theta[pol]))
        return found

    def combined(coefs, pol, comp, l, y):
        p = pol * 6 + comp
        re = im = None
        for (cr, ci), v in zip(coefs[pol], (v0, v1, v2, v3)):
            a, b = v[p, l, y : y + 8, :], v[p + 3, l, y : y + 8, :]
            tr, ti = cr * a - ci * b, cr * b + ci * a
            re, im = (tr, ti) if re is None else (re + tr, im + ti)
        return re, im

    weights = slab_finish(0)
    theta = []
    for pol in range(2):
        square = pick(weights, 3 * pol)
        theta.append(
            (
                2.0 * pick(weights, 3 * pol + 1) / square,
                -pick(weights, 3 * pol + 2) / square,
            )
        )
    mean_coupling = pick(weights, 6) / float(slabs * wide * 128)
    sweep(theta, v0, v1, own_lo + 1, own_hi - 1)
    step(theta, v1, v2, own_lo + 2)
    arrived(0)
    arrived(1)
    kap[1:3] = omega * jnp.exp(lcg[0:2])
    kap[own_hi : own_hi + 3] = omega * jnp.exp(lcg[2:5])
    arrived(2)
    both(theta, v0, v1, own_lo, own_hi - 1, False)
    both(theta, v1, v2, own_lo + 1, own_hi - 2, False)
    step(theta, v2, v3, own_lo + 2)
    arrived(3)
    both(theta, v0, v1, own_lo - 1, own_hi, True)
    both(theta, v1, v2, own_lo, own_hi - 1, False)
    both(theta, v2, v3, own_lo + 1, own_hi - 2, False)
    arrived(4)
    both(theta, v0, v1, own_lo - 2, own_hi + 1, True)
    both(theta, v1, v2, own_lo - 1, own_hi, True)
    both(theta, v2, v3, own_lo, own_hi - 1, False)
    sums = moment_sums(theta)
    pairs = lax.fori_loop(own_lo, own_hi - 1, layer_pair, no_pairs)
    arrived(5)
    step(theta, v0, v1, own_hi + 2, alive_high)
    step(theta, v1, v2, own_hi + 1, alive_high)
    step(theta, v2, v3, own_hi, alive_high)
    pairs = layer_pair(own_hi - 1, pairs)
    sent += slab_start(1, moment_row(sums, pairs))
    row = slab_finish(1)
    coefs = solve_coefficients(row, theta)

    def write_field(l, carry):
        for pol in range(2):
            for comp in range(3):
                for r in range(4):
                    re, im = combined(coefs, pol, comp, l, 8 + 8 * r)
                    field[pol * 6 + comp, l - own_lo, 8 * r : 8 * r + 8, :] = re
                    field[pol * 6 + 3 + comp, l - own_lo, 8 * r : 8 * r + 8, :] = im
        return carry

    lax.fori_loop(own_lo, own_hi, write_field, 0)

    def onehots(n):
        where = recs[n]
        column = lax.broadcasted_iota(jnp.int32, (128, 128), 0) == where % 128
        return where // 128, column.astype(F32).astype(BF16)

    line_of, column = onehots(1)
    taller = jnp.concatenate([column] * 3, axis=0)
    at_row = lax.broadcasted_iota(jnp.int32, (wide, 128), 0) == line_of
    for pol in range(2):
        for ri in range(2):
            for comp in range(3):
                p = pol * 6 + ri * 3 + comp
                plane = field[p].reshape(wide, 128)
                parts = jnp.concatenate(split3(plane), axis=1)
                seen = jnp.dot(parts, taller, preferred_element_type=F32)
                value = jnp.sum(jnp.where(at_row, seen, 0.0), axis=0, keepdims=True)
                misfit = value - obs[pol, comp, ri : ri + 1, :]
                weight = wt[comp, pol : pol + 1, :]
                weighted = weight * weight * misfit
                data[1, p : p + 1, :] = weighted if ri == 0 else -weighted

    data_up = remote(data.at[1], data.at[0], data_send.at[0], data_recv.at[0], above_to)
    data_down = remote(data.at[1], data.at[2], data_send.at[1], data_recv.at[1], below_to)

    @pl.when(has_above)
    def _():
        data_up.start()
        for c in ups:
            c.wait_send()

    @pl.when(has_below)
    def _():
        data_down.start()
        for c in downs:
            c.wait_send()

    prior_copy.wait()
    prior_all[place] = prior_pair[...]
    fan = [
        remote(
            prior_pair,
            prior_all.at[place],
            fan_send.at[0, d],
            fan_recv.at[0, place],
            (base + (place + d) % positions, slab),
        )
        for d in range(1, positions)
    ]
    for c in fan:
        c.start()

    def scatter(n, first_row, count, layer_at):
        line_of, column = onehots(n)
        wider = jnp.concatenate([column] * 3, axis=1)
        rows_here = lax.broadcasted_iota(jnp.int32, (32 * count, 128), 0) + first_row
        hit = rows_here == line_of
        for p in range(12):
            parts = split3(data[n, p : p + 1, :])
            spread = [jnp.where(hit, part.astype(F32), 0.0).astype(BF16) for part in parts]
            placed = lax.dot_general(
                jnp.concatenate(spread, axis=1),
                wider,
                (((1,), (1,)), ((), ())),
                preferred_element_type=F32,
            )
            v0[p, layer_at : layer_at + count, 8:40, :] = placed.reshape(count, 32, 128)

    behind = [(None, -mean_coupling)] * 2
    scatter(1, 0, layers, own_lo)
    sweep(behind, v0, v1, own_lo + 1, own_hi - 1)
    step(behind, v1, v2, own_lo + 2)

    @pl.when(has_below)
    def _():
        data_up.wait_recv()

    @pl.when(has_above)
    def _():
        data_down.wait_recv()

    scatter(0, 32 * (layers - LOW), LOW, 0)
    scatter(2, 0, HIGH, own_hi)
    both(behind, v0, v1, own_lo, own_hi - 1, False)
    sweep(behind, v0, v1, own_lo - 2, own_lo, alive_low)
    sweep(behind, v0, v1, own_hi, own_hi + 3, alive_high)
    both(behind, v1, v2, own_lo + 1, own_hi - 2, False)
    both(behind, v1, v2, own_lo, own_hi - 1, False)
    step(behind, v1, v2, own_lo - 1, alive_low)
    sweep(behind, v1, v2, own_hi, own_hi + 2, alive_high)
    sweep(behind, v2, v3, own_lo, own_hi)
    step(behind, v2, v3, own_hi, alive_high)
    sums = moment_sums(behind)
    pairs = lax.fori_loop(own_lo, own_hi, layer_pair, no_pairs)
    sent += slab_start(2, moment_row(sums, pairs))
    row = slab_finish(2)
    coefs = solve_coefficients(row, [(jnp.zeros_like(mean_coupling), -mean_coupling)] * 2)

    def write_grad(l, carry):
        for r in range(4):
            total = None
            for pol in range(2):
                for comp in range(3):
                    re, im = combined(coefs, pol, comp, l, 8 + 8 * r)
                    f_re = field[pol * 6 + comp, l - own_lo, 8 * r : 8 * r + 8, :]
                    f_im = field[pol * 6 + 3 + comp, l - own_lo, 8 * r : 8 * r + 8, :]
                    term = re * f_im + im * f_re
                    total = term if total is None else total + term
            at = pl.multiple_of((l - own_lo) * 32 + 8 * r, 8)
            grad[pl.ds(at, 8), :] = kap[l, 8 * r : 8 * r + 8, :] * total
        return carry

    lax.fori_loop(own_lo, own_hi, write_grad, 0)

    for j in range(positions):
        grad_src[j] = grad[chunk * j : chunk * (j + 1), :]
    grad_in[place] = grad_src[place]
    spread = []
    for d in range(1, positions):
        j = (place + d) % positions
        spread.append(
            remote(
                grad_src.at[j],
                grad_in.at[place],
                fan_send.at[1, d],
                fan_recv.at[1, place],
                (base + j, slab),
            )
        )
    for c in spread:
        c.start()

    def gathered(n, ref):
        for d in range(1, positions):
            j = (place + d) % positions
            remote(
                ref.at[j], ref.at[j], fan_send.at[n, d], fan_recv.at[n, j], (base + j, slab)
            ).wait_recv()

    gathered(0, prior_all)
    for y in range(2 * positions):
        for w in range(2):
            for l in range(layers):
                prior[w, 32 * l + y : 32 * l + y + 1, :] = prior_all[
                    y % positions, y // positions, w, l : l + 1, :
                ]
    old_grad, old_dir = prior[0], prior[1]

    def folded(x):
        total = x[0:8]
        for n in range(1, wide // 8):
            total = total + x[8 * n : 8 * n + 8]
        return total

    prior_sums = [folded(old_grad * old_grad), folded(old_dir * old_dir)]

    gathered(1, grad_in)
    partial = grad_in[0]
    for j in range(1, positions):
        partial = partial + grad_in[j]
    grad_pair[half] = partial
    pair_copy = remote(
        grad_pair.at[half], grad_pair.at[half], pair_send.at[1], pair_recv.at[1], partner
    )
    pair_copy.start()
    pair_copy.wait_recv()
    grad_all[place] = grad_pair[0] + grad_pair[1]
    share = []
    for d in range(1, positions):
        to = (base + (place + d) % positions, slab)
        share.append(
            remote(
                grad_all.at[place], grad_all.at[place], fan_send.at[2, d], fan_recv.at[2, place], to
            )
        )
    for c in share:
        c.start()
    gathered(2, grad_all)
    for j in range(positions):
        whole[chunk * j : chunk * (j + 1), :] = grad_all[j]

    g = whole[...]
    sums = [folded(g * g), folded(g * old_grad), folded(g * old_dir)] + prior_sums
    ends[slab] = in_lanes(sums)
    closing = []
    for away, other in [(0, 1 - core)] + [(a, c) for a in (1, -1, 2) for c in range(cores)]:
        n = len(closing)
        to = on_line(away, other)
        source = on_line(-away, other)[1]
        closing.append(
            (
                remote(ends.at[slab], ends.at[slab], end_send.at[n], end_recv.at[slab], to),
                remote(ends.at[source], ends.at[source], end_send.at[n], end_recv.at[source], to),
            )
        )
    for c, _ in closing:
        c.start()
    for _, c in closing:
        c.wait_recv()
    row = ends[0]
    for j in range(1, slabs):
        row = row + ends[j]
    gg, gq, gd, qq, dd = [pick(row, n) for n in range(5)]
    cells = float(slabs * wide * 128)
    mean_square = gg / cells + epsilon
    inverse = 1.0 / jnp.sqrt(mean_square)
    beta = (gg / mean_square - gq * inverse) / (qq + epsilon)
    squared = gg / mean_square - 2.0 * beta * (gd * inverse) + beta * beta * dd
    norm = 1.0 / jnp.sqrt(jnp.maximum(squared, 0.0) / cells + epsilon)
    whole[...] = (-inverse * norm) * whole[...] + (beta * norm) * prior[1]
    for l in range(layers):
        dir_ref[l] = whole[pl.ds(32 * l + freq, 1), :]
    trial_ref[...] = logc[...] + step_ref[0] * whole[...].reshape(layers, 32, 128)

    @pl.when(has_above)
    def _():
        data_up.wait_send()

    @pl.when(has_below)
    def _():
        data_down.wait_send()

    pair_copy.wait_send()
    for c in sent + fan + spread + share + [c for c, _ in closing]:
        c.wait_send()


def per_device(
    slabs,
    positions,
    log_conductivity,
    omega,
    sources,
    receivers,
    observed,
    data_weight,
    prior_gradient,
    prior_direction,
    step_length,
):
    layers = log_conductivity.shape[0]
    total = LOW + layers + HIGH
    wide = layers * 32
    chunk = (positions, wide // positions, 128)
    hbm = pl.BlockSpec(memory_space=pltpu.HBM)
    vmem = pl.BlockSpec(memory_space=pltpu.VMEM)
    state = pltpu.VMEM((12, total, 48, 128), F32)
    return pl.pallas_call(
        functools.partial(kernel, layers, slabs, positions),
        out_shape=(
            jax.ShapeDtypeStruct(prior_gradient.shape, F32),
            jax.ShapeDtypeStruct(log_conductivity.shape, F32),
        ),
        in_specs=[hbm] * 9,
        out_specs=(vmem, vmem),
        scratch_shapes=[
            pltpu.SMEM((1,), F32),
            pltpu.SMEM((1,), F32),
            pltpu.VMEM((layers, 32, 128), F32),
            pltpu.VMEM((2, 3, 2, 128), F32),
            pltpu.VMEM((3, 2, 128), F32),
            pltpu.VMEM((layers, 1, 128), F32),
            pltpu.VMEM((layers, 1, 128), F32),
            state,
            state,
            state,
            state,
            pltpu.VMEM((12, layers, 32, 128), F32),
            pltpu.VMEM((total, 32, 128), F32),
            pltpu.VMEM((5, 32, 128), F32),
            pltpu.VMEM((3, 1, 128), jnp.int32),
            pltpu.VMEM((3, 12, 128), F32),
            pltpu.VMEM((3, slabs, 1, 128), F32),
            pltpu.VMEM((slabs, 1, 128), F32),
            pltpu.VMEM((2, 2, layers, 128), F32),
            pltpu.VMEM((positions, 2, 2, layers, 128), F32),
            pltpu.VMEM((2, wide, 128), F32),
            pltpu.VMEM((wide, 128), F32),
            pltpu.VMEM(chunk, F32),
            pltpu.VMEM(chunk, F32),
            pltpu.VMEM((2,) + chunk[1:], F32),
            pltpu.VMEM(chunk, F32),
            pltpu.VMEM((wide, 128), F32),
            pltpu.SemaphoreType.DMA((9,)),
            pltpu.SemaphoreType.DMA((2, 6)),
            pltpu.SemaphoreType.DMA((2, 6)),
            pltpu.SemaphoreType.DMA((2,)),
            pltpu.SemaphoreType.DMA((2,)),
            pltpu.SemaphoreType.DMA((3, slabs)),
            pltpu.SemaphoreType.DMA((3, slabs)),
            pltpu.SemaphoreType.DMA((slabs,)),
            pltpu.SemaphoreType.DMA((slabs,)),
            pltpu.SemaphoreType.DMA((2,)),
            pltpu.SemaphoreType.DMA((2,)),
            pltpu.SemaphoreType.DMA((3, positions)),
            pltpu.SemaphoreType.DMA((3, positions)),
        ],
        compiler_params=pltpu.CompilerParams(
            collective_id=0, has_side_effects=True, vmem_limit_bytes=60 * 1024 * 1024
        ),
        name="inversion_step",
    )(
        omega,
        step_length,
        log_conductivity,
        sources.reshape(12, layers, 32, 128),
        receivers.reshape(1, 128),
        observed[0].transpose(0, 2, 1, 3),
        data_weight[0].transpose(1, 0, 2),
        prior_gradient,
        prior_direction,
    )


def solution(mesh):
    slabs = mesh.shape["slab"]
    positions = mesh.shape["freq"] // 2
    in_specs = (
        P("slab", None, None),
        P("freq"),
        P("freq", None, None, None, "slab", None, None),
        P("slab"),
        P("freq", None, None, None, "slab"),
        P("freq", None, None, "slab"),
        P("slab", "freq", None),
        P("slab", "freq", None),
        P(),
    )
    out_specs = (P("slab", "freq", None), P("slab", None, None))
    return jax.shard_map(
        functools.partial(per_device, slabs, positions),
        mesh=mesh,
        in_specs=in_specs,
        out_specs=out_specs,
        check_vma=False,
    )
```

```python
import functools

import jax
import jax.numpy as jnp
from jax import lax
from jax.experimental import pallas as pl
from jax.experimental.pallas import tpu as pltpu
from jax.sharding import PartitionSpec as P


MESH = pl.DeviceIdType.MESH
epsilon = 1e-06
F32 = jnp.float32
BF16 = jnp.bfloat16
LOW = 3
HIGH = 4


def cmul(a, b):
    return a[0] * b[0] - a[1] * b[1], a[0] * b[1] + a[1] * b[0]


def cadd(a, b):
    return a[0] + b[0], a[1] + b[1]


def csub(a, b):
    return a[0] - b[0], a[1] - b[1]


def cdiv(a, b):
    modulus = b[0] * b[0] + b[1] * b[1]
    return (a[0] * b[0] + a[1] * b[1]) / modulus, (a[1] * b[0] - a[0] * b[1]) / modulus


def square_poly(p):
    out = [None] * (2 * len(p) - 1)
    for i in range(len(p)):
        for j in range(i, len(p)):
            term = cmul(p[i], p[j])
            if j > i:
                term = (term[0] + term[0], term[1] + term[1])
            out[i + j] = term if out[i + j] is None else cadd(out[i + j], term)
    return out


def against(poly, moments):
    total = None
    for c, m in zip(poly, moments):
        term = cmul(c, m)
        total = term if total is None else cadd(total, term)
    return total


def coefficients(moments, theta):
    one = (jnp.ones_like(moments[0][0]), jnp.zeros_like(moments[0][0]))
    shift = (one[0] - theta[0] * (1.0 / 6.0), -theta[1] * (1.0 / 6.0))
    steps = [csub(cmul(shift, a), b) for a, b in zip(moments, moments[1:])]
    residual, direction, rho = [one], [one], moments[0]
    solution = []
    for iteration in range(4):
        alpha = cdiv(rho, against(square_poly(direction), steps))
        moved = [cmul(alpha, c) for c in direction]
        solution = [cadd(a, b) for a, b in zip(solution, moved)] + moved[len(solution) :]
        if iteration < 3:
            kept = [csub(r, cmul(shift, m)) for r, m in zip(residual, moved)]
            residual = [kept[0]]
            residual += [cadd(kept[k + 1], moved[k]) for k in range(len(moved) - 1)]
            residual += [moved[-1]]
            rho_next = against(square_poly(residual), moments)
            beta = cdiv(rho_next, rho)
            direction = [
                cadd(residual[k], cmul(beta, direction[k])) for k in range(len(direction))
            ] + [residual[-1]]
            rho = rho_next
    return [(c[0] * 6.0 ** -(k + 1), c[1] * 6.0 ** -(k + 1)) for k, c in enumerate(solution)]


def split3(x):
    high = x.astype(BF16)
    rest = x - high.astype(F32)
    mid = rest.astype(BF16)
    low = (rest - mid.astype(F32)).astype(BF16)
    return high, mid, low


def kernel(
    layers,
    slabs,
    positions,
    omega_ref,
    step_ref,
    logc_in,
    src_in,
    rec_in,
    obs_in,
    wt_in,
    pg_in,
    pd_in,
    dir_ref,
    trial_ref,
    logc,
    obs,
    wt,
    pg,
    pd,
    v0,
    v1,
    v2,
    v3,
    u0,
    u1,
    u2,
    u3,
    kap,
    lcg,
    recs,
    wanted,
    weights_at,
    seen,
    data,
    row_hot,
    column_hot,
    products,
    allred,
    ends,
    prior_pair,
    prior_all,
    prior,
    grad,
    grad_src,
    grad_in,
    grad_pair,
    grad_all,
    whole,
    load_sem,
    near_send,
    near_recv,
    seen_send,
    seen_recv,
    ar_send,
    ar_recv,
    end_send,
    end_recv,
    pair_send,
    pair_recv,
    fan_send,
    fan_recv,
):
    freq = lax.axis_index("freq")
    slab = lax.axis_index("slab")
    half = freq // positions
    place = freq % positions
    base = half * positions
    cores = 2
    chips = slabs // cores
    line = 2 * chips
    high = half * chips + slab // cores
    core = slab % cores
    own_lo, own_hi = LOW, LOW + layers
    total_layers = LOW + layers + HIGH
    wide = 32 * layers
    chunk = wide // positions

    def remote(src, dst, send, recv, to):
        return pltpu.make_async_remote_copy(
            src_ref=src, dst_ref=dst, send_sem=send, recv_sem=recv, device_id=to, device_id_type=MESH
        )

    def on_line(away, other_core):
        z = (high + away) % line
        return (z // chips) * positions + place, (z % chips) * cores + other_core

    partner = on_line(chips, core)

    loads = [
        pltpu.make_async_copy(s, d, load_sem.at[n])
        for n, (s, d) in enumerate(
            (
                (src_in, v0.at[:, pl.ds(own_lo, layers), pl.ds(8, 32), :]),
                (logc_in, logc),
                (rec_in, recs.at[1]),
                (pg_in, pg),
                (pd_in, pd),
                (obs_in, obs),
                (wt_in, wt),
            )
        )
    ]
    for c in loads:
        c.start()
    barrier = pltpu.get_barrier_semaphore()
    greeted = [on_line(0, 1 - core)]
    greeted += [on_line(away, c) for away in range(1, line) for c in range(cores)]
    greeted += [(base + (place + d) % positions, slab) for d in range(1, positions)]
    for to in greeted:
        pl.semaphore_signal(barrier, inc=1, device_id=to, device_id_type=MESH)

    edge = jnp.zeros((12, total_layers, 1, 128), F32)

    def clear_edges(arrays):
        for v in arrays:
            v[:, :, 7:8, :] = edge
            v[:, :, 40:41, :] = edge

    clear_edges((v0, v1, v2, v3))
    has_below = slab > 0
    has_above = slab < slabs - 1

    @pl.when(slab == 0)
    def _():
        v0[:, 0:LOW, 8:40, :] = jnp.zeros((12, LOW, 32, 128), F32)
        lcg[0:2] = jnp.zeros((2, 32, 128), F32)
        recs[0] = jnp.zeros((1, 128), jnp.int32)
        wanted[0] = jnp.zeros((2, 2, 3, 128), F32)
        weights_at[0] = jnp.zeros((2, 3, 128), F32)
        seen[0] = jnp.zeros((4, 2, 2, 3, 128), F32)

    @pl.when(slab == slabs - 1)
    def _():
        v0[:, own_hi:total_layers, 8:40, :] = jnp.zeros((12, HIGH, 32, 128), F32)
        lcg[2:5] = jnp.zeros((3, 32, 128), F32)
        recs[2] = jnp.zeros((1, 128), jnp.int32)
        wanted[2] = jnp.zeros((2, 2, 3, 128), F32)
        weights_at[2] = jnp.zeros((2, 3, 128), F32)
        seen[2] = jnp.zeros((4, 2, 2, 3, 128), F32)

    lanes = lax.broadcasted_iota(jnp.int32, (1, 128), 1)
    lane8 = lax.broadcasted_iota(jnp.int32, (8, 128), 1)
    last8 = lane8 == 127

    def in_lanes(sums):
        row = jnp.zeros((1, 128), F32)
        for n, s in enumerate(sums):
            one = jnp.sum(s, axis=0, keepdims=True)
            row = row + jnp.where(lanes == n, jnp.sum(one, axis=1, keepdims=True), 0.0)
        return row

    def pick(row, n):
        return jnp.sum(jnp.where(lanes == n, row, 0.0), axis=1, keepdims=True)

    loads[1].wait()
    omega = omega_ref[0]
    kap[own_lo:own_hi] = omega * jnp.exp(logc[...])
    loads[0].wait()

    def weigh(l, acc):
        acc = list(acc)
        across = jnp.where(l == own_hi - 1, 0.0, layers / (layers - 1.0)).astype(F32)
        beyond = jnp.where(l == own_hi - 1, l, l + 1)
        for r in range(4):
            y = 8 + 8 * r
            coupling = kap[l, 8 * r : 8 * r + 8, :]
            acc[6] = acc[6] + coupling
            for pol in range(2):
                square = product = None
                for p in range(6 * pol, 6 * pol + 6):
                    here = v0[p, l, y : y + 8, :]
                    more = jnp.where(last8, 0.0, pltpu.roll(here, 127, 1))
                    more = more + v0[p, l, y + 1 : y + 9, :]
                    more = more + across * v0[p, beyond, y : y + 8, :]
                    sq, pr = here * here, here * more
                    square = sq if square is None else square + sq
                    product = pr if product is None else product + pr
                acc[3 * pol] = acc[3 * pol] + square
                acc[3 * pol + 1] = acc[3 * pol + 1] + product
                acc[3 * pol + 2] = acc[3 * pol + 2] + coupling * square
        return tuple(acc)

    weights = lax.fori_loop(own_lo, own_hi, weigh, (jnp.zeros((8, 128), F32),) * 7)

    def slab_start(n, row):
        allred[n, slab] = row
        copies = [
            remote(
                allred.at[n, slab],
                allred.at[n, slab],
                ar_send.at[n, d],
                ar_recv.at[n, slab],
                (freq, (slab + d) % slabs),
            )
            for d in range(1, slabs)
        ]
        for c in copies:
            c.start()
        return copies

    def slab_finish(n):
        for d in range(1, slabs):
            other = (slab + d) % slabs
            remote(
                allred.at[n, other],
                allred.at[n, other],
                ar_send.at[n, d],
                ar_recv.at[n, other],
                (freq, other),
            ).wait_recv()
        total = allred[n, 0]
        for j in range(1, slabs):
            total = total + allred[n, j]
        return total

    weights = in_lanes(weights)
    for n in range(2, len(loads)):
        loads[n].wait()
    for pol in range(2):
        for comp in range(3):
            at = slice(comp, comp + 1)
            weights_at[1, pol, at, :] = wt[comp, pol : pol + 1, :]
            for ri in range(2):
                wanted[1, pol, ri, at, :] = obs[pol, comp, ri : ri + 1, :]
    pl.semaphore_wait(barrier, len(greeted))
    sent = slab_start(0, weights)

    rows = pl.ds(8, 32)
    below_to = (freq, lax.max(slab - 1, 0))
    above_to = (freq, lax.min(slab + 1, slabs - 1))
    upward = [
        (recs.at[1], recs.at[0]),
        (logc.at[pl.ds(layers - 2, 2)], lcg.at[pl.ds(0, 2)]),
    ]
    downward = [
        (recs.at[1], recs.at[2]),
        (logc.at[pl.ds(0, 3)], lcg.at[pl.ds(2, 3)]),
    ]
    for k in range(HIGH):
        if k < LOW:
            upward.append(
                (v0.at[:, own_hi - 1 - k, rows, :], v0.at[:, own_lo - 1 - k, rows, :])
            )
        downward.append((v0.at[:, own_lo + k, rows, :], v0.at[:, own_hi + k, rows, :]))
    for ref in (wanted, weights_at):
        upward.append((ref.at[1], ref.at[0]))
        downward.append((ref.at[1], ref.at[2]))
    ups = [
        remote(s, d, near_send.at[0, n], near_recv.at[0, n], above_to)
        for n, (s, d) in enumerate(upward)
    ]
    downs = [
        remote(s, d, near_send.at[1, n], near_recv.at[1, n], below_to)
        for n, (s, d) in enumerate(downward)
    ]

    @pl.when(has_above)
    def _():
        for c in ups:
            c.start()

    @pl.when(has_below)
    def _():
        for c in downs:
            c.start()

    for l in range(layers):
        prior_pair[half, 0, l : l + 1, :] = pg[l]
        prior_pair[half, 1, l : l + 1, :] = pd[l]
    prior_copy = remote(
        prior_pair.at[half], prior_pair.at[half], pair_send.at[0], pair_recv.at[0], partner
    )
    prior_copy.start()

    def arrived(from_below, from_above):
        @pl.when(has_below)
        def _():
            for n in from_below:
                ups[n].wait_recv()

        @pl.when(has_above)
        def _():
            for n in from_above:
                downs[n].wait_recv()

    lane = lax.broadcasted_iota(jnp.int32, (32, 128), 1)
    first_lane, last_lane = lane == 0, lane == 127
    alive_low = jnp.where(slab == 0, 0.0, 1.0).astype(F32)
    alive_high = jnp.where(slab == slabs - 1, 0.0, 1.0).astype(F32)

    def step(theta, src, dst, l, mask=None):
        def around(p):
            here = src[p, l, 8:40, :]
            total = src[p, l - 1, 8:40, :] + src[p, l + 1, 8:40, :]
            total = total + (src[p, l, 7:39, :] + src[p, l, 9:41, :])
            left = jnp.where(first_lane, 0.0, pltpu.roll(here, 1, 1))
            right = jnp.where(last_lane, 0.0, pltpu.roll(here, 127, 1))
            return here, total + (left + right)

        for pol in range(2):
            shift_re, shift_im = theta[pol]
            coupling = kap[l] + shift_im
            for comp in range(3):
                p = pol * 6 + comp
                re, around_re = around(p)
                im, around_im = around(p + 3)
                if shift_re is not None:
                    around_re = around_re - shift_re * re
                    around_im = around_im - shift_re * im
                new_re = around_re + coupling * im
                new_im = around_im - coupling * re
                if mask is not None:
                    new_re, new_im = mask * new_re, mask * new_im
                dst[p, l, 8:40, :] = new_re
                dst[p + 3, l, 8:40, :] = new_im

    def sweep(theta, src, dst, lo, hi, ghosts):
        def body(n, carry):
            for l in (lo + 2 * n, lo + 2 * n + 1):
                mask = None
                if ghosts:
                    mask = jnp.where(l < own_lo, alive_low, 1.0)
                    mask = jnp.where(l >= own_hi, alive_high, mask)
                step(theta, src, dst, l, mask)
            return carry

        lax.fori_loop(0, (hi - lo) // 2, body, 0)
        if (hi - lo) % 2:
            step(theta, src, dst, hi - 1)

    def both(theta, src, dst, low, high, ghost):
        def body(n, carry):
            mask = jnp.where(n == 0, alive_low, alive_high) if ghost else None
            step(theta, src, dst, low + n * (high - low), mask)
            return carry

        lax.fori_loop(0, 2, body, 0)

    def moment_sums(theta, v_list):
        v3 = v_list[3]
        sums = []
        for pol in range(2):
            shift_re, shift_im = theta[pol]

            def body(l, acc):
                acc = list(acc)

                def add(k, value):
                    acc[k] = acc[k] + value

                for r in range(4):
                    y = 8 + 8 * r
                    coupling = kap[l, 8 * r : 8 * r + 8, :] + shift_im
                    for comp in range(3):
                        p = pol * 6 + comp
                        vs = [(v[p, l, y : y + 8, :], v[p + 3, l, y : y + 8, :]) for v in v_list]
                        for k in range(4):
                            re, im = vs[k]
                            add(4 * k, (re - im) * (re + im))
                            add(4 * k + 1, re * im)
                        halves = []
                        for q in (p, p + 3):
                            here = v3[q, l, y : y + 8, :]
                            right = jnp.where(last8, 0.0, pltpu.roll(here, 127, 1))
                            more = v3[q, l, y + 1 : y + 9, :] + right
                            halves.append(more + more)
                        re, im = vs[3]
                        if shift_re is not None:
                            halves = [halves[0] - shift_re * re, halves[1] - shift_re * im]
                        after = (halves[0] + coupling * im, halves[1] - coupling * re)
                        pairs = [(vs[0], vs[1]), (vs[1], vs[2]), (vs[2], vs[3]), (vs[3], after)]
                        for k, (u, w) in enumerate(pairs):
                            add(4 * k + 2, u[0] * w[0] - u[1] * w[1])
                            add(4 * k + 3, u[0] * w[1] + u[1] * w[0])
                return tuple(acc)

            zero = jnp.zeros((8, 128), F32)
            sums += list(lax.fori_loop(own_lo, own_hi, body, (zero,) * 16))
        return sums

    def layer_pair(v3, l, acc):
        acc = list(acc)
        for pol in range(2):
            for comp in range(3):
                for r in range(4):
                    p, y = pol * 6 + comp, 8 + 8 * r
                    u = (v3[p, l, y : y + 8, :], v3[p + 3, l, y : y + 8, :])
                    w = (v3[p, l + 1, y : y + 8, :], v3[p + 3, l + 1, y : y + 8, :])
                    acc[2 * pol] = acc[2 * pol] + (u[0] * w[0] - u[1] * w[1])
                    acc[2 * pol + 1] = acc[2 * pol + 1] + (u[0] * w[1] + u[1] * w[0])
        return tuple(acc)

    def pair_row(pairs):
        row = in_lanes([p + p for p in pairs])
        spread = jnp.zeros((1, 128), F32)
        for n, at in enumerate((14, 15, 30, 31)):
            spread = spread + jnp.where(lanes == at, pick(row, n), 0.0)
        return spread

    no_pairs = (jnp.zeros((8, 128), F32),) * 4

    def solve_coefficients(row, theta):
        found = []
        for pol in range(2):
            moments = []
            for k in range(8):
                re = pick(row, 16 * pol + 2 * k) * 6.0**-k
                im = pick(row, 16 * pol + 2 * k + 1) * 6.0**-k
                if k % 2 == 0:
                    im = im + im
                moments.append((re, im))
            most = None
            for m in moments:
                size = jnp.maximum(jnp.abs(m[0]), jnp.abs(m[1]))
                most = size if most is None else jnp.maximum(most, size)
            scale = 1.0 / most
            moments = [(m[0] * scale, m[1] * scale) for m in moments]
            found.append(coefficients(moments, theta[pol]))
        return found

    def combined(coefs, v_list, pol, comp, l, y):
        p = pol * 6 + comp
        re = im = None
        for (cr, ci), v in zip(coefs[pol], v_list):
            a, b = v[p, l, y : y + 8, :], v[p + 3, l, y : y + 8, :]
            tr, ti = cr * a - ci * b, cr * b + ci * a
            re, im = (tr, ti) if re is None else (re + tr, im + ti)
        return re, im

    line_of, lane_of = recs[1] // 128, recs[1] % 128
    column = lax.broadcasted_iota(jnp.int32, (128, 128), 0) == lane_of
    column_hot[1] = column.astype(F32).astype(BF16)
    at_row = lax.broadcasted_iota(jnp.int32, (wide, 128), 0) == line_of

    def look(j, v):
        def body(pol, carry):
            column = column_hot[1]
            taller = jnp.concatenate([column] * 3, axis=0)
            for ri in range(2):
                for comp in range(3):
                    plane = v[pol * 6 + ri * 3 + comp, own_lo:own_hi, 8:40, :].reshape(wide, 128)
                    parts = jnp.concatenate(split3(plane), axis=1)
                    found = jnp.dot(parts, taller, preferred_element_type=F32)
                    value = jnp.sum(jnp.where(at_row, found, 0.0), axis=0, keepdims=True)
                    seen[1, j, pol, ri, comp : comp + 1, :] = value
            return carry

        lax.fori_loop(0, 2, body, 0)

    forward, backward = (v0, v1, v2, v3), (u0, u1, u2, u3)
    clear_edges(backward)
    look(0, v0)
    weights = slab_finish(0)
    theta = []
    for pol in range(2):
        square = pick(weights, 3 * pol)
        theta.append(
            (
                2.0 * pick(weights, 3 * pol + 1) / square,
                -pick(weights, 3 * pol + 2) / square,
            )
        )
    mean_coupling = pick(weights, 6) / float(slabs * wide * 128)
    sweep(theta, v0, v1, own_lo + 1, own_hi - 1, False)
    step(theta, v1, v2, own_lo + 2)
    arrived((0, 1), (0, 1))
    kap[1:3] = omega * jnp.exp(lcg[0:2])
    kap[own_hi : own_hi + 3] = omega * jnp.exp(lcg[2:5])
    arrived((2,), (2,))
    both(theta, v0, v1, own_lo, own_hi - 1, False)
    both(theta, v1, v2, own_lo + 1, own_hi - 2, False)
    step(theta, v2, v3, own_lo + 2)
    look(1, v1)
    arrived((3,), (3,))
    both(theta, v0, v1, own_lo - 1, own_hi, True)
    both(theta, v1, v2, own_lo, own_hi - 1, False)
    both(theta, v2, v3, own_lo + 1, own_hi - 2, False)
    look(2, v2)
    arrived((4,), (4,))
    both(theta, v0, v1, own_lo - 2, own_hi + 1, True)
    both(theta, v1, v2, own_lo - 1, own_hi, True)
    both(theta, v2, v3, own_lo, own_hi - 1, False)
    pair = functools.partial(layer_pair, v3)
    row = in_lanes(moment_sums(theta, forward))
    pairs = lax.fori_loop(own_lo, own_hi - 1, pair, no_pairs)
    arrived((), (5,))
    step(theta, v0, v1, own_hi + 2, alive_high)
    step(theta, v1, v2, own_hi + 1, alive_high)
    step(theta, v2, v3, own_hi, alive_high)
    sent += slab_start(1, row + pair_row(pair(own_hi - 1, pairs)))

    look(3, v3)
    seen_up = remote(seen.at[1], seen.at[0], seen_send.at[0], seen_recv.at[0], above_to)
    seen_down = remote(seen.at[1], seen.at[2], seen_send.at[1], seen_recv.at[1], below_to)

    @pl.when(has_above)
    def _():
        seen_up.start()

    @pl.when(has_below)
    def _():
        seen_down.start()

    spots = ((0, 32 * (layers - LOW), LOW, 0), (1, 0, layers, own_lo), (2, 0, HIGH, own_hi))
    for n, first_row, count, layer_at in spots:
        line_of, lane_of = recs[n] // 128, recs[n] % 128
        if n != 1:
            column = lax.broadcasted_iota(jnp.int32, (128, 128), 0) == lane_of
            column_hot[n] = column.astype(F32).astype(BF16)
        rows_here = lax.broadcasted_iota(jnp.int32, (32 * count, 128), 0) + first_row
        hit = (rows_here == line_of).astype(F32).astype(BF16)
        row_hot[32 * layer_at : 32 * (layer_at + count), :] = hit

    prior_copy.wait()
    prior_all[place] = prior_pair[...]
    fan = [
        remote(
            prior_pair,
            prior_all.at[place],
            fan_send.at[0, d],
            fan_recv.at[0, place],
            (base + (place + d) % positions, slab),
        )
        for d in range(1, positions)
    ]
    for c in fan:
        c.start()

    arrived((5, 6), (6, 7))

    @pl.when(has_below)
    def _():
        seen_up.wait_recv()

    @pl.when(has_above)
    def _():
        seen_down.wait_recv()

    row = slab_finish(1)
    coefs = solve_coefficients(row, theta)

    for n in range(3):
        for pol in range(2):
            re = im = None
            for j, (cr, ci) in enumerate(coefs[pol]):
                a, b = seen[n, j, pol, 0], seen[n, j, pol, 1]
                tr, ti = cr * a - ci * b, cr * b + ci * a
                re, im = (tr, ti) if re is None else (re + tr, im + ti)
            weight = weights_at[n, pol]
            square = weight * weight
            data[n, pol, 0] = square * (re - wanted[n, pol, 0])
            data[n, pol, 1] = -square * (im - wanted[n, pol, 1])

    for n, first_row, count, layer_at in spots:

        def place_sources(pol, carry, n=n, count=count, layer_at=layer_at):
            hit = row_hot[32 * layer_at : 32 * (layer_at + count), :]
            wider = jnp.concatenate([column_hot[n]] * 3, axis=1)
            for ri in range(2):
                for comp in range(3):
                    parts = split3(data[n, pol, ri, comp : comp + 1, :])
                    placed = lax.dot_general(
                        jnp.concatenate([hit * part for part in parts], axis=1),
                        wider,
                        (((1,), (1,)), ((), ())),
                        preferred_element_type=F32,
                    )
                    p = pol * 6 + ri * 3 + comp
                    u0[p, layer_at : layer_at + count, 8:40, :] = placed.reshape(count, 32, 128)
            return carry

        lax.fori_loop(0, 2, place_sources, 0)

    behind = [(None, -mean_coupling)] * 2
    sweep(behind, u0, u1, own_lo - 2, own_hi + 3, True)
    sweep(behind, u1, u2, own_lo - 1, own_hi + 2, True)
    sweep(behind, u2, u3, own_lo, own_hi + 1, True)
    sums = moment_sums(behind, backward)
    pairs = lax.fori_loop(own_lo, own_hi, functools.partial(layer_pair, u3), no_pairs)
    for pol in range(2):
        for part in range(2):
            at, more = 16 * pol + 14 + part, pairs[2 * pol + part]
            sums[at] = sums[at] + (more + more)
    sent += slab_start(2, in_lanes(sums))

    def multiply(l, carry):
        for r in range(4):
            y = 8 + 8 * r
            at = pl.multiple_of((l - own_lo) * 32 + 8 * r, 8)
            coupling = kap[l, 8 * r : 8 * r + 8, :]
            for pol in range(2):
                fields = [combined(coefs, forward, pol, comp, l, y) for comp in range(3)]
                for j, u in enumerate(backward):
                    first = second = None
                    for comp in range(3):
                        p = pol * 6 + comp
                        re, im = u[p, l, y : y + 8, :], u[p + 3, l, y : y + 8, :]
                        f_re, f_im = fields[comp]
                        x, z = re * f_im + im * f_re, re * f_re - im * f_im
                        first, second = (x, z) if first is None else (first + x, second + z)
                    products[pol, j, 0, pl.ds(at, 8), :] = coupling * first
                    products[pol, j, 1, pl.ds(at, 8), :] = coupling * second
        return carry

    lax.fori_loop(own_lo, own_hi, multiply, 0)
    row = slab_finish(2)
    coefs = solve_coefficients(row, [(jnp.zeros_like(mean_coupling), -mean_coupling)] * 2)
    for n in range(wide // 8):
        total = None
        for pol in range(2):
            for j in range(4):
                for part in range(2):
                    term = coefs[pol][j][part] * products[pol, j, part, 8 * n : 8 * n + 8, :]
                    total = term if total is None else total + term
        grad[8 * n : 8 * n + 8, :] = total

    for j in range(positions):
        grad_src[j] = grad[chunk * j : chunk * (j + 1), :]
    grad_in[place] = grad_src[place]
    spread = []
    for d in range(1, positions):
        j = (place + d) % positions
        spread.append(
            remote(
                grad_src.at[j],
                grad_in.at[place],
                fan_send.at[1, d],
                fan_recv.at[1, place],
                (base + j, slab),
            )
        )
    for c in spread:
        c.start()

    def gathered(n, ref):
        for d in range(1, positions):
            j = (place + d) % positions
            remote(
                ref.at[j], ref.at[j], fan_send.at[n, d], fan_recv.at[n, j], (base + j, slab)
            ).wait_recv()

    gathered(0, prior_all)
    for y in range(2 * positions):
        for w in range(2):
            for l in range(layers):
                prior[w, 32 * l + y : 32 * l + y + 1, :] = prior_all[
                    y % positions, y // positions, w, l : l + 1, :
                ]
    old_grad, old_dir = prior[0], prior[1]

    def folded(x):
        total = x[0:8]
        for n in range(1, wide // 8):
            total = total + x[8 * n : 8 * n + 8]
        return total

    prior_sums = [folded(old_grad * old_grad), folded(old_dir * old_dir)]

    gathered(1, grad_in)
    partial = grad_in[0]
    for j in range(1, positions):
        partial = partial + grad_in[j]
    grad_pair[half] = partial
    pair_copy = remote(
        grad_pair.at[half], grad_pair.at[half], pair_send.at[1], pair_recv.at[1], partner
    )
    pair_copy.start()
    pair_copy.wait_recv()
    grad_all[place] = grad_pair[0] + grad_pair[1]
    share = []
    for d in range(1, positions):
        to = (base + (place + d) % positions, slab)
        share.append(
            remote(
                grad_all.at[place], grad_all.at[place], fan_send.at[2, d], fan_recv.at[2, place], to
            )
        )
    for c in share:
        c.start()
    gathered(2, grad_all)
    for j in range(positions):
        whole[chunk * j : chunk * (j + 1), :] = grad_all[j]

    g = whole[...]
    sums = [folded(g * g), folded(g * old_grad), folded(g * old_dir)] + prior_sums
    ends[slab] = in_lanes(sums)
    closing = []
    for away, other in [(0, 1 - core)] + [(a, c) for a in (1, -1, 2) for c in range(cores)]:
        n = len(closing)
        to = on_line(away, other)
        source = on_line(-away, other)[1]
        closing.append(
            (
                remote(ends.at[slab], ends.at[slab], end_send.at[n], end_recv.at[slab], to),
                remote(ends.at[source], ends.at[source], end_send.at[n], end_recv.at[source], to),
            )
        )
    for c, _ in closing:
        c.start()
    for _, c in closing:
        c.wait_recv()
    row = ends[0]
    for j in range(1, slabs):
        row = row + ends[j]
    gg, gq, gd, qq, dd = [pick(row, n) for n in range(5)]
    cells = float(slabs * wide * 128)
    mean_square = gg / cells + epsilon
    inverse = 1.0 / jnp.sqrt(mean_square)
    beta = (gg / mean_square - gq * inverse) / (qq + epsilon)
    squared = gg / mean_square - 2.0 * beta * (gd * inverse) + beta * beta * dd
    norm = 1.0 / jnp.sqrt(jnp.maximum(squared, 0.0) / cells + epsilon)
    whole[...] = (-inverse * norm) * whole[...] + (beta * norm) * prior[1]
    for l in range(layers):
        dir_ref[l] = whole[pl.ds(32 * l + freq, 1), :]
    trial_ref[...] = logc[...] + step_ref[0] * whole[...].reshape(layers, 32, 128)

    @pl.when(has_above)
    def _():
        for c in ups + [seen_up]:
            c.wait_send()

    @pl.when(has_below)
    def _():
        for c in downs + [seen_down]:
            c.wait_send()

    pair_copy.wait_send()
    for c in sent + fan + spread + share + [c for c, _ in closing]:
        c.wait_send()


def per_device(
    slabs,
    positions,
    log_conductivity,
    omega,
    sources,
    receivers,
    observed,
    data_weight,
    prior_gradient,
    prior_direction,
    step_length,
):
    layers = log_conductivity.shape[0]
    total = LOW + layers + HIGH
    wide = layers * 32
    chunk = (positions, wide // positions, 128)
    hbm = pl.BlockSpec(memory_space=pltpu.HBM)
    smem = pl.BlockSpec(memory_space=pltpu.SMEM)
    vmem = pl.BlockSpec(memory_space=pltpu.VMEM)
    state = pltpu.VMEM((12, total, 48, 128), F32)
    return pl.pallas_call(
        functools.partial(kernel, layers, slabs, positions),
        out_shape=(
            jax.ShapeDtypeStruct(prior_gradient.shape, F32),
            jax.ShapeDtypeStruct(log_conductivity.shape, F32),
        ),
        in_specs=[smem] * 2 + [hbm] * 7,
        out_specs=(vmem, vmem),
        scratch_shapes=[
            pltpu.VMEM((layers, 32, 128), F32),
            pltpu.VMEM((2, 3, 2, 128), F32),
            pltpu.VMEM((3, 2, 128), F32),
            pltpu.VMEM((layers, 1, 128), F32),
            pltpu.VMEM((layers, 1, 128), F32),
            *[state] * 8,
            pltpu.VMEM((total, 32, 128), F32),
            pltpu.VMEM((5, 32, 128), F32),
            pltpu.VMEM((3, 1, 128), jnp.int32),
            pltpu.VMEM((3, 2, 2, 3, 128), F32),
            pltpu.VMEM((3, 2, 3, 128), F32),
            pltpu.VMEM((3, 4, 2, 2, 3, 128), F32),
            pltpu.VMEM((3, 2, 2, 3, 128), F32),
            pltpu.VMEM((32 * total, 128), BF16),
            pltpu.VMEM((3, 128, 128), BF16),
            pltpu.VMEM((2, 4, 2, wide, 128), F32),
            pltpu.VMEM((3, slabs, 1, 128), F32),
            pltpu.VMEM((slabs, 1, 128), F32),
            pltpu.VMEM((2, 2, layers, 128), F32),
            pltpu.VMEM((positions, 2, 2, layers, 128), F32),
            pltpu.VMEM((2, wide, 128), F32),
            pltpu.VMEM((wide, 128), F32),
            pltpu.VMEM(chunk, F32),
            pltpu.VMEM(chunk, F32),
            pltpu.VMEM((2,) + chunk[1:], F32),
            pltpu.VMEM(chunk, F32),
            pltpu.VMEM((wide, 128), F32),
            pltpu.SemaphoreType.DMA((7,)),
            pltpu.SemaphoreType.DMA((2, 8)),
            pltpu.SemaphoreType.DMA((2, 8)),
            pltpu.SemaphoreType.DMA((2,)),
            pltpu.SemaphoreType.DMA((2,)),
            pltpu.SemaphoreType.DMA((3, slabs)),
            pltpu.SemaphoreType.DMA((3, slabs)),
            pltpu.SemaphoreType.DMA((slabs,)),
            pltpu.SemaphoreType.DMA((slabs,)),
            pltpu.SemaphoreType.DMA((2,)),
            pltpu.SemaphoreType.DMA((2,)),
            pltpu.SemaphoreType.DMA((3, positions)),
            pltpu.SemaphoreType.DMA((3, positions)),
        ],
        compiler_params=pltpu.CompilerParams(
            collective_id=0, has_side_effects=True, vmem_limit_bytes=48 * 1024 * 1024
        ),
        name="inversion_step",
    )(
        omega,
        step_length,
        *(
            pltpu.with_memory_space_constraint(x, pltpu.HBM)
            for x in (
                log_conductivity,
                sources.reshape(12, layers, 32, 128),
                receivers.reshape(1, 128),
                observed[0].transpose(0, 2, 1, 3),
                data_weight[0].transpose(1, 0, 2),
                prior_gradient,
                prior_direction,
            )
        ),
    )


def solution(mesh):
    slabs = mesh.shape["slab"]
    positions = mesh.shape["freq"] // 2
    in_specs = (
        P("slab", None, None),
        P("freq"),
        P("freq", None, None, None, "slab", None, None),
        P("slab"),
        P("freq", None, None, None, "slab"),
        P("freq", None, None, "slab"),
        P("slab", "freq", None),
        P("slab", "freq", None),
        P(),
    )
    out_specs = (P("slab", "freq", None), P("slab", None, None))
    return jax.shard_map(
        functools.partial(per_device, slabs, positions),
        mesh=mesh,
        in_specs=in_specs,
        out_specs=out_specs,
        check_vma=False,
    )
```

```python
import functools

import jax
import jax.numpy as jnp
from jax import lax
from jax.experimental import pallas as pl
from jax.experimental.pallas import tpu as pltpu
from jax.sharding import PartitionSpec as P


MESH = pl.DeviceIdType.MESH
epsilon = 1e-06
F32 = jnp.float32
BF16 = jnp.bfloat16
LOW = 3
HIGH = 4


def cmul(a, b):
    return a[0] * b[0] - a[1] * b[1], a[0] * b[1] + a[1] * b[0]


def cadd(a, b):
    return a[0] + b[0], a[1] + b[1]


def csub(a, b):
    return a[0] - b[0], a[1] - b[1]


def cdiv(a, b):
    modulus = b[0] * b[0] + b[1] * b[1]
    return (a[0] * b[0] + a[1] * b[1]) / modulus, (a[1] * b[0] - a[0] * b[1]) / modulus


def square_poly(p):
    out = [None] * (2 * len(p) - 1)
    for i in range(len(p)):
        for j in range(i, len(p)):
            term = cmul(p[i], p[j])
            if j > i:
                term = (term[0] + term[0], term[1] + term[1])
            out[i + j] = term if out[i + j] is None else cadd(out[i + j], term)
    return out


def against(poly, moments):
    total = None
    for c, m in zip(poly, moments):
        term = cmul(c, m)
        total = term if total is None else cadd(total, term)
    return total


def coefficients(moments, theta):
    one = (jnp.ones_like(moments[0][0]), jnp.zeros_like(moments[0][0]))
    shift = (one[0] - theta[0] * (1.0 / 6.0), -theta[1] * (1.0 / 6.0))
    steps = [csub(cmul(shift, a), b) for a, b in zip(moments, moments[1:])]
    residual, direction, rho = [one], [one], moments[0]
    solution = []
    for iteration in range(4):
        alpha = cdiv(rho, against(square_poly(direction), steps))
        moved = [cmul(alpha, c) for c in direction]
        solution = [cadd(a, b) for a, b in zip(solution, moved)] + moved[len(solution) :]
        if iteration < 3:
            kept = [csub(r, cmul(shift, m)) for r, m in zip(residual, moved)]
            residual = [kept[0]]
            residual += [cadd(kept[k + 1], moved[k]) for k in range(len(moved) - 1)]
            residual += [moved[-1]]
            rho_next = against(square_poly(residual), moments)
            beta = cdiv(rho_next, rho)
            direction = [
                cadd(residual[k], cmul(beta, direction[k])) for k in range(len(direction))
            ] + [residual[-1]]
            rho = rho_next
    return [(c[0] * 6.0 ** -(k + 1), c[1] * 6.0 ** -(k + 1)) for k, c in enumerate(solution)]


def split3(x):
    high = x.astype(BF16)
    rest = x - high.astype(F32)
    mid = rest.astype(BF16)
    low = (rest - mid.astype(F32)).astype(BF16)
    return high, mid, low


def kernel(
    layers,
    slabs,
    positions,
    omega_ref,
    step_ref,
    logc_in,
    src_in,
    rec_in,
    obs_in,
    wt_in,
    pg_in,
    pd_in,
    dir_ref,
    trial_ref,
    logc,
    obs,
    wt,
    pg,
    pd,
    v0,
    v1,
    v2,
    v3,
    u0,
    u1,
    u2,
    u3,
    kap,
    lcg,
    recs,
    wanted,
    weights_at,
    seen,
    data,
    row_hot,
    column_hot,
    products,
    allred,
    ends,
    prior_pair,
    prior_all,
    prior,
    grad,
    grad_src,
    grad_in,
    grad_pair,
    grad_all,
    whole,
    load_sem,
    near_send,
    near_recv,
    seen_send,
    seen_recv,
    ar_send,
    ar_recv,
    end_send,
    end_recv,
    pair_send,
    pair_recv,
    fan_send,
    fan_recv,
):
    freq = lax.axis_index("freq")
    slab = lax.axis_index("slab")
    half = freq // positions
    place = freq % positions
    base = half * positions
    cores = 2
    chips = slabs // cores
    line = 2 * chips
    high = half * chips + slab // cores
    core = slab % cores
    own_lo, own_hi = LOW, LOW + layers
    total_layers = LOW + layers + HIGH
    wide = 32 * layers
    chunk = wide // positions

    def remote(src, dst, send, recv, to):
        return pltpu.make_async_remote_copy(
            src_ref=src, dst_ref=dst, send_sem=send, recv_sem=recv, device_id=to, device_id_type=MESH
        )

    def on_line(away, other_core):
        z = (high + away) % line
        return (z // chips) * positions + place, (z % chips) * cores + other_core

    partner = on_line(chips, core)
    side = 4
    offsets = [(dy, dx) for dy in range(positions // side) for dx in range(side)][1:]
    offsets.sort(key=lambda o: -sum(min(k, side - k) for k in o))

    def in_plane(d):
        dy, dx = offsets[d]
        y = (place // side + dy) % (positions // side)
        return y * side + (place % side + dx) % side

    loads = [
        pltpu.make_async_copy(s, d, load_sem.at[n])
        for n, (s, d) in enumerate(
            (
                (src_in, v0.at[:, pl.ds(own_lo, layers), pl.ds(8, 32), :]),
                (logc_in, logc),
                (rec_in, recs.at[1]),
                (pg_in, pg),
                (pd_in, pd),
                (obs_in, obs),
                (wt_in, wt),
            )
        )
    ]
    for c in loads:
        c.start()
    barrier = pltpu.get_barrier_semaphore()
    greeted = [on_line(0, 1 - core)]
    greeted += [on_line(away, c) for away in range(1, line) for c in range(cores)]
    greeted += [(base + in_plane(d), slab) for d in range(positions - 1)]
    for to in greeted:
        pl.semaphore_signal(barrier, inc=1, device_id=to, device_id_type=MESH)

    edge = jnp.zeros((12, total_layers, 1, 128), F32)

    def clear_edges(arrays):
        for v in arrays:
            v[:, :, 7:8, :] = edge
            v[:, :, 40:41, :] = edge

    clear_edges((v0, v1, v2, v3))
    has_below = slab > 0
    has_above = slab < slabs - 1

    @pl.when(slab == 0)
    def _():
        v0[:, 0:LOW, 8:40, :] = jnp.zeros((12, LOW, 32, 128), F32)
        lcg[0:2] = jnp.zeros((2, 32, 128), F32)
        recs[0] = jnp.zeros((1, 128), jnp.int32)
        wanted[0] = jnp.zeros((2, 2, 3, 128), F32)
        weights_at[0] = jnp.zeros((2, 3, 128), F32)
        seen[0] = jnp.zeros((4, 2, 2, 3, 128), F32)

    @pl.when(slab == slabs - 1)
    def _():
        v0[:, own_hi:total_layers, 8:40, :] = jnp.zeros((12, HIGH, 32, 128), F32)
        lcg[2:5] = jnp.zeros((3, 32, 128), F32)
        recs[2] = jnp.zeros((1, 128), jnp.int32)
        wanted[2] = jnp.zeros((2, 2, 3, 128), F32)
        weights_at[2] = jnp.zeros((2, 3, 128), F32)
        seen[2] = jnp.zeros((4, 2, 2, 3, 128), F32)

    lanes = lax.broadcasted_iota(jnp.int32, (1, 128), 1)
    lane8 = lax.broadcasted_iota(jnp.int32, (8, 128), 1)
    last8 = lane8 == 127

    def in_lanes(sums):
        row = jnp.zeros((1, 128), F32)
        for n, s in enumerate(sums):
            one = jnp.sum(s, axis=0, keepdims=True)
            row = row + jnp.where(lanes == n, jnp.sum(one, axis=1, keepdims=True), 0.0)
        return row

    def pick(row, n):
        return jnp.sum(jnp.where(lanes == n, row, 0.0), axis=1, keepdims=True)

    loads[1].wait()
    omega = omega_ref[0]
    kap[own_lo:own_hi] = omega * jnp.exp(logc[...])
    loads[0].wait()

    def weigh(l, acc):
        acc = list(acc)
        across = jnp.where(l == own_hi - 1, 0.0, layers / (layers - 1.0)).astype(F32)
        beyond = jnp.where(l == own_hi - 1, l, l + 1)
        for r in range(4):
            y = 8 + 8 * r
            coupling = kap[l, 8 * r : 8 * r + 8, :]
            acc[6] = acc[6] + coupling
            for pol in range(2):
                square = product = None
                for p in range(6 * pol, 6 * pol + 6):
                    here = v0[p, l, y : y + 8, :]
                    more = jnp.where(last8, 0.0, pltpu.roll(here, 127, 1))
                    more = more + v0[p, l, y + 1 : y + 9, :]
                    more = more + across * v0[p, beyond, y : y + 8, :]
                    sq, pr = here * here, here * more
                    square = sq if square is None else square + sq
                    product = pr if product is None else product + pr
                acc[3 * pol] = acc[3 * pol] + square
                acc[3 * pol + 1] = acc[3 * pol + 1] + product
                acc[3 * pol + 2] = acc[3 * pol + 2] + coupling * square
        return tuple(acc)

    weights = lax.fori_loop(own_lo, own_hi, weigh, (jnp.zeros((8, 128), F32),) * 7)

    def slab_start(n, row):
        allred[n, slab] = row
        copies = []
        for d in range(slabs - 1):
            down, up = slabs - 1 - d, d
            down = jnp.where(down > slab, down, down - 1)
            up = jnp.where(up < slab, up, up + 1)
            copies.append(
                remote(
                    allred.at[n, slab],
                    allred.at[n, slab],
                    ar_send.at[n, d],
                    ar_recv.at[n, slab],
                    (freq, jnp.where(slab < slabs // 2, down, up)),
                )
            )
        for c in copies:
            c.start()
        return copies

    def slab_finish(n):
        for d in range(1, slabs):
            other = (slab + d) % slabs
            remote(
                allred.at[n, other],
                allred.at[n, other],
                ar_send.at[n, d],
                ar_recv.at[n, other],
                (freq, other),
            ).wait_recv()
        total = allred[n, 0]
        for j in range(1, slabs):
            total = total + allred[n, j]
        return total

    weights = in_lanes(weights)
    for n in range(2, len(loads)):
        loads[n].wait()
    for pol in range(2):
        for comp in range(3):
            at = slice(comp, comp + 1)
            weights_at[1, pol, at, :] = wt[comp, pol : pol + 1, :]
            for ri in range(2):
                wanted[1, pol, ri, at, :] = obs[pol, comp, ri : ri + 1, :]
    pl.semaphore_wait(barrier, len(greeted))
    sent = slab_start(0, weights)

    rows = pl.ds(8, 32)
    below_to = (freq, lax.max(slab - 1, 0))
    above_to = (freq, lax.min(slab + 1, slabs - 1))
    upward = [
        (recs.at[1], recs.at[0]),
        (logc.at[pl.ds(layers - 2, 2)], lcg.at[pl.ds(0, 2)]),
    ]
    downward = [
        (recs.at[1], recs.at[2]),
        (logc.at[pl.ds(0, 3)], lcg.at[pl.ds(2, 3)]),
    ]
    for k in range(HIGH):
        if k < LOW:
            upward.append(
                (v0.at[:, own_hi - 1 - k, rows, :], v0.at[:, own_lo - 1 - k, rows, :])
            )
        downward.append((v0.at[:, own_lo + k, rows, :], v0.at[:, own_hi + k, rows, :]))
    for ref in (wanted, weights_at):
        upward.append((ref.at[1], ref.at[0]))
        downward.append((ref.at[1], ref.at[2]))
    ups = [
        remote(s, d, near_send.at[0, n], near_recv.at[0, n], above_to)
        for n, (s, d) in enumerate(upward)
    ]
    downs = [
        remote(s, d, near_send.at[1, n], near_recv.at[1, n], below_to)
        for n, (s, d) in enumerate(downward)
    ]

    @pl.when(has_above)
    def _():
        for c in ups:
            c.start()

    @pl.when(has_below)
    def _():
        for c in downs:
            c.start()

    for l in range(layers):
        prior_pair[half, 0, l : l + 1, :] = pg[l]
        prior_pair[half, 1, l : l + 1, :] = pd[l]
    prior_copy = remote(
        prior_pair.at[half], prior_pair.at[half], pair_send.at[0], pair_recv.at[0], partner
    )
    prior_copy.start()

    def arrived(from_below, from_above):
        @pl.when(has_below)
        def _():
            for n in from_below:
                ups[n].wait_recv()

        @pl.when(has_above)
        def _():
            for n in from_above:
                downs[n].wait_recv()

    lane = lax.broadcasted_iota(jnp.int32, (32, 128), 1)
    first_lane, last_lane = lane == 0, lane == 127
    alive_low = jnp.where(slab == 0, 0.0, 1.0).astype(F32)
    alive_high = jnp.where(slab == slabs - 1, 0.0, 1.0).astype(F32)

    def step(theta, src, dst, l, mask=None):
        def around(p):
            here = src[p, l, 8:40, :]
            total = src[p, l - 1, 8:40, :] + src[p, l + 1, 8:40, :]
            total = total + (src[p, l, 7:39, :] + src[p, l, 9:41, :])
            left = jnp.where(first_lane, 0.0, pltpu.roll(here, 1, 1))
            right = jnp.where(last_lane, 0.0, pltpu.roll(here, 127, 1))
            return here, total + (left + right)

        for pol in range(2):
            shift_re, shift_im = theta[pol]
            coupling = kap[l] + shift_im
            for comp in range(3):
                p = pol * 6 + comp
                re, around_re = around(p)
                im, around_im = around(p + 3)
                if shift_re is not None:
                    around_re = around_re - shift_re * re
                    around_im = around_im - shift_re * im
                new_re = around_re + coupling * im
                new_im = around_im - coupling * re
                if mask is not None:
                    new_re, new_im = mask * new_re, mask * new_im
                dst[p, l, 8:40, :] = new_re
                dst[p + 3, l, 8:40, :] = new_im

    def sweep(theta, src, dst, lo, hi, ghosts):
        def body(n, carry):
            for l in (lo + 2 * n, lo + 2 * n + 1):
                mask = None
                if ghosts:
                    mask = jnp.where(l < own_lo, alive_low, 1.0)
                    mask = jnp.where(l >= own_hi, alive_high, mask)
                step(theta, src, dst, l, mask)
            return carry

        lax.fori_loop(0, (hi - lo) // 2, body, 0)
        if (hi - lo) % 2:
            step(theta, src, dst, hi - 1)

    def both(theta, src, dst, low, high, ghost):
        def body(n, carry):
            mask = jnp.where(n == 0, alive_low, alive_high) if ghost else None
            step(theta, src, dst, low + n * (high - low), mask)
            return carry

        lax.fori_loop(0, 2, body, 0)

    def moment_sums(theta, v_list):
        v3 = v_list[3]
        sums = []
        for pol in range(2):
            shift_re, shift_im = theta[pol]

            def body(l, acc):
                acc = list(acc)

                def add(k, value):
                    acc[k] = acc[k] + value

                for r in range(4):
                    y = 8 + 8 * r
                    coupling = kap[l, 8 * r : 8 * r + 8, :] + shift_im
                    for comp in range(3):
                        p = pol * 6 + comp
                        vs = [(v[p, l, y : y + 8, :], v[p + 3, l, y : y + 8, :]) for v in v_list]
                        for k in range(4):
                            re, im = vs[k]
                            add(4 * k, (re - im) * (re + im))
                            add(4 * k + 1, re * im)
                        halves = []
                        for q in (p, p + 3):
                            here = v3[q, l, y : y + 8, :]
                            right = jnp.where(last8, 0.0, pltpu.roll(here, 127, 1))
                            more = v3[q, l, y + 1 : y + 9, :] + right
                            halves.append(more + more)
                        re, im = vs[3]
                        if shift_re is not None:
                            halves = [halves[0] - shift_re * re, halves[1] - shift_re * im]
                        after = (halves[0] + coupling * im, halves[1] - coupling * re)
                        pairs = [(vs[0], vs[1]), (vs[1], vs[2]), (vs[2], vs[3]), (vs[3], after)]
                        for k, (u, w) in enumerate(pairs):
                            add(4 * k + 2, u[0] * w[0] - u[1] * w[1])
                            add(4 * k + 3, u[0] * w[1] + u[1] * w[0])
                return tuple(acc)

            zero = jnp.zeros((8, 128), F32)
            sums += list(lax.fori_loop(own_lo, own_hi, body, (zero,) * 16))
        return sums

    def layer_pair(v3, l, acc):
        acc = list(acc)
        for pol in range(2):
            for comp in range(3):
                for r in range(4):
                    p, y = pol * 6 + comp, 8 + 8 * r
                    u = (v3[p, l, y : y + 8, :], v3[p + 3, l, y : y + 8, :])
                    w = (v3[p, l + 1, y : y + 8, :], v3[p + 3, l + 1, y : y + 8, :])
                    acc[2 * pol] = acc[2 * pol] + (u[0] * w[0] - u[1] * w[1])
                    acc[2 * pol + 1] = acc[2 * pol + 1] + (u[0] * w[1] + u[1] * w[0])
        return tuple(acc)

    def pair_row(pairs):
        row = in_lanes([p + p for p in pairs])
        spread = jnp.zeros((1, 128), F32)
        for n, at in enumerate((14, 15, 30, 31)):
            spread = spread + jnp.where(lanes == at, pick(row, n), 0.0)
        return spread

    no_pairs = (jnp.zeros((8, 128), F32),) * 4

    def solve_coefficients(row, theta):
        found = []
        for pol in range(2):
            moments = []
            for k in range(8):
                re = pick(row, 16 * pol + 2 * k) * 6.0**-k
                im = pick(row, 16 * pol + 2 * k + 1) * 6.0**-k
                if k % 2 == 0:
                    im = im + im
                moments.append((re, im))
            most = None
            for m in moments:
                size = jnp.maximum(jnp.abs(m[0]), jnp.abs(m[1]))
                most = size if most is None else jnp.maximum(most, size)
            scale = 1.0 / most
            moments = [(m[0] * scale, m[1] * scale) for m in moments]
            found.append(coefficients(moments, theta[pol]))
        return found

    def combined(coefs, v_list, pol, comp, l, y):
        p = pol * 6 + comp
        re = im = None
        for (cr, ci), v in zip(coefs[pol], v_list):
            a, b = v[p, l, y : y + 8, :], v[p + 3, l, y : y + 8, :]
            tr, ti = cr * a - ci * b, cr * b + ci * a
            re, im = (tr, ti) if re is None else (re + tr, im + ti)
        return re, im

    line_of, lane_of = recs[1] // 128, recs[1] % 128
    column = lax.broadcasted_iota(jnp.int32, (128, 128), 0) == lane_of
    column_hot[1] = column.astype(F32).astype(BF16)
    at_row = lax.broadcasted_iota(jnp.int32, (wide, 128), 0) == line_of

    def look(j, v):
        def body(pol, carry):
            column = column_hot[1]
            taller = jnp.concatenate([column] * 3, axis=0)
            for ri in range(2):
                for comp in range(3):
                    plane = v[pol * 6 + ri * 3 + comp, own_lo:own_hi, 8:40, :].reshape(wide, 128)
                    parts = jnp.concatenate(split3(plane), axis=1)
                    found = jnp.dot(parts, taller, preferred_element_type=F32)
                    value = jnp.sum(jnp.where(at_row, found, 0.0), axis=0, keepdims=True)
                    seen[1, j, pol, ri, comp : comp + 1, :] = value
            return carry

        lax.fori_loop(0, 2, body, 0)

    forward, backward = (v0, v1, v2, v3), (u0, u1, u2, u3)
    clear_edges(backward)
    look(0, v0)
    weights = slab_finish(0)
    theta = []
    for pol in range(2):
        square = pick(weights, 3 * pol)
        theta.append(
            (
                2.0 * pick(weights, 3 * pol + 1) / square,
                -pick(weights, 3 * pol + 2) / square,
            )
        )
    mean_coupling = pick(weights, 6) / float(slabs * wide * 128)
    sweep(theta, v0, v1, own_lo + 1, own_hi - 1, False)
    step(theta, v1, v2, own_lo + 2)
    arrived((0, 1), (0, 1))
    kap[1:3] = omega * jnp.exp(lcg[0:2])
    kap[own_hi : own_hi + 3] = omega * jnp.exp(lcg[2:5])
    arrived((2,), (2,))
    both(theta, v0, v1, own_lo, own_hi - 1, False)
    both(theta, v1, v2, own_lo + 1, own_hi - 2, False)
    step(theta, v2, v3, own_lo + 2)
    look(1, v1)
    arrived((3,), (3,))
    both(theta, v0, v1, own_lo - 1, own_hi, True)
    both(theta, v1, v2, own_lo, own_hi - 1, False)
    both(theta, v2, v3, own_lo + 1, own_hi - 2, False)
    look(2, v2)
    arrived((4,), (4,))
    both(theta, v0, v1, own_lo - 2, own_hi + 1, True)
    both(theta, v1, v2, own_lo - 1, own_hi, True)
    both(theta, v2, v3, own_lo, own_hi - 1, False)
    pair = functools.partial(layer_pair, v3)
    row = in_lanes(moment_sums(theta, forward))
    pairs = lax.fori_loop(own_lo, own_hi - 1, pair, no_pairs)
    arrived((), (5,))
    step(theta, v0, v1, own_hi + 2, alive_high)
    step(theta, v1, v2, own_hi + 1, alive_high)
    step(theta, v2, v3, own_hi, alive_high)
    sent += slab_start(1, row + pair_row(pair(own_hi - 1, pairs)))

    look(3, v3)
    seen_up = remote(seen.at[1], seen.at[0], seen_send.at[0], seen_recv.at[0], above_to)
    seen_down = remote(seen.at[1], seen.at[2], seen_send.at[1], seen_recv.at[1], below_to)

    @pl.when(has_above)
    def _():
        seen_up.start()

    @pl.when(has_below)
    def _():
        seen_down.start()

    spots = ((0, 32 * (layers - LOW), LOW, 0), (1, 0, layers, own_lo), (2, 0, HIGH, own_hi))
    for n, first_row, count, layer_at in spots:
        line_of, lane_of = recs[n] // 128, recs[n] % 128
        if n != 1:
            column = lax.broadcasted_iota(jnp.int32, (128, 128), 0) == lane_of
            column_hot[n] = column.astype(F32).astype(BF16)
        rows_here = lax.broadcasted_iota(jnp.int32, (32 * count, 128), 0) + first_row
        hit = (rows_here == line_of).astype(F32).astype(BF16)
        row_hot[32 * layer_at : 32 * (layer_at + count), :] = hit

    prior_copy.wait()
    prior_all[place] = prior_pair[...]
    fan = [
        remote(
            prior_pair,
            prior_all.at[place],
            fan_send.at[0, d],
            fan_recv.at[0, place],
            (base + in_plane(d), slab),
        )
        for d in range(positions - 1)
    ]
    for c in fan:
        c.start()

    arrived((5, 6), (6, 7))

    @pl.when(has_below)
    def _():
        seen_up.wait_recv()

    @pl.when(has_above)
    def _():
        seen_down.wait_recv()

    row = slab_finish(1)
    coefs = solve_coefficients(row, theta)

    for n in range(3):
        for pol in range(2):
            re = im = None
            for j, (cr, ci) in enumerate(coefs[pol]):
                a, b = seen[n, j, pol, 0], seen[n, j, pol, 1]
                tr, ti = cr * a - ci * b, cr * b + ci * a
                re, im = (tr, ti) if re is None else (re + tr, im + ti)
            weight = weights_at[n, pol]
            square = weight * weight
            data[n, pol, 0] = square * (re - wanted[n, pol, 0])
            data[n, pol, 1] = -square * (im - wanted[n, pol, 1])

    for n, first_row, count, layer_at in spots:

        def place_sources(pol, carry, n=n, count=count, layer_at=layer_at):
            hit = row_hot[32 * layer_at : 32 * (layer_at + count), :]
            wider = jnp.concatenate([column_hot[n]] * 3, axis=1)
            for ri in range(2):
                for comp in range(3):
                    parts = split3(data[n, pol, ri, comp : comp + 1, :])
                    placed = lax.dot_general(
                        jnp.concatenate([hit * part for part in parts], axis=1),
                        wider,
                        (((1,), (1,)), ((), ())),
                        preferred_element_type=F32,
                    )
                    p = pol * 6 + ri * 3 + comp
                    u0[p, layer_at : layer_at + count, 8:40, :] = placed.reshape(count, 32, 128)
            return carry

        lax.fori_loop(0, 2, place_sources, 0)

    behind = [(None, -mean_coupling)] * 2
    sweep(behind, u0, u1, own_lo - 2, own_hi + 3, True)
    sweep(behind, u1, u2, own_lo - 1, own_hi + 2, True)
    sweep(behind, u2, u3, own_lo, own_hi + 1, True)
    sums = moment_sums(behind, backward)
    pairs = lax.fori_loop(own_lo, own_hi, functools.partial(layer_pair, u3), no_pairs)
    for pol in range(2):
        for part in range(2):
            at, more = 16 * pol + 14 + part, pairs[2 * pol + part]
            sums[at] = sums[at] + (more + more)
    sent += slab_start(2, in_lanes(sums))

    def multiply(l, carry):
        for r in range(4):
            y = 8 + 8 * r
            at = pl.multiple_of((l - own_lo) * 32 + 8 * r, 8)
            coupling = kap[l, 8 * r : 8 * r + 8, :]
            for pol in range(2):
                fields = [combined(coefs, forward, pol, comp, l, y) for comp in range(3)]
                for j, u in enumerate(backward):
                    first = second = None
                    for comp in range(3):
                        p = pol * 6 + comp
                        re, im = u[p, l, y : y + 8, :], u[p + 3, l, y : y + 8, :]
                        f_re, f_im = fields[comp]
                        x, z = re * f_im + im * f_re, re * f_re - im * f_im
                        first, second = (x, z) if first is None else (first + x, second + z)
                    products[pol, j, 0, pl.ds(at, 8), :] = coupling * first
                    products[pol, j, 1, pl.ds(at, 8), :] = coupling * second
        return carry

    lax.fori_loop(own_lo, own_hi, multiply, 0)
    row = slab_finish(2)
    coefs = solve_coefficients(row, [(jnp.zeros_like(mean_coupling), -mean_coupling)] * 2)
    for n in range(wide // 8):
        total = None
        for pol in range(2):
            for j in range(4):
                for part in range(2):
                    term = coefs[pol][j][part] * products[pol, j, part, 8 * n : 8 * n + 8, :]
                    total = term if total is None else total + term
        grad[8 * n : 8 * n + 8, :] = total

    for j in range(positions):
        grad_src[j] = grad[chunk * j : chunk * (j + 1), :]
    grad_in[place] = grad_src[place]
    spread = []
    for d in range(positions - 1):
        j = in_plane(d)
        spread.append(
            remote(
                grad_src.at[j],
                grad_in.at[place],
                fan_send.at[1, d],
                fan_recv.at[1, place],
                (base + j, slab),
            )
        )
    for c in spread:
        c.start()

    def gathered(n, ref):
        for d in range(positions - 1):
            j = in_plane(d)
            remote(
                ref.at[j], ref.at[j], fan_send.at[n, d], fan_recv.at[n, j], (base + j, slab)
            ).wait_recv()

    gathered(0, prior_all)
    for y in range(2 * positions):
        for w in range(2):
            for l in range(layers):
                prior[w, 32 * l + y : 32 * l + y + 1, :] = prior_all[
                    y % positions, y // positions, w, l : l + 1, :
                ]
    old_grad, old_dir = prior[0], prior[1]

    def folded(x):
        total = x[0:8]
        for n in range(1, wide // 8):
            total = total + x[8 * n : 8 * n + 8]
        return total

    prior_sums = [folded(old_grad * old_grad), folded(old_dir * old_dir)]

    gathered(1, grad_in)
    partial = grad_in[0]
    for j in range(1, positions):
        partial = partial + grad_in[j]
    grad_pair[half] = partial
    pair_copy = remote(
        grad_pair.at[half], grad_pair.at[half], pair_send.at[1], pair_recv.at[1], partner
    )
    pair_copy.start()
    pair_copy.wait_recv()
    grad_all[place] = grad_pair[0] + grad_pair[1]
    share = []
    for d in range(positions - 1):
        to = (base + in_plane(d), slab)
        share.append(
            remote(
                grad_all.at[place], grad_all.at[place], fan_send.at[2, d], fan_recv.at[2, place], to
            )
        )
    for c in share:
        c.start()
    gathered(2, grad_all)
    for j in range(positions):
        whole[chunk * j : chunk * (j + 1), :] = grad_all[j]

    g = whole[...]
    sums = [folded(g * g), folded(g * old_grad), folded(g * old_dir)] + prior_sums
    ends[slab] = in_lanes(sums)
    closing = []
    for away, other in [(a, c) for a in (2, 1, -1) for c in range(cores)] + [(0, 1 - core)]:
        n = len(closing)
        to = on_line(away, other)
        source = on_line(-away, other)[1]
        closing.append(
            (
                remote(ends.at[slab], ends.at[slab], end_send.at[n], end_recv.at[slab], to),
                remote(ends.at[source], ends.at[source], end_send.at[n], end_recv.at[source], to),
            )
        )
    for c, _ in closing:
        c.start()
    for _, c in closing:
        c.wait_recv()
    row = ends[0]
    for j in range(1, slabs):
        row = row + ends[j]
    gg, gq, gd, qq, dd = [pick(row, n) for n in range(5)]
    cells = float(slabs * wide * 128)
    mean_square = gg / cells + epsilon
    inverse = 1.0 / jnp.sqrt(mean_square)
    beta = (gg / mean_square - gq * inverse) / (qq + epsilon)
    squared = gg / mean_square - 2.0 * beta * (gd * inverse) + beta * beta * dd
    norm = 1.0 / jnp.sqrt(jnp.maximum(squared, 0.0) / cells + epsilon)
    whole[...] = (-inverse * norm) * whole[...] + (beta * norm) * prior[1]
    for l in range(layers):
        dir_ref[l] = whole[pl.ds(32 * l + freq, 1), :]
    trial_ref[...] = logc[...] + step_ref[0] * whole[...].reshape(layers, 32, 128)

    @pl.when(has_above)
    def _():
        for c in ups + [seen_up]:
            c.wait_send()

    @pl.when(has_below)
    def _():
        for c in downs + [seen_down]:
            c.wait_send()

    pair_copy.wait_send()
    for c in sent + fan + spread + share + [c for c, _ in closing]:
        c.wait_send()


def per_device(
    slabs,
    positions,
    log_conductivity,
    omega,
    sources,
    receivers,
    observed,
    data_weight,
    prior_gradient,
    prior_direction,
    step_length,
):
    layers = log_conductivity.shape[0]
    total = LOW + layers + HIGH
    wide = layers * 32
    chunk = (positions, wide // positions, 128)
    hbm = pl.BlockSpec(memory_space=pltpu.HBM)
    smem = pl.BlockSpec(memory_space=pltpu.SMEM)
    vmem = pl.BlockSpec(memory_space=pltpu.VMEM)
    state = pltpu.VMEM((12, total, 48, 128), F32)
    return pl.pallas_call(
        functools.partial(kernel, layers, slabs, positions),
        out_shape=(
            jax.ShapeDtypeStruct(prior_gradient.shape, F32),
            jax.ShapeDtypeStruct(log_conductivity.shape, F32),
        ),
        in_specs=[smem] * 2 + [hbm] * 7,
        out_specs=(vmem, vmem),
        scratch_shapes=[
            pltpu.VMEM((layers, 32, 128), F32),
            pltpu.VMEM((2, 3, 2, 128), F32),
            pltpu.VMEM((3, 2, 128), F32),
            pltpu.VMEM((layers, 1, 128), F32),
            pltpu.VMEM((layers, 1, 128), F32),
            *[state] * 8,
            pltpu.VMEM((total, 32, 128), F32),
            pltpu.VMEM((5, 32, 128), F32),
            pltpu.VMEM((3, 1, 128), jnp.int32),
            pltpu.VMEM((3, 2, 2, 3, 128), F32),
            pltpu.VMEM((3, 2, 3, 128), F32),
            pltpu.VMEM((3, 4, 2, 2, 3, 128), F32),
            pltpu.VMEM((3, 2, 2, 3, 128), F32),
            pltpu.VMEM((32 * total, 128), BF16),
            pltpu.VMEM((3, 128, 128), BF16),
            pltpu.VMEM((2, 4, 2, wide, 128), F32),
            pltpu.VMEM((3, slabs, 1, 128), F32),
            pltpu.VMEM((slabs, 1, 128), F32),
            pltpu.VMEM((2, 2, layers, 128), F32),
            pltpu.VMEM((positions, 2, 2, layers, 128), F32),
            pltpu.VMEM((2, wide, 128), F32),
            pltpu.VMEM((wide, 128), F32),
            pltpu.VMEM(chunk, F32),
            pltpu.VMEM(chunk, F32),
            pltpu.VMEM((2,) + chunk[1:], F32),
            pltpu.VMEM(chunk, F32),
            pltpu.VMEM((wide, 128), F32),
            pltpu.SemaphoreType.DMA((7,)),
            pltpu.SemaphoreType.DMA((2, 8)),
            pltpu.SemaphoreType.DMA((2, 8)),
            pltpu.SemaphoreType.DMA((2,)),
            pltpu.SemaphoreType.DMA((2,)),
            pltpu.SemaphoreType.DMA((3, slabs)),
            pltpu.SemaphoreType.DMA((3, slabs)),
            pltpu.SemaphoreType.DMA((slabs,)),
            pltpu.SemaphoreType.DMA((slabs,)),
            pltpu.SemaphoreType.DMA((2,)),
            pltpu.SemaphoreType.DMA((2,)),
            pltpu.SemaphoreType.DMA((3, positions)),
            pltpu.SemaphoreType.DMA((3, positions)),
        ],
        compiler_params=pltpu.CompilerParams(
            collective_id=0, has_side_effects=True, vmem_limit_bytes=48 * 1024 * 1024
        ),
        name="inversion_step",
    )(
        omega,
        step_length,
        *(
            pltpu.with_memory_space_constraint(x, pltpu.HBM)
            for x in (
                log_conductivity,
                sources.reshape(12, layers, 32, 128),
                receivers.reshape(1, 128),
                observed[0].transpose(0, 2, 1, 3),
                data_weight[0].transpose(1, 0, 2),
                prior_gradient,
                prior_direction,
            )
        ),
    )


def solution(mesh):
    slabs = mesh.shape["slab"]
    positions = mesh.shape["freq"] // 2
    in_specs = (
        P("slab", None, None),
        P("freq"),
        P("freq", None, None, None, "slab", None, None),
        P("slab"),
        P("freq", None, None, None, "slab"),
        P("freq", None, None, "slab"),
        P("slab", "freq", None),
        P("slab", "freq", None),
        P(),
    )
    out_specs = (P("slab", "freq", None), P("slab", None, None))
    return jax.shard_map(
        functools.partial(per_device, slabs, positions),
        mesh=mesh,
        in_specs=in_specs,
        out_specs=out_specs,
        check_vma=False,
    )
```

```python
import functools

import jax
import jax.numpy as jnp
from jax import lax
from jax.experimental import pallas as pl
from jax.experimental.pallas import tpu as pltpu
from jax.sharding import PartitionSpec as P


MESH = pl.DeviceIdType.MESH
epsilon = 1e-06
F32 = jnp.float32
BF16 = jnp.bfloat16
GHOSTS = 4


def cmul(a, b):
    return a[0] * b[0] - a[1] * b[1], a[0] * b[1] + a[1] * b[0]


def cadd(a, b):
    return a[0] + b[0], a[1] + b[1]


def csub(a, b):
    return a[0] - b[0], a[1] - b[1]


def cdiv(a, b):
    modulus = b[0] * b[0] + b[1] * b[1]
    return (a[0] * b[0] + a[1] * b[1]) / modulus, (a[1] * b[0] - a[0] * b[1]) / modulus


def square_poly(p):
    out = [None] * (2 * len(p) - 1)
    for i in range(len(p)):
        for j in range(i, len(p)):
            term = cmul(p[i], p[j])
            if j > i:
                term = (term[0] + term[0], term[1] + term[1])
            out[i + j] = term if out[i + j] is None else cadd(out[i + j], term)
    return out


def against(poly, moments):
    total = None
    for c, m in zip(poly, moments):
        term = cmul(c, m)
        total = term if total is None else cadd(total, term)
    return total


def coefficients(moments, theta):
    one = (jnp.ones_like(moments[0][0]), jnp.zeros_like(moments[0][0]))
    shift = (one[0] - theta[0] * (1.0 / 6.0), -theta[1] * (1.0 / 6.0))
    steps = [csub(cmul(shift, a), b) for a, b in zip(moments, moments[1:])]
    residual, direction, rho = [one], [one], moments[0]
    solution = []
    for iteration in range(4):
        alpha = cdiv(rho, against(square_poly(direction), steps))
        moved = [cmul(alpha, c) for c in direction]
        solution = [cadd(a, b) for a, b in zip(solution, moved)] + moved[len(solution) :]
        if iteration < 3:
            kept = [csub(r, cmul(shift, m)) for r, m in zip(residual, moved)]
            residual = [kept[0]]
            residual += [cadd(kept[k + 1], moved[k]) for k in range(len(moved) - 1)]
            residual += [moved[-1]]
            rho_next = against(square_poly(residual), moments)
            beta = cdiv(rho_next, rho)
            direction = [
                cadd(residual[k], cmul(beta, direction[k])) for k in range(len(direction))
            ] + [residual[-1]]
            rho = rho_next
    return [(c[0] * 6.0 ** -(k + 1), c[1] * 6.0 ** -(k + 1)) for k, c in enumerate(solution)]


def split3(x):
    high = x.astype(BF16)
    rest = x - high.astype(F32)
    mid = rest.astype(BF16)
    low = (rest - mid.astype(F32)).astype(BF16)
    return high, mid, low


def kernel(
    layers,
    slabs,
    positions,
    omega_ref,
    step_ref,
    logc_in,
    src_in,
    rec_in,
    obs_in,
    wt_in,
    pg_in,
    pd_in,
    dir_ref,
    trial_ref,
    logc,
    obs,
    wt,
    pg,
    pd,
    v0,
    v1,
    v2,
    v3,
    u0,
    u1,
    u2,
    u3,
    kap,
    lcg,
    recs,
    wanted,
    weights_at,
    seen,
    data,
    row_hot,
    column_hot,
    products,
    allred,
    ends,
    prior_pair,
    prior_all,
    prior,
    grad,
    grad_src,
    grad_in,
    grad_pair,
    grad_all,
    whole,
    load_sem,
    near_send,
    near_recv,
    seen_send,
    seen_recv,
    ar_send,
    ar_recv,
    end_send,
    end_recv,
    pair_send,
    pair_recv,
    fan_send,
    fan_recv,
):
    freq = lax.axis_index("freq")
    slab = lax.axis_index("slab")
    half = freq // positions
    place = freq % positions
    base = half * positions
    cores = 2
    chips = slabs // cores
    line = 2 * chips
    high = half * chips + slab // cores
    core = slab % cores
    own_lo, own_hi = GHOSTS, GHOSTS + layers
    total_layers = layers + 2 * GHOSTS
    wide = 32 * layers
    chunk = wide // positions

    def remote(src, dst, send, recv, to):
        return pltpu.make_async_remote_copy(
            src_ref=src, dst_ref=dst, send_sem=send, recv_sem=recv, device_id=to, device_id_type=MESH
        )

    def on_line(away, other_core):
        z = (high + away) % line
        return (z // chips) * positions + place, (z % chips) * cores + other_core

    partner = on_line(chips, core)
    side = 4
    offsets = [(dy, dx) for dy in range(positions // side) for dx in range(side)][1:]
    offsets.sort(key=lambda o: -sum(min(k, side - k) for k in o))

    def in_plane(d):
        dy, dx = offsets[d]
        y = (place // side + dy) % (positions // side)
        return y * side + (place % side + dx) % side

    loads = [
        pltpu.make_async_copy(s, d, load_sem.at[n])
        for n, (s, d) in enumerate(
            (
                (src_in, v0.at[:, pl.ds(own_lo, layers), pl.ds(8, 32), :]),
                (logc_in, logc),
                (rec_in, recs.at[1]),
                (pg_in, pg),
                (pd_in, pd),
                (obs_in, obs),
                (wt_in, wt),
            )
        )
    ]
    for c in loads:
        c.start()
    barrier = pltpu.get_barrier_semaphore()
    greeted = [on_line(0, 1 - core)]
    greeted += [on_line(away, c) for away in range(1, line) for c in range(cores)]
    greeted += [(base + in_plane(d), slab) for d in range(positions - 1)]
    for to in greeted:
        pl.semaphore_signal(barrier, inc=1, device_id=to, device_id_type=MESH)

    edge = jnp.zeros((12, total_layers, 1, 128), F32)

    def clear_edges(arrays):
        for v in arrays:
            v[:, :, 7:8, :] = edge
            v[:, :, 40:41, :] = edge

    clear_edges((v0, v1, v2, v3))
    has_below = slab > 0
    has_above = slab < slabs - 1

    @pl.when(slab == 0)
    def _():
        v0[:, 0:own_lo, 8:40, :] = jnp.zeros((12, GHOSTS, 32, 128), F32)
        lcg[0:3] = jnp.zeros((3, 32, 128), F32)
        recs[0] = jnp.zeros((1, 128), jnp.int32)
        wanted[0] = jnp.zeros((2, 2, 3, 128), F32)
        weights_at[0] = jnp.zeros((2, 3, 128), F32)
        seen[0] = jnp.zeros((4, 2, 2, 3, 128), F32)

    @pl.when(slab == slabs - 1)
    def _():
        v0[:, own_hi:total_layers, 8:40, :] = jnp.zeros((12, GHOSTS, 32, 128), F32)
        lcg[3:6] = jnp.zeros((3, 32, 128), F32)
        recs[2] = jnp.zeros((1, 128), jnp.int32)
        wanted[2] = jnp.zeros((2, 2, 3, 128), F32)
        weights_at[2] = jnp.zeros((2, 3, 128), F32)
        seen[2] = jnp.zeros((4, 2, 2, 3, 128), F32)

    lanes = lax.broadcasted_iota(jnp.int32, (1, 128), 1)
    lane8 = lax.broadcasted_iota(jnp.int32, (8, 128), 1)
    last8 = lane8 == 127

    def in_lanes(sums):
        row = jnp.zeros((1, 128), F32)
        for n, s in enumerate(sums):
            one = jnp.sum(s, axis=0, keepdims=True)
            row = row + jnp.where(lanes == n, jnp.sum(one, axis=1, keepdims=True), 0.0)
        return row

    def pick(row, n):
        return jnp.sum(jnp.where(lanes == n, row, 0.0), axis=1, keepdims=True)

    loads[1].wait()
    omega = omega_ref[0]
    kap[own_lo:own_hi] = omega * jnp.exp(logc[...])
    loads[0].wait()

    def weigh(l, acc):
        acc = list(acc)
        across = jnp.where(l == own_hi - 1, 0.0, layers / (layers - 1.0)).astype(F32)
        beyond = jnp.where(l == own_hi - 1, l, l + 1)
        for r in range(4):
            y = 8 + 8 * r
            coupling = kap[l, 8 * r : 8 * r + 8, :]
            acc[6] = acc[6] + coupling
            for pol in range(2):
                square = product = None
                for p in range(6 * pol, 6 * pol + 6):
                    here = v0[p, l, y : y + 8, :]
                    more = jnp.where(last8, 0.0, pltpu.roll(here, 127, 1))
                    more = more + v0[p, l, y + 1 : y + 9, :]
                    more = more + across * v0[p, beyond, y : y + 8, :]
                    sq, pr = here * here, here * more
                    square = sq if square is None else square + sq
                    product = pr if product is None else product + pr
                acc[3 * pol] = acc[3 * pol] + square
                acc[3 * pol + 1] = acc[3 * pol + 1] + product
                acc[3 * pol + 2] = acc[3 * pol + 2] + coupling * square
        return tuple(acc)

    weights = lax.fori_loop(own_lo, own_hi, weigh, (jnp.zeros((8, 128), F32),) * 7)

    def slab_start(n, row):
        allred[n, slab] = row
        copies = []
        for d in range(slabs - 1):
            down, up = slabs - 1 - d, d
            down = jnp.where(down > slab, down, down - 1)
            up = jnp.where(up < slab, up, up + 1)
            copies.append(
                remote(
                    allred.at[n, slab],
                    allred.at[n, slab],
                    ar_send.at[n, d],
                    ar_recv.at[n, slab],
                    (freq, jnp.where(slab < slabs // 2, down, up)),
                )
            )
        for c in copies:
            c.start()
        return copies

    def slab_finish(n):
        for d in range(1, slabs):
            other = (slab + d) % slabs
            remote(
                allred.at[n, other],
                allred.at[n, other],
                ar_send.at[n, d],
                ar_recv.at[n, other],
                (freq, other),
            ).wait_recv()
        total = allred[n, 0]
        for j in range(1, slabs):
            total = total + allred[n, j]
        return total

    weights = in_lanes(weights)
    for n in range(2, len(loads)):
        loads[n].wait()
    for pol in range(2):
        for comp in range(3):
            at = slice(comp, comp + 1)
            weights_at[1, pol, at, :] = wt[comp, pol : pol + 1, :]
            for ri in range(2):
                wanted[1, pol, ri, at, :] = obs[pol, comp, ri : ri + 1, :]
    pl.semaphore_wait(barrier, len(greeted))
    sent = slab_start(0, weights)

    rows = pl.ds(8, 32)
    below_to = (freq, lax.max(slab - 1, 0))
    above_to = (freq, lax.min(slab + 1, slabs - 1))
    upward = [
        (recs.at[1], recs.at[0]),
        (logc.at[pl.ds(layers - 3, 3)], lcg.at[pl.ds(0, 3)]),
    ]
    downward = [
        (recs.at[1], recs.at[2]),
        (logc.at[pl.ds(0, 3)], lcg.at[pl.ds(3, 3)]),
    ]
    for k in range(GHOSTS):
        last = k == GHOSTS - 1
        of = pl.ds(6, 6) if last else slice(None)
        upward.append(
            (v0.at[of, own_hi - 1 - k, rows, :], v0.at[of, own_lo - 1 - k, rows, :])
        )
        of = pl.ds(0, 6) if last else slice(None)
        downward.append((v0.at[of, own_lo + k, rows, :], v0.at[of, own_hi + k, rows, :]))
    for ref in (wanted, weights_at):
        upward.append((ref.at[1], ref.at[0]))
        downward.append((ref.at[1], ref.at[2]))
    ups = [
        remote(s, d, near_send.at[0, n], near_recv.at[0, n], above_to)
        for n, (s, d) in enumerate(upward)
    ]
    downs = [
        remote(s, d, near_send.at[1, n], near_recv.at[1, n], below_to)
        for n, (s, d) in enumerate(downward)
    ]

    @pl.when(has_above)
    def _():
        for c in ups:
            c.start()

    @pl.when(has_below)
    def _():
        for c in downs:
            c.start()

    for l in range(layers):
        prior_pair[half, 0, l : l + 1, :] = pg[l]
        prior_pair[half, 1, l : l + 1, :] = pd[l]
    prior_copy = remote(
        prior_pair.at[half], prior_pair.at[half], pair_send.at[0], pair_recv.at[0], partner
    )
    prior_copy.start()

    def arrived(from_below, from_above):
        @pl.when(has_below)
        def _():
            for n in from_below:
                ups[n].wait_recv()

        @pl.when(has_above)
        def _():
            for n in from_above:
                downs[n].wait_recv()

    lane = lax.broadcasted_iota(jnp.int32, (32, 128), 1)
    first_lane, last_lane = lane == 0, lane == 127
    alive_low = jnp.where(slab == 0, 0.0, 1.0).astype(F32)
    alive_high = jnp.where(slab == slabs - 1, 0.0, 1.0).astype(F32)

    def alive(l):
        inside = jnp.where(l < own_lo, alive_low, 1.0)
        return jnp.where(l >= own_hi, alive_high, inside)

    def step(theta, src, dst, where, ghosts):
        for pol in range(2):
            l = where[pol]

            def around(p, l=l):
                here = src[p, l, 8:40, :]
                total = src[p, l - 1, 8:40, :] + src[p, l + 1, 8:40, :]
                total = total + (src[p, l, 7:39, :] + src[p, l, 9:41, :])
                left = jnp.where(first_lane, 0.0, pltpu.roll(here, 1, 1))
                right = jnp.where(last_lane, 0.0, pltpu.roll(here, 127, 1))
                return here, total + (left + right)

            shift_re, shift_im = theta[pol]
            coupling = kap[l] + shift_im
            mask = alive(l) if ghosts else None
            for comp in range(3):
                p = pol * 6 + comp
                re, around_re = around(p)
                im, around_im = around(p + 3)
                if shift_re is not None:
                    around_re = around_re - shift_re * re
                    around_im = around_im - shift_re * im
                new_re = around_re + coupling * im
                new_im = around_im - coupling * re
                if mask is not None:
                    new_re, new_im = mask * new_re, mask * new_im
                dst[p, l, 8:40, :] = new_re
                dst[p + 3, l, 8:40, :] = new_im

    def sweep(theta, src, dst, starts, count, ghosts):
        def body(n, carry):
            for k in range(2):
                step(theta, src, dst, [at + 2 * n + k for at in starts], ghosts)
            return carry

        lax.fori_loop(0, count // 2, body, 0)
        if count % 2:
            step(theta, src, dst, [at + count - 1 for at in starts], ghosts)

    def both(theta, src, dst, low, high, ghosts):
        def body(n, carry):
            l = low + n * (high - low)
            step(theta, src, dst, (l, l), ghosts)
            return carry

        lax.fori_loop(0, 2, body, 0)

    def moment_sums(theta, v_list):
        v3 = v_list[3]
        sums = []
        for pol in range(2):
            shift_re, shift_im = theta[pol]

            def body(l, acc):
                acc = list(acc)

                def add(k, value):
                    acc[k] = acc[k] + value

                for r in range(4):
                    y = 8 + 8 * r
                    coupling = kap[l, 8 * r : 8 * r + 8, :] + shift_im
                    for comp in range(3):
                        p = pol * 6 + comp
                        vs = [(v[p, l, y : y + 8, :], v[p + 3, l, y : y + 8, :]) for v in v_list]
                        for k in range(4):
                            re, im = vs[k]
                            add(4 * k, (re - im) * (re + im))
                            add(4 * k + 1, re * im)
                        halves = []
                        for q in (p, p + 3):
                            here = v3[q, l, y : y + 8, :]
                            right = jnp.where(last8, 0.0, pltpu.roll(here, 127, 1))
                            more = v3[q, l, y + 1 : y + 9, :] + right
                            halves.append(more + more)
                        re, im = vs[3]
                        if shift_re is not None:
                            halves = [halves[0] - shift_re * re, halves[1] - shift_re * im]
                        after = (halves[0] + coupling * im, halves[1] - coupling * re)
                        pairs = [(vs[0], vs[1]), (vs[1], vs[2]), (vs[2], vs[3]), (vs[3], after)]
                        for k, (u, w) in enumerate(pairs):
                            add(4 * k + 2, u[0] * w[0] - u[1] * w[1])
                            add(4 * k + 3, u[0] * w[1] + u[1] * w[0])
                return tuple(acc)

            zero = jnp.zeros((8, 128), F32)
            sums += list(lax.fori_loop(own_lo, own_hi, body, (zero,) * 16))
        return sums

    def layer_pair(v3, where, acc):
        acc = list(acc)
        for pol in range(2):
            l = where[pol]
            for comp in range(3):
                for r in range(4):
                    p, y = pol * 6 + comp, 8 + 8 * r
                    u = (v3[p, l, y : y + 8, :], v3[p + 3, l, y : y + 8, :])
                    w = (v3[p, l + 1, y : y + 8, :], v3[p + 3, l + 1, y : y + 8, :])
                    acc[2 * pol] = acc[2 * pol] + (u[0] * w[0] - u[1] * w[1])
                    acc[2 * pol + 1] = acc[2 * pol + 1] + (u[0] * w[1] + u[1] * w[0])
        return tuple(acc)

    def pair_row(pairs):
        row = in_lanes([p + p for p in pairs])
        spread = jnp.zeros((1, 128), F32)
        for n, at in enumerate((14, 15, 30, 31)):
            spread = spread + jnp.where(lanes == at, pick(row, n), 0.0)
        return spread

    def layer_pairs(v3, starts, count):
        def body(n, acc):
            return layer_pair(v3, [at + n for at in starts], acc)

        return lax.fori_loop(0, count, body, (jnp.zeros((8, 128), F32),) * 4)

    def solve_coefficients(row, theta):
        found = []
        for pol in range(2):
            moments = []
            for k in range(8):
                re = pick(row, 16 * pol + 2 * k) * 6.0**-k
                im = pick(row, 16 * pol + 2 * k + 1) * 6.0**-k
                if k % 2 == 0:
                    im = im + im
                moments.append((re, im))
            most = None
            for m in moments:
                size = jnp.maximum(jnp.abs(m[0]), jnp.abs(m[1]))
                most = size if most is None else jnp.maximum(most, size)
            scale = 1.0 / most
            moments = [(m[0] * scale, m[1] * scale) for m in moments]
            found.append(coefficients(moments, theta[pol]))
        return found

    def combined(coefs, v_list, pol, comp, l, y):
        p = pol * 6 + comp
        re = im = None
        for (cr, ci), v in zip(coefs[pol], v_list):
            a, b = v[p, l, y : y + 8, :], v[p + 3, l, y : y + 8, :]
            tr, ti = cr * a - ci * b, cr * b + ci * a
            re, im = (tr, ti) if re is None else (re + tr, im + ti)
        return re, im

    line_of, lane_of = recs[1] // 128, recs[1] % 128
    column = lax.broadcasted_iota(jnp.int32, (128, 128), 0) == lane_of
    column_hot[1] = column.astype(F32).astype(BF16)
    at_row = lax.broadcasted_iota(jnp.int32, (wide, 128), 0) == line_of

    def look(j, v):
        def body(pol, carry):
            column = column_hot[1]
            taller = jnp.concatenate([column] * 3, axis=0)
            for ri in range(2):
                for comp in range(3):
                    plane = v[pol * 6 + ri * 3 + comp, own_lo:own_hi, 8:40, :].reshape(wide, 128)
                    parts = jnp.concatenate(split3(plane), axis=1)
                    found = jnp.dot(parts, taller, preferred_element_type=F32)
                    value = jnp.sum(jnp.where(at_row, found, 0.0), axis=0, keepdims=True)
                    seen[1, j, pol, ri, comp : comp + 1, :] = value
            return carry

        lax.fori_loop(0, 2, body, 0)

    forward, backward = (v0, v1, v2, v3), (u0, u1, u2, u3)
    clear_edges(backward)
    look(0, v0)
    weights = slab_finish(0)
    theta = []
    for pol in range(2):
        square = pick(weights, 3 * pol)
        theta.append(
            (
                2.0 * pick(weights, 3 * pol + 1) / square,
                -pick(weights, 3 * pol + 2) / square,
            )
        )
    mean_coupling = pick(weights, 6) / float(slabs * wide * 128)
    middle = own_lo + layers // 2
    sweep(theta, v0, v1, (own_lo + 1,) * 2, layers - 2, False)
    step(theta, v1, v2, (middle, middle), False)
    arrived((0, 1), (0, 1))
    kap[own_lo - 3 : own_lo] = omega * jnp.exp(lcg[0:3])
    kap[own_hi : own_hi + 3] = omega * jnp.exp(lcg[3:6])
    arrived((2,), (2,))
    both(theta, v0, v1, own_lo, own_hi - 1, False)
    both(theta, v1, v2, own_lo + 1, own_hi - 2, False)
    step(theta, v2, v3, (middle, middle), False)
    look(1, v1)
    arrived((3,), (3,))
    both(theta, v0, v1, own_lo - 1, own_hi, True)
    both(theta, v1, v2, own_lo, own_hi - 1, False)
    both(theta, v2, v3, own_lo + 1, own_hi - 2, False)
    look(2, v2)
    arrived((4,), (4,))
    both(theta, v0, v1, own_lo - 2, own_hi + 1, True)
    both(theta, v1, v2, own_lo - 1, own_hi, True)
    both(theta, v2, v3, own_lo, own_hi - 1, False)
    row = in_lanes(moment_sums(theta, forward))
    pairs = layer_pairs(v3, (own_lo, own_lo), layers - 1)
    arrived((5,), (5,))
    step(theta, v0, v1, (own_hi + 2, own_lo - 3), True)
    step(theta, v1, v2, (own_hi + 1, own_lo - 2), True)
    step(theta, v2, v3, (own_hi, own_lo - 1), True)
    pairs = layer_pair(v3, (own_hi - 1, own_lo - 1), pairs)
    sent += slab_start(1, row + pair_row(pairs))

    look(3, v3)
    seen_up = remote(seen.at[1], seen.at[0], seen_send.at[0], seen_recv.at[0], above_to)
    seen_down = remote(seen.at[1], seen.at[2], seen_send.at[1], seen_recv.at[1], below_to)

    @pl.when(has_above)
    def _():
        seen_up.start()

    @pl.when(has_below)
    def _():
        seen_down.start()

    spots = (
        (0, 32 * (layers - GHOSTS), GHOSTS, 0),
        (1, 0, layers, own_lo),
        (2, 0, GHOSTS, own_hi),
    )
    for n, first_row, count, layer_at in spots:
        line_of, lane_of = recs[n] // 128, recs[n] % 128
        if n != 1:
            column = lax.broadcasted_iota(jnp.int32, (128, 128), 0) == lane_of
            column_hot[n] = column.astype(F32).astype(BF16)
        rows_here = lax.broadcasted_iota(jnp.int32, (32 * count, 128), 0) + first_row
        hit = (rows_here == line_of).astype(F32).astype(BF16)
        row_hot[32 * layer_at : 32 * (layer_at + count), :] = hit

    prior_copy.wait()
    prior_all[place] = prior_pair[...]
    fan = [
        remote(
            prior_pair,
            prior_all.at[place],
            fan_send.at[0, d],
            fan_recv.at[0, place],
            (base + in_plane(d), slab),
        )
        for d in range(positions - 1)
    ]
    for c in fan:
        c.start()

    arrived((6, 7), (6, 7))

    @pl.when(has_below)
    def _():
        seen_up.wait_recv()

    @pl.when(has_above)
    def _():
        seen_down.wait_recv()

    row = slab_finish(1)
    coefs = solve_coefficients(row, theta)

    for n in range(3):
        for pol in range(2):
            re = im = None
            for j, (cr, ci) in enumerate(coefs[pol]):
                a, b = seen[n, j, pol, 0], seen[n, j, pol, 1]
                tr, ti = cr * a - ci * b, cr * b + ci * a
                re, im = (tr, ti) if re is None else (re + tr, im + ti)
            weight = weights_at[n, pol]
            square = weight * weight
            data[n, pol, 0] = square * (re - wanted[n, pol, 0])
            data[n, pol, 1] = -square * (im - wanted[n, pol, 1])

    for n, _, count, layer_at in spots:
        wider = jnp.concatenate([column_hot[n]] * 3, axis=1)
        for pol in range(2):
            first, much = layer_at, count
            if n == 2 - 2 * pol:
                pass
            elif n != 1:
                much = count - 1
                first = layer_at + (1 if n == 0 else 0)
            hit = row_hot[32 * first : 32 * (first + much), :]
            spread = []
            for ri in range(2):
                for comp in range(3):
                    parts = split3(data[n, pol, ri, comp : comp + 1, :])
                    spread.append(jnp.concatenate([hit * part for part in parts], axis=1))
            placed = lax.dot_general(
                jnp.concatenate(spread, axis=0),
                wider,
                (((1,), (1,)), ((), ())),
                preferred_element_type=F32,
            )
            u0[6 * pol : 6 * pol + 6, first : first + much, 8:40, :] = placed.reshape(
                6, much, 32, 128
            )

    behind = [(None, -mean_coupling)] * 2
    sweep(behind, u0, u1, (own_lo - 2, own_lo - 3), layers + 5, True)
    sweep(behind, u1, u2, (own_lo - 1, own_lo - 2), layers + 3, True)
    sweep(behind, u2, u3, (own_lo, own_lo - 1), layers + 1, True)
    sums = moment_sums(behind, backward)
    pairs = layer_pairs(u3, (own_lo, own_lo - 1), layers)
    for pol in range(2):
        for part in range(2):
            at, more = 16 * pol + 14 + part, pairs[2 * pol + part]
            sums[at] = sums[at] + (more + more)
    sent += slab_start(2, in_lanes(sums))

    def multiply(l, carry):
        for r in range(4):
            y = 8 + 8 * r
            at = pl.multiple_of((l - own_lo) * 32 + 8 * r, 8)
            coupling = kap[l, 8 * r : 8 * r + 8, :]
            for pol in range(2):
                fields = [combined(coefs, forward, pol, comp, l, y) for comp in range(3)]
                for j, u in enumerate(backward):
                    first = second = None
                    for comp in range(3):
                        p = pol * 6 + comp
                        re, im = u[p, l, y : y + 8, :], u[p + 3, l, y : y + 8, :]
                        f_re, f_im = fields[comp]
                        x, z = re * f_im + im * f_re, re * f_re - im * f_im
                        first, second = (x, z) if first is None else (first + x, second + z)
                    products[pol, j, 0, pl.ds(at, 8), :] = coupling * first
                    products[pol, j, 1, pl.ds(at, 8), :] = coupling * second
        return carry

    lax.fori_loop(own_lo, own_hi, multiply, 0)
    row = slab_finish(2)
    coefs = solve_coefficients(row, [(jnp.zeros_like(mean_coupling), -mean_coupling)] * 2)
    for n in range(wide // 8):
        total = None
        for pol in range(2):
            for j in range(4):
                for part in range(2):
                    term = coefs[pol][j][part] * products[pol, j, part, 8 * n : 8 * n + 8, :]
                    total = term if total is None else total + term
        grad[8 * n : 8 * n + 8, :] = total

    for j in range(positions):
        grad_src[j] = grad[chunk * j : chunk * (j + 1), :]
    grad_in[place] = grad_src[place]
    spread = []
    for d in range(positions - 1):
        j = in_plane(d)
        spread.append(
            remote(
                grad_src.at[j],
                grad_in.at[place],
                fan_send.at[1, d],
                fan_recv.at[1, place],
                (base + j, slab),
            )
        )
    for c in spread:
        c.start()

    def gathered(n, ref):
        for d in range(positions - 1):
            j = in_plane(d)
            remote(
                ref.at[j], ref.at[j], fan_send.at[n, d], fan_recv.at[n, j], (base + j, slab)
            ).wait_recv()

    gathered(0, prior_all)
    for y in range(2 * positions):
        for w in range(2):
            for l in range(layers):
                prior[w, 32 * l + y : 32 * l + y + 1, :] = prior_all[
                    y % positions, y // positions, w, l : l + 1, :
                ]
    old_grad, old_dir = prior[0], prior[1]

    def folded(x):
        total = x[0:8]
        for n in range(1, wide // 8):
            total = total + x[8 * n : 8 * n + 8]
        return total

    prior_sums = [folded(old_grad * old_grad), folded(old_dir * old_dir)]

    gathered(1, grad_in)
    partial = grad_in[0]
    for j in range(1, positions):
        partial = partial + grad_in[j]
    grad_pair[half] = partial
    pair_copy = remote(
        grad_pair.at[half], grad_pair.at[half], pair_send.at[1], pair_recv.at[1], partner
    )
    pair_copy.start()
    pair_copy.wait_recv()
    grad_all[place] = grad_pair[0] + grad_pair[1]
    share = []
    for d in range(positions - 1):
        to = (base + in_plane(d), slab)
        share.append(
            remote(
                grad_all.at[place], grad_all.at[place], fan_send.at[2, d], fan_recv.at[2, place], to
            )
        )
    for c in share:
        c.start()
    gathered(2, grad_all)
    for j in range(positions):
        whole[chunk * j : chunk * (j + 1), :] = grad_all[j]

    g = whole[...]
    sums = [folded(g * g), folded(g * old_grad), folded(g * old_dir)] + prior_sums
    ends[slab] = in_lanes(sums)
    closing = []
    for away, other in [(a, c) for a in (2, 1, -1) for c in range(cores)] + [(0, 1 - core)]:
        n = len(closing)
        to = on_line(away, other)
        source = on_line(-away, other)[1]
        closing.append(
            (
                remote(ends.at[slab], ends.at[slab], end_send.at[n], end_recv.at[slab], to),
                remote(ends.at[source], ends.at[source], end_send.at[n], end_recv.at[source], to),
            )
        )
    for c, _ in closing:
        c.start()
    for _, c in closing:
        c.wait_recv()
    row = ends[0]
    for j in range(1, slabs):
        row = row + ends[j]
    gg, gq, gd, qq, dd = [pick(row, n) for n in range(5)]
    cells = float(slabs * wide * 128)
    mean_square = gg / cells + epsilon
    inverse = 1.0 / jnp.sqrt(mean_square)
    beta = (gg / mean_square - gq * inverse) / (qq + epsilon)
    squared = gg / mean_square - 2.0 * beta * (gd * inverse) + beta * beta * dd
    norm = 1.0 / jnp.sqrt(jnp.maximum(squared, 0.0) / cells + epsilon)
    whole[...] = (-inverse * norm) * whole[...] + (beta * norm) * prior[1]
    for l in range(layers):
        dir_ref[l] = whole[pl.ds(32 * l + freq, 1), :]
    trial_ref[...] = logc[...] + step_ref[0] * whole[...].reshape(layers, 32, 128)

    @pl.when(has_above)
    def _():
        for c in ups + [seen_up]:
            c.wait_send()

    @pl.when(has_below)
    def _():
        for c in downs + [seen_down]:
            c.wait_send()

    pair_copy.wait_send()
    for c in sent + fan + spread + share + [c for c, _ in closing]:
        c.wait_send()


def per_device(
    slabs,
    positions,
    log_conductivity,
    omega,
    sources,
    receivers,
    observed,
    data_weight,
    prior_gradient,
    prior_direction,
    step_length,
):
    layers = log_conductivity.shape[0]
    total = layers + 2 * GHOSTS
    wide = layers * 32
    chunk = (positions, wide // positions, 128)
    hbm = pl.BlockSpec(memory_space=pltpu.HBM)
    smem = pl.BlockSpec(memory_space=pltpu.SMEM)
    vmem = pl.BlockSpec(memory_space=pltpu.VMEM)
    state = pltpu.VMEM((12, total, 48, 128), F32)
    return pl.pallas_call(
        functools.partial(kernel, layers, slabs, positions),
        out_shape=(
            jax.ShapeDtypeStruct(prior_gradient.shape, F32),
            jax.ShapeDtypeStruct(log_conductivity.shape, F32),
        ),
        in_specs=[smem] * 2 + [hbm] * 7,
        out_specs=(vmem, vmem),
        scratch_shapes=[
            pltpu.VMEM((layers, 32, 128), F32),
            pltpu.VMEM((2, 3, 2, 128), F32),
            pltpu.VMEM((3, 2, 128), F32),
            pltpu.VMEM((layers, 1, 128), F32),
            pltpu.VMEM((layers, 1, 128), F32),
            *[state] * 8,
            pltpu.VMEM((total, 32, 128), F32),
            pltpu.VMEM((6, 32, 128), F32),
            pltpu.VMEM((3, 1, 128), jnp.int32),
            pltpu.VMEM((3, 2, 2, 3, 128), F32),
            pltpu.VMEM((3, 2, 3, 128), F32),
            pltpu.VMEM((3, 4, 2, 2, 3, 128), F32),
            pltpu.VMEM((3, 2, 2, 3, 128), F32),
            pltpu.VMEM((32 * total, 128), BF16),
            pltpu.VMEM((3, 128, 128), BF16),
            pltpu.VMEM((2, 4, 2, wide, 128), F32),
            pltpu.VMEM((3, slabs, 1, 128), F32),
            pltpu.VMEM((slabs, 1, 128), F32),
            pltpu.VMEM((2, 2, layers, 128), F32),
            pltpu.VMEM((positions, 2, 2, layers, 128), F32),
            pltpu.VMEM((2, wide, 128), F32),
            pltpu.VMEM((wide, 128), F32),
            pltpu.VMEM(chunk, F32),
            pltpu.VMEM(chunk, F32),
            pltpu.VMEM((2,) + chunk[1:], F32),
            pltpu.VMEM(chunk, F32),
            pltpu.VMEM((wide, 128), F32),
            pltpu.SemaphoreType.DMA((7,)),
            pltpu.SemaphoreType.DMA((2, 8)),
            pltpu.SemaphoreType.DMA((2, 8)),
            pltpu.SemaphoreType.DMA((2,)),
            pltpu.SemaphoreType.DMA((2,)),
            pltpu.SemaphoreType.DMA((3, slabs)),
            pltpu.SemaphoreType.DMA((3, slabs)),
            pltpu.SemaphoreType.DMA((slabs,)),
            pltpu.SemaphoreType.DMA((slabs,)),
            pltpu.SemaphoreType.DMA((2,)),
            pltpu.SemaphoreType.DMA((2,)),
            pltpu.SemaphoreType.DMA((3, positions)),
            pltpu.SemaphoreType.DMA((3, positions)),
        ],
        compiler_params=pltpu.CompilerParams(
            collective_id=0, has_side_effects=True, vmem_limit_bytes=48 * 1024 * 1024
        ),
        name="inversion_step",
    )(
        omega,
        step_length,
        *(
            pltpu.with_memory_space_constraint(x, pltpu.HBM)
            for x in (
                log_conductivity,
                sources.reshape(12, layers, 32, 128),
                receivers.reshape(1, 128),
                observed[0].transpose(0, 2, 1, 3),
                data_weight[0].transpose(1, 0, 2),
                prior_gradient,
                prior_direction,
            )
        ),
    )


def solution(mesh):
    slabs = mesh.shape["slab"]
    positions = mesh.shape["freq"] // 2
    in_specs = (
        P("slab", None, None),
        P("freq"),
        P("freq", None, None, None, "slab", None, None),
        P("slab"),
        P("freq", None, None, None, "slab"),
        P("freq", None, None, "slab"),
        P("slab", "freq", None),
        P("slab", "freq", None),
        P(),
    )
    out_specs = (P("slab", "freq", None), P("slab", None, None))
    return jax.shard_map(
        functools.partial(per_device, slabs, positions),
        mesh=mesh,
        in_specs=in_specs,
        out_specs=out_specs,
        check_vma=False,
    )
```

```python
import functools

import jax
import jax.numpy as jnp
from jax import lax
from jax.experimental import pallas as pl
from jax.experimental.pallas import tpu as pltpu
from jax.sharding import PartitionSpec as P


MESH = pl.DeviceIdType.MESH
epsilon = 1e-06
F32 = jnp.float32
BF16 = jnp.bfloat16
GHOSTS = 4


def cmul(a, b):
    return a[0] * b[0] - a[1] * b[1], a[0] * b[1] + a[1] * b[0]


def cadd(a, b):
    return a[0] + b[0], a[1] + b[1]


def csub(a, b):
    return a[0] - b[0], a[1] - b[1]


def cdiv(a, b):
    modulus = b[0] * b[0] + b[1] * b[1]
    return (a[0] * b[0] + a[1] * b[1]) / modulus, (a[1] * b[0] - a[0] * b[1]) / modulus


def square_poly(p):
    out = [None] * (2 * len(p) - 1)
    for i in range(len(p)):
        for j in range(i, len(p)):
            term = cmul(p[i], p[j])
            if j > i:
                term = (term[0] + term[0], term[1] + term[1])
            out[i + j] = term if out[i + j] is None else cadd(out[i + j], term)
    return out


def against(poly, moments):
    total = None
    for c, m in zip(poly, moments):
        term = cmul(c, m)
        total = term if total is None else cadd(total, term)
    return total


def coefficients(moments, theta):
    one = (jnp.ones_like(moments[0][0]), jnp.zeros_like(moments[0][0]))
    shift = (one[0] - theta[0] * (1.0 / 6.0), -theta[1] * (1.0 / 6.0))
    steps = [csub(cmul(shift, a), b) for a, b in zip(moments, moments[1:])]
    residual, direction, rho = [one], [one], moments[0]
    solution = []
    for iteration in range(4):
        alpha = cdiv(rho, against(square_poly(direction), steps))
        moved = [cmul(alpha, c) for c in direction]
        solution = [cadd(a, b) for a, b in zip(solution, moved)] + moved[len(solution) :]
        if iteration < 3:
            kept = [csub(r, cmul(shift, m)) for r, m in zip(residual, moved)]
            residual = [kept[0]]
            residual += [cadd(kept[k + 1], moved[k]) for k in range(len(moved) - 1)]
            residual += [moved[-1]]
            rho_next = against(square_poly(residual), moments)
            beta = cdiv(rho_next, rho)
            direction = [
                cadd(residual[k], cmul(beta, direction[k])) for k in range(len(direction))
            ] + [residual[-1]]
            rho = rho_next
    return [(c[0] * 6.0 ** -(k + 1), c[1] * 6.0 ** -(k + 1)) for k, c in enumerate(solution)]


def split3(x):
    high = x.astype(BF16)
    rest = x - high.astype(F32)
    mid = rest.astype(BF16)
    low = (rest - mid.astype(F32)).astype(BF16)
    return high, mid, low


def kernel(
    layers,
    slabs,
    positions,
    omega_ref,
    step_ref,
    logc_in,
    src_in,
    rec_in,
    obs_in,
    wt_in,
    pg_in,
    pd_in,
    dir_ref,
    trial_ref,
    logc,
    obs,
    wt,
    pg,
    pd,
    v0,
    v1,
    v2,
    v3,
    u0,
    u1,
    u2,
    u3,
    sides,
    kap,
    lcg,
    recs,
    wanted,
    weights_at,
    seen,
    data,
    row_hot,
    column_hot,
    products,
    allred,
    ends,
    prior_pair,
    prior_all,
    prior,
    prior_src,
    grad,
    grad_src,
    grad_in,
    grad_pair,
    grad_all,
    whole,
    load_sem,
    near_send,
    near_recv,
    seen_send,
    seen_recv,
    ar_send,
    ar_recv,
    end_send,
    end_recv,
    pair_send,
    pair_recv,
    fan_send,
    fan_recv,
):
    freq = lax.axis_index("freq")
    slab = lax.axis_index("slab")
    half = freq // positions
    place = freq % positions
    base = half * positions
    cores = 2
    chips = slabs // cores
    line = 2 * chips
    high = half * chips + slab // cores
    core = slab % cores
    own_lo, own_hi = GHOSTS, GHOSTS + layers
    total_layers = layers + 2 * GHOSTS
    wide = 32 * layers
    chunk = wide // positions

    def remote(src, dst, send, recv, to):
        return pltpu.make_async_remote_copy(
            src_ref=src, dst_ref=dst, send_sem=send, recv_sem=recv, device_id=to, device_id_type=MESH
        )

    def on_line(away, other_core):
        z = (high + away) % line
        return (z // chips) * positions + place, (z % chips) * cores + other_core

    partner = on_line(chips, core)
    side = 4
    offsets = [(dy, dx) for dy in range(positions // side) for dx in range(side)][1:]
    offsets.sort(key=lambda o: -sum(min(k, side - k) for k in o))

    def in_plane(d):
        dy, dx = offsets[d]
        y = (place // side + dy) % (positions // side)
        return y * side + (place % side + dx) % side

    loads = [
        pltpu.make_async_copy(s, d, load_sem.at[n])
        for n, (s, d) in enumerate(
            (
                (src_in, v0.at[:, pl.ds(own_lo, layers), pl.ds(8, 32), :]),
                (logc_in, logc),
                (rec_in, recs.at[1]),
                (pg_in, pg),
                (pd_in, pd),
                (obs_in, obs),
                (wt_in, wt),
            )
        )
    ]
    for c in loads:
        c.start()
    barrier = pltpu.get_barrier_semaphore()
    greeted = [on_line(0, 1 - core)]
    greeted += [on_line(away, c) for away in range(1, line) for c in range(cores)]
    greeted += [(base + in_plane(d), slab) for d in range(positions - 1)]
    for to in greeted:
        pl.semaphore_signal(barrier, inc=1, device_id=to, device_id_type=MESH)

    edge = jnp.zeros((12, total_layers, 1, 128), F32)

    def clear_edges(arrays):
        for v in arrays:
            v[:, :, 7:8, :] = edge
            v[:, :, 40:41, :] = edge

    clear_edges((v0,))
    has_below = slab > 0
    has_above = slab < slabs - 1

    @pl.when(slab == 0)
    def _():
        v0[:, 0:own_lo, 8:40, :] = jnp.zeros((12, GHOSTS, 32, 128), F32)
        lcg[0:3] = jnp.zeros((3, 32, 128), F32)
        recs[0] = jnp.zeros((1, 128), jnp.int32)
        wanted[0] = jnp.zeros((2, 2, 3, 128), F32)
        weights_at[0] = jnp.zeros((2, 3, 128), F32)
        seen[0] = jnp.zeros((4, 2, 2, 3, 128), F32)

    @pl.when(slab == slabs - 1)
    def _():
        v0[:, own_hi:total_layers, 8:40, :] = jnp.zeros((12, GHOSTS, 32, 128), F32)
        lcg[3:6] = jnp.zeros((3, 32, 128), F32)
        recs[2] = jnp.zeros((1, 128), jnp.int32)
        wanted[2] = jnp.zeros((2, 2, 3, 128), F32)
        weights_at[2] = jnp.zeros((2, 3, 128), F32)
        seen[2] = jnp.zeros((4, 2, 2, 3, 128), F32)

    lanes = lax.broadcasted_iota(jnp.int32, (1, 128), 1)
    lane8 = lax.broadcasted_iota(jnp.int32, (8, 128), 1)
    last8 = lane8 == 127

    def in_lanes(sums):
        row = jnp.zeros((1, 128), F32)
        for n, s in enumerate(sums):
            one = jnp.sum(s, axis=0, keepdims=True)
            row = row + jnp.where(lanes == n, jnp.sum(one, axis=1, keepdims=True), 0.0)
        return row

    def pick(row, n):
        return jnp.sum(jnp.where(lanes == n, row, 0.0), axis=1, keepdims=True)

    loads[1].wait()
    omega = omega_ref[0]
    kap[own_lo:own_hi] = omega * jnp.exp(logc[...])
    loads[0].wait()

    def weigh(l, acc):
        acc = list(acc)
        across = jnp.where(l == own_hi - 1, 0.0, layers / (layers - 1.0)).astype(F32)
        beyond = jnp.where(l == own_hi - 1, l, l + 1)
        for r in range(4):
            y = 8 + 8 * r
            coupling = kap[l, 8 * r : 8 * r + 8, :]
            acc[6] = acc[6] + coupling
            for pol in range(2):
                square = product = None
                for p in range(6 * pol, 6 * pol + 6):
                    here = v0[p, l, y : y + 8, :]
                    more = jnp.where(last8, 0.0, pltpu.roll(here, 127, 1))
                    more = more + v0[p, l, y + 1 : y + 9, :]
                    more = more + across * v0[p, beyond, y : y + 8, :]
                    sq, pr = here * here, here * more
                    square = sq if square is None else square + sq
                    product = pr if product is None else product + pr
                acc[3 * pol] = acc[3 * pol] + square
                acc[3 * pol + 1] = acc[3 * pol + 1] + product
                acc[3 * pol + 2] = acc[3 * pol + 2] + coupling * square
        return tuple(acc)

    weights = lax.fori_loop(own_lo, own_hi, weigh, (jnp.zeros((8, 128), F32),) * 7)

    def slab_start(n, row):
        allred[n, slab] = row
        copies = []
        for d in range(slabs - 1):
            down, up = slabs - 1 - d, d
            down = jnp.where(down > slab, down, down - 1)
            up = jnp.where(up < slab, up, up + 1)
            copies.append(
                remote(
                    allred.at[n, slab],
                    allred.at[n, slab],
                    ar_send.at[n, d],
                    ar_recv.at[n, slab],
                    (freq, jnp.where(slab < slabs // 2, down, up)),
                )
            )
        for c in copies:
            c.start()
        return copies

    def slab_finish(n):
        for d in range(1, slabs):
            other = (slab + d) % slabs
            remote(
                allred.at[n, other],
                allred.at[n, other],
                ar_send.at[n, d],
                ar_recv.at[n, other],
                (freq, other),
            ).wait_recv()
        total = allred[n, 0]
        for j in range(1, slabs):
            total = total + allred[n, j]
        return total

    weights = in_lanes(weights)
    for n in range(2, len(loads)):
        loads[n].wait()
    for pol in range(2):
        for comp in range(3):
            at = slice(comp, comp + 1)
            weights_at[1, pol, at, :] = wt[comp, pol : pol + 1, :]
            for ri in range(2):
                wanted[1, pol, ri, at, :] = obs[pol, comp, ri : ri + 1, :]
    pl.semaphore_wait(barrier, len(greeted))
    sent = slab_start(0, weights)

    rows = pl.ds(8, 32)
    below_to = (freq, lax.max(slab - 1, 0))
    above_to = (freq, lax.min(slab + 1, slabs - 1))
    upward = [
        (recs.at[1], recs.at[0]),
        (logc.at[pl.ds(layers - 3, 3)], lcg.at[pl.ds(0, 3)]),
    ]
    downward = [
        (recs.at[1], recs.at[2]),
        (logc.at[pl.ds(0, 3)], lcg.at[pl.ds(3, 3)]),
    ]
    for k in range(GHOSTS):
        last = k == GHOSTS - 1
        of = pl.ds(6, 6) if last else slice(None)
        upward.append(
            (v0.at[of, own_hi - 1 - k, rows, :], v0.at[of, own_lo - 1 - k, rows, :])
        )
        of = pl.ds(0, 6) if last else slice(None)
        downward.append((v0.at[of, own_lo + k, rows, :], v0.at[of, own_hi + k, rows, :]))
    for ref in (wanted, weights_at):
        upward.append((ref.at[1], ref.at[0]))
        downward.append((ref.at[1], ref.at[2]))
    ups = [
        remote(s, d, near_send.at[0, n], near_recv.at[0, n], above_to)
        for n, (s, d) in enumerate(upward)
    ]
    downs = [
        remote(s, d, near_send.at[1, n], near_recv.at[1, n], below_to)
        for n, (s, d) in enumerate(downward)
    ]

    @pl.when(has_above)
    def _():
        for c in ups:
            c.start()

    @pl.when(has_below)
    def _():
        for c in downs:
            c.start()

    for l in range(layers):
        prior_pair[half, 0, l : l + 1, :] = pg[l]
        prior_pair[half, 1, l : l + 1, :] = pd[l]
    prior_copy = remote(
        prior_pair.at[half], prior_pair.at[half], pair_send.at[0], pair_recv.at[0], partner
    )
    prior_copy.start()

    def arrived(from_below, from_above):
        @pl.when(has_below)
        def _():
            for n in from_below:
                ups[n].wait_recv()

        @pl.when(has_above)
        def _():
            for n in from_above:
                downs[n].wait_recv()

    lane = lax.broadcasted_iota(jnp.int32, (32, 128), 1)
    first_lane, last_lane = lane == 0, lane == 127
    alive_low = jnp.where(slab == 0, 0.0, 1.0).astype(F32)
    alive_high = jnp.where(slab == slabs - 1, 0.0, 1.0).astype(F32)

    def alive(l):
        inside = jnp.where(l < own_lo, alive_low, 1.0)
        return jnp.where(l >= own_hi, alive_high, inside)

    def step(theta, src, dst, where, ghosts, beside=None):
        for pol in range(2):
            l = where[pol]

            def around(p, l=l):
                here = src[p, l, 8:40, :]
                total = src[p, l - 1, 8:40, :] + src[p, l + 1, 8:40, :]
                total = total + (src[p, l, 7:39, :] + src[p, l, 9:41, :])
                if beside is not None:
                    return here, total + beside[p, l]
                left = jnp.where(first_lane, 0.0, pltpu.roll(here, 1, 1))
                right = jnp.where(last_lane, 0.0, pltpu.roll(here, 127, 1))
                return here, total + (left + right)

            shift_re, shift_im = theta[pol]
            coupling = kap[l] + shift_im
            mask = alive(l) if ghosts else None
            for comp in range(3):
                p = pol * 6 + comp
                re, around_re = around(p)
                im, around_im = around(p + 3)
                if shift_re is not None:
                    around_re = around_re - shift_re * re
                    around_im = around_im - shift_re * im
                new_re = around_re + coupling * im
                new_im = around_im - coupling * re
                if mask is not None:
                    new_re, new_im = mask * new_re, mask * new_im
                dst[p, l, 8:40, :] = new_re
                dst[p + 3, l, 8:40, :] = new_im

    def sweep(theta, src, dst, starts, count, ghosts, beside=None):
        def body(n, carry):
            for k in range(2):
                step(theta, src, dst, [at + 2 * n + k for at in starts], ghosts, beside)
            return carry

        lax.fori_loop(0, count // 2, body, 0)
        if count % 2:
            step(theta, src, dst, [at + count - 1 for at in starts], ghosts, beside)

    def both(theta, src, dst, low, high, ghosts):
        for l in (low, high):
            step(theta, src, dst, (l, l), ghosts)

    def moment_sums(theta, v_list):
        v3 = v_list[3]
        sums = []
        for pol in range(2):
            shift_re, shift_im = theta[pol]

            def body(l, acc):
                acc = list(acc)

                def add(k, value):
                    acc[k] = acc[k] + value

                for r in range(4):
                    y = 8 + 8 * r
                    coupling = kap[l, 8 * r : 8 * r + 8, :] + shift_im
                    for comp in range(3):
                        p = pol * 6 + comp
                        vs = [(v[p, l, y : y + 8, :], v[p + 3, l, y : y + 8, :]) for v in v_list]
                        for k in range(4):
                            re, im = vs[k]
                            add(4 * k, (re - im) * (re + im))
                            add(4 * k + 1, re * im)
                        halves = []
                        for q in (p, p + 3):
                            here = v3[q, l, y : y + 8, :]
                            right = jnp.where(last8, 0.0, pltpu.roll(here, 127, 1))
                            more = v3[q, l, y + 1 : y + 9, :] + right
                            halves.append(more + more)
                        re, im = vs[3]
                        if shift_re is not None:
                            halves = [halves[0] - shift_re * re, halves[1] - shift_re * im]
                        after = (halves[0] + coupling * im, halves[1] - coupling * re)
                        pairs = [(vs[0], vs[1]), (vs[1], vs[2]), (vs[2], vs[3]), (vs[3], after)]
                        for k, (u, w) in enumerate(pairs):
                            add(4 * k + 2, u[0] * w[0] - u[1] * w[1])
                            add(4 * k + 3, u[0] * w[1] + u[1] * w[0])
                return tuple(acc)

            zero = jnp.zeros((8, 128), F32)
            sums += list(lax.fori_loop(own_lo, own_hi, body, (zero,) * 16))
        return sums

    def layer_pair(v3, where, acc):
        acc = list(acc)
        for pol in range(2):
            l = where[pol]
            for comp in range(3):
                for r in range(4):
                    p, y = pol * 6 + comp, 8 + 8 * r
                    u = (v3[p, l, y : y + 8, :], v3[p + 3, l, y : y + 8, :])
                    w = (v3[p, l + 1, y : y + 8, :], v3[p + 3, l + 1, y : y + 8, :])
                    acc[2 * pol] = acc[2 * pol] + (u[0] * w[0] - u[1] * w[1])
                    acc[2 * pol + 1] = acc[2 * pol + 1] + (u[0] * w[1] + u[1] * w[0])
        return tuple(acc)

    def pair_row(pairs):
        row = in_lanes([p + p for p in pairs])
        spread = jnp.zeros((1, 128), F32)
        for n, at in enumerate((14, 15, 30, 31)):
            spread = spread + jnp.where(lanes == at, pick(row, n), 0.0)
        return spread

    def layer_pairs(v3, starts, count):
        def body(n, acc):
            return layer_pair(v3, [at + n for at in starts], acc)

        return lax.fori_loop(0, count, body, (jnp.zeros((8, 128), F32),) * 4)

    def solve_coefficients(row, theta):
        found = []
        for pol in range(2):
            moments = []
            for k in range(8):
                re = pick(row, 16 * pol + 2 * k) * 6.0**-k
                im = pick(row, 16 * pol + 2 * k + 1) * 6.0**-k
                if k % 2 == 0:
                    im = im + im
                moments.append((re, im))
            most = None
            for m in moments:
                size = jnp.maximum(jnp.abs(m[0]), jnp.abs(m[1]))
                most = size if most is None else jnp.maximum(most, size)
            scale = 1.0 / most
            moments = [(m[0] * scale, m[1] * scale) for m in moments]
            found.append(coefficients(moments, theta[pol]))
        return found

    def combined(coefs, v_list, pol, comp, l, y):
        p = pol * 6 + comp
        re = im = None
        for (cr, ci), v in zip(coefs[pol], v_list):
            a, b = v[p, l, y : y + 8, :], v[p + 3, l, y : y + 8, :]
            tr, ti = cr * a - ci * b, cr * b + ci * a
            re, im = (tr, ti) if re is None else (re + tr, im + ti)
        return re, im

    line_of, lane_of = recs[1] // 128, recs[1] % 128

    def columns(lane_of):
        distance = jnp.abs(lax.broadcasted_iota(jnp.int32, (128, 128), 0) - lane_of)
        both = jnp.concatenate([distance == 0, distance == 1], axis=0)
        return both.astype(F32).astype(BF16)

    column_hot[1] = columns(lane_of)
    at_row = lax.broadcasted_iota(jnp.int32, (wide, 128), 0) == line_of

    def look(j, v):
        def body(pol, carry):
            column = column_hot[1, 0:128]
            taller = jnp.concatenate([column] * 3, axis=0)
            planes = v[pl.ds(pol * 6, 6), own_lo:own_hi, 8:40, :].reshape(6 * wide, 128)
            parts = jnp.concatenate(split3(planes), axis=1)
            found = jnp.dot(parts, taller, preferred_element_type=F32)
            for k in range(6):
                rows = jnp.where(at_row, found[wide * k : wide * (k + 1)], 0.0)
                value = jnp.sum(rows, axis=0, keepdims=True)
                seen[1, j, pol, k // 3, k % 3 : k % 3 + 1, :] = value
            return carry

        lax.fori_loop(0, 2, body, 0)

    forward, backward = (v0, v1, v2, v3), (u0, u1, u2, u3)
    clear_edges(forward[1:] + backward)
    look(0, v0)
    weights = slab_finish(0)
    theta = []
    for pol in range(2):
        square = pick(weights, 3 * pol)
        theta.append(
            (
                2.0 * pick(weights, 3 * pol + 1) / square,
                -pick(weights, 3 * pol + 2) / square,
            )
        )
    mean_coupling = pick(weights, 6) / float(slabs * wide * 128)
    middle = own_lo + layers // 2
    sweep(theta, v0, v1, (own_lo + 1,) * 2, layers - 2, False)
    step(theta, v1, v2, (middle, middle), False)
    arrived((0, 1), (0, 1))
    kap[own_lo - 3 : own_lo] = omega * jnp.exp(lcg[0:3])
    kap[own_hi : own_hi + 3] = omega * jnp.exp(lcg[3:6])
    arrived((2,), (2,))
    both(theta, v0, v1, own_lo, own_hi - 1, False)
    both(theta, v1, v2, own_lo + 1, own_hi - 2, False)
    step(theta, v2, v3, (middle, middle), False)
    look(1, v1)
    arrived((3,), (3,))
    both(theta, v0, v1, own_lo - 1, own_hi, True)
    both(theta, v1, v2, own_lo, own_hi - 1, False)
    both(theta, v2, v3, own_lo + 1, own_hi - 2, False)
    look(2, v2)
    arrived((4,), (4,))
    both(theta, v0, v1, own_lo - 2, own_hi + 1, True)
    both(theta, v1, v2, own_lo - 1, own_hi, True)
    both(theta, v2, v3, own_lo, own_hi - 1, False)
    row = in_lanes(moment_sums(theta, forward))
    pairs = layer_pairs(v3, (own_lo, own_lo), layers - 1)
    arrived((5,), (5,))
    step(theta, v0, v1, (own_hi + 2, own_lo - 3), True)
    step(theta, v1, v2, (own_hi + 1, own_lo - 2), True)
    step(theta, v2, v3, (own_hi, own_lo - 1), True)
    pairs = layer_pair(v3, (own_hi - 1, own_lo - 1), pairs)
    sent += slab_start(1, row + pair_row(pairs))

    look(3, v3)
    seen_up = remote(seen.at[1], seen.at[0], seen_send.at[0], seen_recv.at[0], above_to)
    seen_down = remote(seen.at[1], seen.at[2], seen_send.at[1], seen_recv.at[1], below_to)

    @pl.when(has_above)
    def _():
        seen_up.start()

    @pl.when(has_below)
    def _():
        seen_down.start()

    spots = (
        (0, 32 * (layers - GHOSTS), GHOSTS, 0),
        (1, 0, layers, own_lo),
        (2, 0, GHOSTS, own_hi),
    )
    for n, first_row, count, layer_at in spots:
        line_of, lane_of = recs[n] // 128, recs[n] % 128
        if n != 1:
            column_hot[n] = columns(lane_of)
        rows_here = lax.broadcasted_iota(jnp.int32, (32 * count, 128), 0) + first_row
        hit = (rows_here == line_of).astype(F32).astype(BF16)
        row_hot[32 * layer_at : 32 * (layer_at + count), :] = hit

    arrived((6, 7), (6, 7))

    @pl.when(has_below)
    def _():
        seen_up.wait_recv()

    @pl.when(has_above)
    def _():
        seen_down.wait_recv()

    row = slab_finish(1)
    coefs = solve_coefficients(row, theta)

    for n in range(3):
        for pol in range(2):
            re = im = None
            for j, (cr, ci) in enumerate(coefs[pol]):
                a, b = seen[n, j, pol, 0], seen[n, j, pol, 1]
                tr, ti = cr * a - ci * b, cr * b + ci * a
                re, im = (tr, ti) if re is None else (re + tr, im + ti)
            weight = weights_at[n, pol]
            square = weight * weight
            data[n, pol, 0] = square * (re - wanted[n, pol, 0])
            data[n, pol, 1] = -square * (im - wanted[n, pol, 1])

    for n, _, count, layer_at in spots:
        wider = jnp.concatenate([column_hot[n]] * 3, axis=1)
        for pol in range(2):
            first, much = layer_at, count
            if n == 2 - 2 * pol:
                pass
            elif n != 1:
                much = count - 1
                first = layer_at + (1 if n == 0 else 0)
            hit = row_hot[32 * first : 32 * (first + much), :]
            spread = []
            for ri in range(2):
                for comp in range(3):
                    parts = split3(data[n, pol, ri, comp : comp + 1, :])
                    spread.append(jnp.concatenate([hit * part for part in parts], axis=1))
            placed = lax.dot_general(
                jnp.concatenate(spread, axis=0),
                wider,
                (((1,), (1,)), ((), ())),
                preferred_element_type=F32,
            )
            own = slice(6 * pol, 6 * pol + 6), slice(first, first + much)
            u0[*own, 8:40, :] = placed[:, 0:128].reshape(6, much, 32, 128)
            sides[*own] = placed[:, 128:256].reshape(6, much, 32, 128)

    behind = [(None, -mean_coupling)] * 2
    sweep(behind, u0, u1, (own_lo - 2, own_lo - 3), layers + 5, True, sides)
    sweep(behind, u1, u2, (own_lo - 1, own_lo - 2), layers + 3, True)
    sweep(behind, u2, u3, (own_lo, own_lo - 1), layers + 1, True)
    sums = moment_sums(behind, backward)
    pairs = layer_pairs(u3, (own_lo, own_lo - 1), layers)
    for pol in range(2):
        for part in range(2):
            at, more = 16 * pol + 14 + part, pairs[2 * pol + part]
            sums[at] = sums[at] + (more + more)
    sent += slab_start(2, in_lanes(sums))

    prior_copy.wait()
    prior_all[place] = prior_pair[...]
    fan = [
        remote(
            prior_pair,
            prior_all.at[place],
            fan_send.at[0, d],
            fan_recv.at[0, place],
            (base + in_plane(d), slab),
        )
        for d in range(positions - 1)
    ]
    for c in fan:
        c.start()

    def multiply(l, carry):
        for r in range(4):
            y = 8 + 8 * r
            at = pl.multiple_of((l - own_lo) * 32 + 8 * r, 8)
            coupling = kap[l, 8 * r : 8 * r + 8, :]
            for pol in range(2):
                fields = [combined(coefs, forward, pol, comp, l, y) for comp in range(3)]
                for j, u in enumerate(backward):
                    first = second = None
                    for comp in range(3):
                        p = pol * 6 + comp
                        re, im = u[p, l, y : y + 8, :], u[p + 3, l, y : y + 8, :]
                        f_re, f_im = fields[comp]
                        x, z = re * f_im + im * f_re, re * f_re - im * f_im
                        first, second = (x, z) if first is None else (first + x, second + z)
                    products[pol, j, 0, pl.ds(at, 8), :] = coupling * first
                    products[pol, j, 1, pl.ds(at, 8), :] = coupling * second
        return carry

    lax.fori_loop(own_lo, own_hi, multiply, 0)
    row = slab_finish(2)
    coefs = solve_coefficients(row, [(jnp.zeros_like(mean_coupling), -mean_coupling)] * 2)
    for n in range(wide // 8):
        total = None
        for pol in range(2):
            for j in range(4):
                for part in range(2):
                    term = coefs[pol][j][part] * products[pol, j, part, 8 * n : 8 * n + 8, :]
                    total = term if total is None else total + term
        grad[8 * n : 8 * n + 8, :] = total

    for j in range(positions):
        grad_src[j] = grad[chunk * j : chunk * (j + 1), :]
    grad_in[place] = grad_src[place]
    spread = []
    for d in range(positions - 1):
        j = in_plane(d)
        spread.append(
            remote(
                grad_src.at[j],
                grad_in.at[place],
                fan_send.at[1, d],
                fan_recv.at[1, place],
                (base + j, slab),
            )
        )
    for c in spread:
        c.start()

    def gathered(n, ref):
        for d in range(positions - 1):
            j = in_plane(d)
            remote(
                ref.at[j], ref.at[j], fan_send.at[n, d], fan_recv.at[n, j], (base + j, slab)
            ).wait_recv()

    gathered(0, prior_all)
    for y in range(2 * positions):
        for w in range(2):
            for l in range(layers):
                prior[w, 32 * l + y : 32 * l + y + 1, :] = prior_all[
                    y % positions, y // positions, w, l : l + 1, :
                ]
    for w in range(2):
        for j in range(positions):
            prior_src[w, j] = prior[w, chunk * j : chunk * (j + 1), :]

    def over_chunks(a, b):
        total = a[0] * b[0]
        for j in range(1, positions):
            total = total + a[j] * b[j]
        return total

    old_grad, old_dir = prior_src.at[0], prior_src.at[1]
    prior_row = in_lanes(
        [jnp.zeros((chunk, 128), F32)] * 3
        + [over_chunks(old_grad, old_grad), over_chunks(old_dir, old_dir)]
    )

    gathered(1, grad_in)
    partial = grad_in[0]
    for j in range(1, positions):
        partial = partial + grad_in[j]
    grad_pair[half] = partial
    pair_copy = remote(
        grad_pair.at[half], grad_pair.at[half], pair_send.at[1], pair_recv.at[1], partner
    )
    pair_copy.start()
    pair_copy.wait_recv()
    grad_all[place] = grad_pair[0] + grad_pair[1]
    share = []
    for d in range(positions - 1):
        to = (base + in_plane(d), slab)
        share.append(
            remote(
                grad_all.at[place], grad_all.at[place], fan_send.at[2, d], fan_recv.at[2, place], to
            )
        )
    for c in share:
        c.start()
    gathered(2, grad_all)

    others = (grad_all, old_grad, old_dir)
    ends[slab] = in_lanes([over_chunks(grad_all, x) for x in others]) + prior_row
    closing = []
    for away, other in [(a, c) for a in (2, 1, -1) for c in range(cores)] + [(0, 1 - core)]:
        n = len(closing)
        to = on_line(away, other)
        source = on_line(-away, other)[1]
        closing.append(
            (
                remote(ends.at[slab], ends.at[slab], end_send.at[n], end_recv.at[slab], to),
                remote(ends.at[source], ends.at[source], end_send.at[n], end_recv.at[source], to),
            )
        )
    for c, _ in closing:
        c.start()
    for j in range(positions):
        whole[chunk * j : chunk * (j + 1), :] = grad_all[j]
    for _, c in closing:
        c.wait_recv()
    row = ends[0]
    for j in range(1, slabs):
        row = row + ends[j]
    gg, gq, gd, qq, dd = [pick(row, n) for n in range(5)]
    cells = float(slabs * wide * 128)
    mean_square = gg / cells + epsilon
    inverse = 1.0 / jnp.sqrt(mean_square)
    beta = (gg / mean_square - gq * inverse) / (qq + epsilon)
    squared = gg / mean_square - 2.0 * beta * (gd * inverse) + beta * beta * dd
    norm = 1.0 / jnp.sqrt(jnp.maximum(squared, 0.0) / cells + epsilon)
    whole[...] = (-inverse * norm) * whole[...] + (beta * norm) * prior[1]
    for l in range(layers):
        dir_ref[l] = whole[pl.ds(32 * l + freq, 1), :]
    trial_ref[...] = logc[...] + step_ref[0] * whole[...].reshape(layers, 32, 128)

    @pl.when(has_above)
    def _():
        for c in ups + [seen_up]:
            c.wait_send()

    @pl.when(has_below)
    def _():
        for c in downs + [seen_down]:
            c.wait_send()

    pair_copy.wait_send()
    for c in sent + fan + spread + share + [c for c, _ in closing]:
        c.wait_send()


def deliver(dir_in, trial_in, dir_out, trial_out, sems):
    copies = [
        pltpu.make_async_copy(dir_in, dir_out, sems.at[0]),
        pltpu.make_async_copy(trial_in, trial_out, sems.at[1]),
    ]
    for c in copies:
        c.start()
    for c in copies:
        c.wait()


def per_device(
    slabs,
    positions,
    log_conductivity,
    omega,
    sources,
    receivers,
    observed,
    data_weight,
    prior_gradient,
    prior_direction,
    step_length,
):
    layers = log_conductivity.shape[0]
    total = layers + 2 * GHOSTS
    wide = layers * 32
    chunk = (positions, wide // positions, 128)
    hbm = pl.BlockSpec(memory_space=pltpu.HBM)
    smem = pl.BlockSpec(memory_space=pltpu.SMEM)
    vmem = pl.BlockSpec(memory_space=pltpu.VMEM)
    state = pltpu.VMEM((12, total, 48, 128), F32)
    results = pl.pallas_call(
        functools.partial(kernel, layers, slabs, positions),
        out_shape=(
            jax.ShapeDtypeStruct(prior_gradient.shape, F32),
            jax.ShapeDtypeStruct(log_conductivity.shape, F32),
        ),
        in_specs=[smem] * 2 + [hbm] * 7,
        out_specs=(vmem, vmem),
        scratch_shapes=[
            pltpu.VMEM((layers, 32, 128), F32),
            pltpu.VMEM((2, 3, 2, 128), F32),
            pltpu.VMEM((3, 2, 128), F32),
            pltpu.VMEM((layers, 1, 128), F32),
            pltpu.VMEM((layers, 1, 128), F32),
            *[state] * 8,
            pltpu.VMEM((12, total, 32, 128), F32),
            pltpu.VMEM((total, 32, 128), F32),
            pltpu.VMEM((6, 32, 128), F32),
            pltpu.VMEM((3, 1, 128), jnp.int32),
            pltpu.VMEM((3, 2, 2, 3, 128), F32),
            pltpu.VMEM((3, 2, 3, 128), F32),
            pltpu.VMEM((3, 4, 2, 2, 3, 128), F32),
            pltpu.VMEM((3, 2, 2, 3, 128), F32),
            pltpu.VMEM((32 * total, 128), BF16),
            pltpu.VMEM((3, 256, 128), BF16),
            pltpu.VMEM((2, 4, 2, wide, 128), F32),
            pltpu.VMEM((3, slabs, 1, 128), F32),
            pltpu.VMEM((slabs, 1, 128), F32),
            pltpu.VMEM((2, 2, layers, 128), F32),
            pltpu.VMEM((positions, 2, 2, layers, 128), F32),
            pltpu.VMEM((2, wide, 128), F32),
            pltpu.VMEM((2,) + chunk, F32),
            pltpu.VMEM((wide, 128), F32),
            pltpu.VMEM(chunk, F32),
            pltpu.VMEM(chunk, F32),
            pltpu.VMEM((2,) + chunk[1:], F32),
            pltpu.VMEM(chunk, F32),
            pltpu.VMEM((wide, 128), F32),
            pltpu.SemaphoreType.DMA((7,)),
            pltpu.SemaphoreType.DMA((2, 8)),
            pltpu.SemaphoreType.DMA((2, 8)),
            pltpu.SemaphoreType.DMA((2,)),
            pltpu.SemaphoreType.DMA((2,)),
            pltpu.SemaphoreType.DMA((3, slabs)),
            pltpu.SemaphoreType.DMA((3, slabs)),
            pltpu.SemaphoreType.DMA((slabs,)),
            pltpu.SemaphoreType.DMA((slabs,)),
            pltpu.SemaphoreType.DMA((2,)),
            pltpu.SemaphoreType.DMA((2,)),
            pltpu.SemaphoreType.DMA((3, positions)),
            pltpu.SemaphoreType.DMA((3, positions)),
        ],
        compiler_params=pltpu.CompilerParams(
            collective_id=0, has_side_effects=True, vmem_limit_bytes=48 * 1024 * 1024
        ),
        name="inversion_step",
    )(
        omega,
        step_length,
        *(
            pltpu.with_memory_space_constraint(x, pltpu.HBM)
            for x in (
                log_conductivity,
                sources.reshape(12, layers, 32, 128),
                receivers.reshape(1, 128),
                observed[0].transpose(0, 2, 1, 3),
                data_weight[0].transpose(1, 0, 2),
                prior_gradient,
                prior_direction,
            )
        ),
    )
    return pl.pallas_call(
        deliver,
        out_shape=tuple(jax.ShapeDtypeStruct(r.shape, F32) for r in results),
        in_specs=[vmem] * 2,
        out_specs=(hbm, hbm),
        scratch_shapes=[pltpu.SemaphoreType.DMA((2,))],
        compiler_params=pltpu.CompilerParams(vmem_limit_bytes=16 * 1024 * 1024),
        name="deliver",
    )(*results)


def solution(mesh):
    slabs = mesh.shape["slab"]
    positions = mesh.shape["freq"] // 2
    in_specs = (
        P("slab", None, None),
        P("freq"),
        P("freq", None, None, None, "slab", None, None),
        P("slab"),
        P("freq", None, None, None, "slab"),
        P("freq", None, None, "slab"),
        P("slab", "freq", None),
        P("slab", "freq", None),
        P(),
    )
    out_specs = (P("slab", "freq", None), P("slab", None, None))
    return jax.shard_map(
        functools.partial(per_device, slabs, positions),
        mesh=mesh,
        in_specs=in_specs,
        out_specs=out_specs,
        check_vma=False,
    )
```
